32 devices in a mesh: parts: 32 (over z, y, x, core).
Axes of the slice: x: 2, y: 2, z: 4, core: 2. Of those that a mesh axis runs over, the one named last changes fastest.
Arguments:
- rhs: float32 [216, 16384], P(None, 'parts'), may hold values from -60 to 90
- start: float32 [216, 16384], P(None, 'parts'), may hold values from -3.75 to 5.625
- spectrum_top: float32 [1], replicated, may hold values from 10 to 20
- elem_code: int32 [16384], P('parts'), may hold values from 0 to 2, as said below
- rec_elem: int32 [98304], P('parts'), may hold values from 0 to 511, as said below
- rec_dir: int32 [98304], P('parts'), may hold values from 0 to 5
- rec_sub: int32 [98304], P('parts'), may hold values from 0 to 5, as said below
- rec_peer: int32 [98304], P('parts'), may hold values from -1 to 31, as said below
- rec_index: int32 [98304], P('parts'), may hold values from 0 to 3071, as said below
- send_rec: int32 [262144], P('parts'), may hold values from 0 to 3071, as said below
Outputs:
- solution: float32 [216, 16384], P(None, 'parts')
- norms: float32 [3, 2], replicated
The draws below stay inside these ranges and needn't reach their ends.
Inputs may be any that keep to these rules, and one draw needn't show every extreme that they name: `elem_code`: 0 marks an empty slot, 1 a fine element, 2 a coarse element; a device's live slots come first. `rec_elem`: always a live element of the record's device. `rec_sub`: 0 to 3: a quarter of a coarse face facing a fine element; 4: the whole face; 5: an unused slot, which comes after the device's used records. `rec_peer`: -1 at the channel's ends and on unused slots. A partner is never more than 7 devices away; its face has the opposite direction, and the partner's partner is the record itself. `rec_index`: A record index on the same device, or a slot of the partner device's send list to this device. `send_rec`: entries of slots that no record names are arbitrary. At most 256 slots are named from one device to another, and some pair of devices uses all 256.
All inputs are finite; a program needn't handle non-finite values.
Results may differ from the reference program's by a relative error of at most 0.0003.
Values sent between devices are 32-bit elements; how exact they have to be, the bound alone decides.
A program may use at most 128 MiB of HBM per device.

```python
import math
import jax
import jax.numpy as jnp
import numpy as np
from jax import lax

NODES = 216
US = 8
LX_DEV = 1
LD = 4
ITERS = 3
ELEMS = 16384
N_PARTS = 32


def spread_bits(number):
    result = jnp.zeros_like(number)
    for bit_index in range(4):
        result = result | (number >> bit_index & 1) << 2 * bit_index
    return result


def gather_bits(number):
    result = jnp.zeros_like(number)
    for bit_index in range(4):
        result = result | (number >> 2 * bit_index & 1) << bit_index
    return result


def shuffle_group(sub_key):
    return jax.random.permutation(sub_key, LD).astype(jnp.int32)


def mesh_layout(key):
    units_dev = LX_DEV * US * US
    unit_total = N_PARTS * units_dev
    elem_dev = 8 * units_dev
    rec_dev = 48 * units_dev
    capacity = max(4 * US * US, 8 * LX_DEV * US)
    cross_span = 2 * US
    group_count = N_PARTS // LD
    length_span = group_count * LX_DEV
    far_reach = 2 * LD - 1
    group_keys = jax.random.split(jax.random.fold_in(key, 11), group_count)
    place_of = jax.vmap(shuffle_group)(group_keys)
    quadrant_of = jnp.argsort(place_of, axis=1).astype(jnp.int32)
    unit_id = jnp.arange(unit_total, dtype=jnp.int32)
    device_of = unit_id // units_dev
    coin_flip = jax.random.randint(jax.random.fold_in(key, 7), (unit_total,), 0, 5)
    refined = (coin_flip < 2) | (device_of < 2 * LD)
    local_unit = unit_id % units_dev
    morton = local_unit % (US * US)
    own_quadrant = quadrant_of[device_of // LD, device_of % LD]
    coord_x = device_of // LD * LX_DEV + local_unit // (US * US)
    coord_y = own_quadrant % 2 * US + gather_bits(morton)
    coord_z = own_quadrant // 2 * US + gather_bits(morton >> 1)

    def unit_at(pos_x, pos_y, pos_z):
        group_index = pos_x // LX_DEV
        quadrant = pos_y // US + 2 * (pos_z // US)
        device = group_index * LD + place_of[group_index, quadrant]
        inner_index = spread_bits(pos_y % US) | spread_bits(pos_z % US) << 1
        return device * units_dev + pos_x % LX_DEV * US * US + inner_index
    child_index = jnp.arange(8, dtype=jnp.int32)[None, :, None]
    direction = jnp.arange(6, dtype=jnp.int32)[None, None, :]
    axis_index = direction // 2
    face_side = direction % 2
    bit_x = child_index & 1
    bit_y = child_index >> 1 & 1
    bit_z = child_index >> 2 & 1
    bit_axis = jnp.where(axis_index == 0, bit_x, jnp.where(axis_index == 1, bit_y, bit_z))
    first_bit = jnp.where(axis_index == 0, bit_y, bit_x)
    second_bit = jnp.where(axis_index == 2, bit_y, bit_z)
    step_sign = 2 * face_side - 1
    near_x = coord_x[:, None, None] + step_sign * (axis_index == 0).astype(jnp.int32)
    near_y = (coord_y[:, None, None] + step_sign * (axis_index == 1).astype(jnp.int32)) % cross_span
    near_z = (coord_z[:, None, None] + step_sign * (axis_index == 2).astype(jnp.int32)) % cross_span
    outside = (near_x < 0) | (near_x >= length_span)
    near_unit = unit_at(jnp.clip(near_x, 0, length_span - 1), near_y, near_z)
    near_refined = refined[near_unit]
    own_refined = refined[:, None, None]
    internal = own_refined & (bit_axis != face_side)
    flip_child = child_index ^ 1 << axis_index
    coarse_slot = first_bit + 2 * second_bit
    facing = 1 - face_side
    low_bit = child_index & 1
    high_bit = child_index >> 1 & 1
    facing_child = jnp.where(axis_index == 0, facing + 2 * low_bit + 4 * high_bit, jnp.where(axis_index == 1, low_bit + 2 * facing + 4 * high_bit, low_bit + 2 * high_bit + 4 * facing))
    shape_all = (unit_total, 8, 6)
    partner_unit = jnp.where(internal, unit_id[:, None, None], near_unit)
    partner_child = jnp.where(own_refined, jnp.where(internal | near_refined, flip_child, coarse_slot), jnp.where(near_refined, facing_child, 0))
    boundary = jnp.logical_not(internal) & outside
    valid_mask = jnp.where(own_refined, True, (child_index == 0) | (child_index < 4) & near_refined & jnp.logical_not(outside))
    sub_code = jnp.where(own_refined | outside | jnp.logical_not(near_refined), 4, child_index)
    unit_size = jnp.where(refined, 8, 1).astype(jnp.int32)
    start_all = jnp.cumsum(unit_size) - unit_size
    elem_offset = start_all - start_all[device_of * units_dev]
    elem_local = elem_offset[:, None, None] + jnp.where(own_refined, child_index, 0)
    child_row = jnp.arange(8, dtype=jnp.int32)[None, :]
    elem_slot = device_of[:, None] * elem_dev + elem_offset[:, None] + child_row
    keep_slot = refined[:, None] | (child_row == 0)
    elem_value = jnp.broadcast_to(jnp.where(refined, 1, 2).astype(jnp.int32)[:, None], (unit_total, 8))
    elem_code = jnp.zeros((N_PARTS * elem_dev,), jnp.int32).at[jnp.where(keep_slot, elem_slot, N_PARTS * elem_dev).reshape(-1)].set(elem_value.reshape(-1), mode='drop')
    valid_flat = jnp.broadcast_to(valid_mask, shape_all).reshape(-1)
    bound_flat = jnp.broadcast_to(boundary, shape_all).reshape(-1)
    valid_count = valid_flat.astype(jnp.int32)
    before = jnp.cumsum(valid_count) - valid_count
    cand_total = unit_total * 48
    cand_device = jnp.arange(cand_total, dtype=jnp.int32) // rec_dev
    local_rec = before - before[cand_device * rec_dev]
    partner_cand = (jnp.broadcast_to(partner_unit, shape_all) * 48 + jnp.broadcast_to(partner_child, shape_all) * 6 + jnp.broadcast_to(direction ^ 1, shape_all)).reshape(-1)
    partner_cand = jnp.where(bound_flat, 0, partner_cand)
    partner_device = partner_cand // rec_dev
    remote = valid_flat & jnp.logical_not(bound_flat) & (partner_device != cand_device)
    offset = jnp.clip(partner_device - cand_device + far_reach, 0, 2 * far_reach)
    onehot = ((offset[:, None] == jnp.arange(2 * far_reach + 1, dtype=jnp.int32)[None, :]) & remote[:, None]).astype(jnp.int32)
    running = jnp.cumsum(onehot, axis=0) - onehot
    running = running - running[cand_device * rec_dev]
    send_slot = jnp.take_along_axis(running, offset[:, None], axis=1)[:, 0]
    target = jnp.where(valid_flat, cand_device * rec_dev + local_rec, N_PARTS * rec_dev)
    slot_total = N_PARTS * rec_dev
    rec_elem = jnp.zeros((slot_total,), jnp.int32).at[target].set(jnp.broadcast_to(elem_local, shape_all).reshape(-1), mode='drop')
    rec_dir = jnp.zeros((slot_total,), jnp.int32).at[target].set(jnp.broadcast_to(direction, shape_all).reshape(-1), mode='drop')
    rec_sub = jnp.full((slot_total,), 5, jnp.int32).at[target].set(jnp.broadcast_to(sub_code, shape_all).reshape(-1), mode='drop')
    rec_peer = jnp.full((slot_total,), -1, jnp.int32).at[target].set(jnp.where(bound_flat, -1, partner_device), mode='drop')
    index_value = jnp.where(bound_flat, 0, jnp.where(remote, send_slot[partner_cand], local_rec[partner_cand]))
    rec_index = jnp.zeros((slot_total,), jnp.int32).at[target].set(index_value, mode='drop')
    link_total = N_PARTS * N_PARTS * capacity
    link_slot = jnp.where(remote, (cand_device * N_PARTS + partner_device) * capacity + send_slot, link_total)
    send_rec = jnp.zeros((link_total,), jnp.int32).at[link_slot].set(local_rec, mode='drop')
    return (elem_code, rec_elem, rec_dir, rec_sub, rec_peer, rec_index, send_rec)


def draw_elem_code(key, part):
    return mesh_layout(jax.random.fold_in(key, 3))[0]


def draw_rec_elem(key, part):
    return mesh_layout(jax.random.fold_in(key, 3))[1]


def draw_rec_dir(key, part):
    return mesh_layout(jax.random.fold_in(key, 3))[2]


def draw_rec_sub(key, part):
    return mesh_layout(jax.random.fold_in(key, 3))[3]


def draw_rec_peer(key, part):
    return mesh_layout(jax.random.fold_in(key, 3))[4]


def draw_rec_index(key, part):
    return mesh_layout(jax.random.fold_in(key, 3))[5]


def draw_send_rec(key, part):
    return mesh_layout(jax.random.fold_in(key, 3))[6]


def field_draw(key, base_scale):
    column = jnp.arange(ELEMS, dtype=jnp.float32) / ELEMS
    rough = jnp.clip(jax.random.normal(key, (NODES, ELEMS), jnp.float32), -5.0, 5.0)
    return base_scale * (1.0 + 2.0 * column)[None, :] * rough


def draw_rhs(key, part):
    return field_draw(jax.random.fold_in(key, 21), 4.0)


def draw_start(key, part):
    return field_draw(jax.random.fold_in(key, 22), 0.25)


def setup_inputs(seed: int = 0) -> dict:
    splits = jax.random.split(jax.random.key(seed), 11)
    return {
        "rhs": draw_rhs(jax.random.fold_in(splits[10], 71), 0),
        "start": draw_start(jax.random.fold_in(splits[10], 71), 0),
        "spectrum_top": jnp.clip(jax.random.uniform(splits[2], (1,), jnp.float32, 10.0, 20.0), 10.0, 20.0),
        "elem_code": draw_elem_code(jax.random.fold_in(splits[10], 71), 0),
        "rec_elem": draw_rec_elem(jax.random.fold_in(splits[10], 71), 0),
        "rec_dir": draw_rec_dir(jax.random.fold_in(splits[10], 71), 0),
        "rec_sub": draw_rec_sub(jax.random.fold_in(splits[10], 71), 0),
        "rec_peer": draw_rec_peer(jax.random.fold_in(splits[10], 71), 0),
        "rec_index": draw_rec_index(jax.random.fold_in(splits[10], 71), 0),
        "send_rec": draw_send_rec(jax.random.fold_in(splits[10], 71), 0),
    }


PENALTY = 36.0
BOTTOM_RATIO = 8.0
HIGHEST = lax.Precision.HIGHEST

def lobatto_tables():
    root_seven = math.sqrt(7.0)
    inner_root = math.sqrt(1.0 / 3.0 - 2.0 * root_seven / 21.0)
    outer_root = math.sqrt(1.0 / 3.0 + 2.0 * root_seven / 21.0)
    points = (np.array([-1.0, -outer_root, -inner_root, inner_root, outer_root, 1.0]) + 1.0) / 2.0
    weights = np.array([1.0 / 15.0, (14.0 - root_seven) / 30.0, (14.0 + root_seven) / 30.0, (14.0 + root_seven) / 30.0, (14.0 - root_seven) / 30.0, 1.0 / 15.0]) / 2.0
    barycentric = np.array([1.0 / np.prod([points[j] - points[k] for k in range(6) if k != j]) for j in range(6)])
    derivative = np.zeros((6, 6))
    for i in range(6):
        for j in range(6):
            if i != j:
                derivative[i, j] = barycentric[j] / barycentric[i] / (points[i] - points[j])
        derivative[i, i] = -np.sum(derivative[i])
    halves = np.zeros((2, 6, 6))
    for which_half in range(2):
        targets = (points + which_half) / 2.0
        for i in range(6):
            for j in range(6):
                halves[which_half, i, j] = np.prod([(targets[i] - points[k]) / (points[j] - points[k]) for k in range(6) if k != j])
    column_sums = np.sum(derivative * derivative * weights[:, None], axis=0)
    stiff_diag = column_sums[:, None, None] * weights[None, :, None] * weights[None, None, :] + weights[:, None, None] * column_sums[None, :, None] * weights[None, None, :] + weights[:, None, None] * weights[None, :, None] * column_sums[None, None, :]
    return (weights, derivative, halves, stiff_diag.reshape(216))

def float_tables():
    weights, derivative, halves, stiff_diag = lobatto_tables()
    return (jnp.asarray(weights, dtype=jnp.float32), jnp.asarray(derivative, dtype=jnp.float32), jnp.asarray(halves, dtype=jnp.float32), jnp.asarray(stiff_diag, dtype=jnp.float32))

def face_traces(nodal_field, inv_size, derivative):
    values = []
    normals = []
    for direction in range(6):
        axis_index = direction // 2
        layer_index = 5 * (direction % 2)
        orientation = 2.0 * (direction % 2) - 1.0
        slope_row = derivative[layer_index]
        if axis_index == 0:
            face_value = nodal_field[layer_index]
            normal = jnp.einsum('m,mjke->jke', slope_row, nodal_field, precision=HIGHEST)
        elif axis_index == 1:
            face_value = nodal_field[:, layer_index]
            normal = jnp.einsum('m,imke->ike', slope_row, nodal_field, precision=HIGHEST)
        else:
            face_value = nodal_field[:, :, layer_index]
            normal = jnp.einsum('m,ijme->ije', slope_row, nodal_field, precision=HIGHEST)
        values.append(face_value.reshape(36, -1))
        normals.append((normal * (orientation * inv_size)).reshape(36, -1))
    return (jnp.concatenate(values, axis=1), jnp.concatenate(normals, axis=1))

def lift_faces(face_value, face_slope, inv_size, derivative, elem_count):
    result = jnp.zeros((6, 6, 6, elem_count), jnp.float32)
    for direction in range(6):
        axis_index = direction // 2
        layer_index = 5 * (direction % 2)
        orientation = 2.0 * (direction % 2) - 1.0
        slope_row = derivative[layer_index]
        part_value = face_value[:, direction * elem_count:(direction + 1) * elem_count].reshape(6, 6, elem_count)
        part_slope = face_slope[:, direction * elem_count:(direction + 1) * elem_count].reshape(6, 6, elem_count)
        part_slope = part_slope * (orientation * inv_size)
        if axis_index == 0:
            result = result.at[layer_index].add(part_value)
            result = result + jnp.einsum('m,jke->mjke', slope_row, part_slope, precision=HIGHEST)
        elif axis_index == 1:
            result = result.at[:, layer_index].add(part_value)
            result = result + jnp.einsum('m,ike->imke', slope_row, part_slope, precision=HIGHEST)
        else:
            result = result.at[:, :, layer_index].add(part_value)
            result = result + jnp.einsum('m,ije->ijme', slope_row, part_slope, precision=HIGHEST)
    return result

def volume_term(nodal_field, elem_size, weight_cube, derivative):
    cube_scale = weight_cube[:, :, :, None] * elem_size
    grad_x = jnp.einsum('im,mjke->ijke', derivative, nodal_field, precision=HIGHEST) * cube_scale
    grad_y = jnp.einsum('jm,imke->ijke', derivative, nodal_field, precision=HIGHEST) * cube_scale
    grad_z = jnp.einsum('km,ijme->ijke', derivative, nodal_field, precision=HIGHEST) * cube_scale
    result = jnp.einsum('mi,mjke->ijke', derivative, grad_x, precision=HIGHEST)
    result = result + jnp.einsum('mj,imke->ijke', derivative, grad_y, precision=HIGHEST)
    return result + jnp.einsum('mk,ijme->ijke', derivative, grad_z, precision=HIGHEST)

def onto_mortar(face_nodes, rec_sub, halves):
    whole_face = rec_sub >= 4
    first_bit = rec_sub % 2
    second_bit = rec_sub // 2 % 2
    lower_half = jnp.einsum('ij,jkr->ikr', halves[0], face_nodes, precision=HIGHEST)
    upper_half = jnp.einsum('ij,jkr->ikr', halves[1], face_nodes, precision=HIGHEST)
    face_nodes = jnp.where(whole_face, face_nodes, jnp.where(first_bit == 0, lower_half, upper_half))
    lower_half = jnp.einsum('kj,ijr->ikr', halves[0], face_nodes, precision=HIGHEST)
    upper_half = jnp.einsum('kj,ijr->ikr', halves[1], face_nodes, precision=HIGHEST)
    return jnp.where(whole_face, face_nodes, jnp.where(second_bit == 0, lower_half, upper_half))

def off_mortar(face_nodes, rec_sub, halves):
    whole_face = rec_sub >= 4
    first_bit = rec_sub % 2
    second_bit = rec_sub // 2 % 2
    lower_half = jnp.einsum('jk,ijr->ikr', halves[0], face_nodes, precision=HIGHEST)
    upper_half = jnp.einsum('jk,ijr->ikr', halves[1], face_nodes, precision=HIGHEST)
    face_nodes = jnp.where(whole_face, face_nodes, jnp.where(second_bit == 0, lower_half, upper_half))
    lower_half = jnp.einsum('ji,jkr->ikr', halves[0], face_nodes, precision=HIGHEST)
    upper_half = jnp.einsum('ji,jkr->ikr', halves[1], face_nodes, precision=HIGHEST)
    return jnp.where(whole_face, face_nodes, jnp.where(first_bit == 0, lower_half, upper_half))

def mortar_traces(face_value, face_slope, rec_col, rec_sub, halves):
    record_total = rec_col.shape[0]
    value_part = onto_mortar(face_value[:, rec_col].reshape(6, 6, record_total), rec_sub, halves)
    slope_part = onto_mortar(face_slope[:, rec_col].reshape(6, 6, record_total), rec_sub, halves)
    return jnp.concatenate([value_part.reshape(36, record_total), slope_part.reshape(36, record_total)], axis=0)

def mortar_terms(own_traces, partner, is_bound, mortar_size, live_rec, face_weight):
    own_value = own_traces[:36]
    own_slope = own_traces[36:]
    part_value = jnp.where(is_bound, 0.0, partner[:36])
    part_slope = jnp.where(is_bound, -own_slope, partner[36:])
    jump_value = own_value - part_value
    flux_value = 0.5 * (own_slope - part_slope)
    adjoint = jnp.where(is_bound, 1.0, 0.5)
    area_scale = mortar_size * mortar_size
    weight_live = face_weight[:, None] * live_rec
    term_value = weight_live * (PENALTY * mortar_size * jump_value - area_scale * flux_value)
    term_slope = -weight_live * adjoint * area_scale * jump_value
    return (term_value, term_slope)

def scatter_faces(term_value, term_slope, rec_col, rec_sub, halves, column_count):
    record_total = rec_col.shape[0]
    back_value = off_mortar(term_value.reshape(6, 6, record_total), rec_sub, halves).reshape(36, record_total)
    back_slope = off_mortar(term_slope.reshape(6, 6, record_total), rec_sub, halves).reshape(36, record_total)
    face_value = jnp.zeros((36, column_count), jnp.float32).at[:, rec_col].add(back_value)
    face_slope = jnp.zeros((36, column_count), jnp.float32).at[:, rec_col].add(back_slope)
    return (face_value, face_slope)

def reference(rhs, start, spectrum_top, elem_code, rec_elem, rec_dir, rec_sub, rec_peer, rec_index, send_rec):
    weights, derivative, halves, stiff_diag = float_tables()
    elem_total = rhs.shape[1]
    record_total = rec_elem.shape[0]
    elem_dev = elem_total // N_PARTS
    rec_dev = record_total // N_PARTS
    capacity = send_rec.shape[0] // (N_PARTS * N_PARTS)
    owner_device = jnp.arange(record_total, dtype=jnp.int32) // rec_dev
    global_elem = owner_device * elem_dev + rec_elem
    rec_col = rec_dir * elem_total + global_elem
    code_float = elem_code.astype(jnp.float32)
    elem_size = 0.5 * code_float
    inv_size = jnp.where(elem_code > 0, 2.0 / jnp.maximum(code_float, 1.0), 0.0)
    live_elem = elem_code > 0
    own_size = elem_size[global_elem]
    mortar_size = jnp.where(rec_sub < 4, 0.5 * own_size, own_size)
    live_rec = (rec_sub < 5).astype(jnp.float32)
    is_bound = rec_peer < 0
    is_local = rec_peer == owner_device
    is_remote = jnp.logical_and(jnp.logical_not(is_bound), jnp.logical_not(is_local))
    safe_peer = jnp.maximum(rec_peer, 0)
    link_slot = jnp.where(is_remote, (safe_peer * N_PARTS + owner_device) * capacity + rec_index, 0)
    partner_index = jnp.where(is_remote, safe_peer * rec_dev + send_rec[link_slot], safe_peer * rec_dev + rec_index)
    weight_cube = weights[:, None, None] * weights[None, :, None] * weights[None, None, :]
    face_weight = (weights[:, None] * weights[None, :]).reshape(36)
    precond_scale = inv_size[None, :] / stiff_diag[:, None]

    def apply_operator(flat_field):
        nodal_field = flat_field.reshape(6, 6, 6, elem_total)
        face_value, face_slope = face_traces(nodal_field, inv_size, derivative)
        own_traces = mortar_traces(face_value, face_slope, rec_col, rec_sub, halves)
        volume = volume_term(nodal_field, elem_size, weight_cube, derivative)
        partner = own_traces[:, partner_index]
        term_value, term_slope = mortar_terms(own_traces, partner, is_bound, mortar_size, live_rec, face_weight)
        res_value, res_slope = scatter_faces(term_value, term_slope, rec_col, rec_sub, halves, 6 * elem_total)
        lifted = lift_faces(res_value, res_slope, inv_size, derivative, elem_total)
        return (volume + lifted).reshape(216, elem_total)
    scale_total = 216.0 * elem_total

    def residual_of(solution):
        return jnp.where(live_elem[None, :], rhs - apply_operator(solution), 0.0)

    def log_norms(residual, precond):
        total_sums = jnp.stack([jnp.sum(residual * residual), jnp.sum(residual * precond)])
        return 0.5 * jnp.log(total_sums / scale_total)
    top_value = spectrum_top[0]
    bottom = top_value / BOTTOM_RATIO
    center = 0.5 * (top_value + bottom)
    radius = 0.5 * (top_value - bottom)
    sigma_ratio = center / radius
    rho_prev = 1.0 / sigma_ratio
    solution = start
    residual = residual_of(solution)
    precond = precond_scale * residual
    direction = precond / center
    rows_list = [log_norms(residual, precond)]
    for step_index in range(1, ITERS):
        solution = solution + direction
        residual = residual_of(solution)
        precond = precond_scale * residual
        rows_list.append(log_norms(residual, precond))
        rho_next = 1.0 / (2.0 * sigma_ratio - rho_prev)
        direction = rho_next * rho_prev * direction + 2.0 * rho_next / radius * precond
        rho_prev = rho_next
    solution = solution + direction
    return (solution, jnp.stack(rows_list))
```

```python
import functools
import math

import jax
import jax.numpy as jnp
import numpy as np
from jax import lax
from jax.experimental import pallas as pl
from jax.experimental.pallas import tpu as pltpu
from jax.sharding import PartitionSpec as P

LD = 4
ITERS = 3


PENALTY = 36.0
BOTTOM_RATIO = 8.0


def lobatto_tables():
    root_seven = math.sqrt(7.0)
    inner_root = math.sqrt(1.0 / 3.0 - 2.0 * root_seven / 21.0)
    outer_root = math.sqrt(1.0 / 3.0 + 2.0 * root_seven / 21.0)
    points = (np.array([-1.0, -outer_root, -inner_root, inner_root, outer_root, 1.0]) + 1.0) / 2.0
    weights = (
        np.array(
            [
                1.0 / 15.0,
                (14.0 - root_seven) / 30.0,
                (14.0 + root_seven) / 30.0,
                (14.0 + root_seven) / 30.0,
                (14.0 - root_seven) / 30.0,
                1.0 / 15.0,
            ]
        )
        / 2.0
    )
    barycentric = np.array(
        [1.0 / np.prod([points[j] - points[k] for k in range(6) if k != j]) for j in range(6)]
    )
    derivative = np.zeros((6, 6))
    for i in range(6):
        for j in range(6):
            if i != j:
                derivative[i, j] = barycentric[j] / barycentric[i] / (points[i] - points[j])
        derivative[i, i] = -np.sum(derivative[i])
    halves = np.zeros((2, 6, 6))
    for which_half in range(2):
        targets = (points + which_half) / 2.0
        for i in range(6):
            for j in range(6):
                halves[which_half, i, j] = np.prod(
                    [(targets[i] - points[k]) / (points[j] - points[k]) for k in range(6) if k != j]
                )
    column_sums = np.sum(derivative * derivative * weights[:, None], axis=0)
    stiff_diag = (
        column_sums[:, None, None] * weights[None, :, None] * weights[None, None, :]
        + weights[:, None, None] * column_sums[None, :, None] * weights[None, None, :]
        + weights[:, None, None] * weights[None, :, None] * column_sums[None, None, :]
    )
    return (weights, derivative, halves, stiff_diag.reshape(216))


BF16 = jnp.bfloat16
F32 = jnp.float32


def split_np(matrix):
    high = np.asarray(matrix, np.float32).astype(BF16)
    low = (np.asarray(matrix, np.float64) - high.astype(np.float64)).astype(np.float32).astype(BF16)
    return high, low


def operators():
    weights, derivative, halves, stiff_diag = lobatto_tables()
    eye = np.eye(6)
    trace_rows = []
    for direction in range(6):
        axis_index = direction // 2
        layer_index = 5 * (direction % 2)
        orientation = 2.0 * (direction % 2) - 1.0
        for row in (eye[layer_index], orientation * derivative[layer_index]):
            factors = [eye, eye, eye]
            factors[axis_index] = row[None, :]
            trace_rows.append(np.kron(np.kron(factors[0], factors[1]), factors[2]))
    traces = np.concatenate(trace_rows, axis=0)
    stiff_1d = derivative.T @ (weights[:, None] * derivative)
    mass = np.diag(weights)
    stiffness = (
        np.kron(np.kron(stiff_1d, mass), mass)
        + np.kron(np.kron(mass, stiff_1d), mass)
        + np.kron(np.kron(mass, mass), stiff_1d)
    )
    blocks = []
    for sub in range(4):
        quarter = np.kron(halves[sub % 2], halves[sub // 2])
        blocks.append(np.kron(np.eye(2), quarter))
    return traces, stiffness, np.concatenate(blocks, axis=0), np.outer(weights, weights).reshape(36, 1), stiff_diag


def split(value):
    high = value.astype(BF16)
    return high, (value - high.astype(F32)).astype(BF16)


def dot(left, right):
    return jnp.dot(left, right, preferred_element_type=F32)


def dot3(left_high, left_low, right):
    high, low = split(right)
    return dot(left_high, high) + (dot(left_high, low) + dot(left_low, high))


def one_hot(index_row, rows, base=0):
    count = index_row.shape[1]
    position = lax.broadcasted_iota(jnp.int32, (rows, count), 0)
    return jnp.where(position == index_row - base, 1.0, 0.0).astype(BF16)


def pick(traces, elem, direction, sub, onto):
    wide = dot(traces, one_hot(elem, traces.shape[1]))
    face = jnp.zeros((72, elem.shape[1]), F32)
    for d in range(6):
        both = wide[72 * d : 72 * d + 72] + wide[432 + 72 * d : 432 + 72 * d + 72]
        face = jnp.where(direction == d, both, face)
    high, low = split(face)
    quarters = dot(onto, jnp.concatenate([high, low, high], axis=0))
    result = face
    for s in range(4):
        result = jnp.where(sub == s, quarters[72 * s : 72 * s + 72], result)
    return result


def send_kernel(x_ref, inv_ref, code_ref, mat_high, mat_low, onto_ref, out_ref, traces_ref):
    @pl.when(pl.program_id(0) == 0)
    def _():
        raw = dot3(mat_high[...], mat_low[...], x_ref[...])
        row = lax.broadcasted_iota(jnp.int32, raw.shape, 0)
        raw = jnp.where(lax.rem(row, 72) >= 36, raw * inv_ref[...], raw)
        high, low = split(raw)
        traces_ref[0:432] = high
        traces_ref[432:864] = low

    code = code_ref[...]
    picked = pick(traces_ref[...], code[0:1], code[1:2], code[2:3], onto_ref[...])
    capacity = out_ref.shape[2]
    for k in range(out_ref.shape[0]):
        out_ref[k] = picked[:, k * capacity : (k + 1) * capacity]


def exchange_kernel(
    steps, axis, width, src_ref, x_ref, traces_ref, code_ref, onto_ref, stiff_high, stiff_low,
    dst_ref, own_ref, near_ref, volume_ref, send_sem, recv_sem,
):
    count = lax.axis_size(axis)
    me = lax.axis_index(axis)
    barrier = pltpu.get_barrier_semaphore()
    peers = [lax.rem(me + step + count, count) for step in steps]
    for peer in peers:
        pl.semaphore_signal(barrier, inc=1, device_id=(peer,), device_id_type=pl.DeviceIdType.MESH)
    pl.semaphore_wait(barrier, len(steps))
    copies = []
    for k, peer in enumerate(peers):
        copy = pltpu.make_async_remote_copy(
            src_ref=src_ref.at[k],
            dst_ref=dst_ref.at[k],
            send_sem=send_sem.at[k],
            recv_sem=recv_sem.at[k],
            device_id=(peer,),
            device_id_type=pl.DeviceIdType.MESH,
        )
        copy.start()
        copies.append(copy)

    def step_tile(i, carry):
        part = pl.ds(pl.multiple_of(i * width, width), width)
        code = code_ref[:, part]
        own_ref[:, part] = pick(traces_ref[...], code[0:1], code[1:2], code[2:3], onto_ref[...])
        near_ref[:, part] = pick(traces_ref[...], code[3:4], code[4:5], code[5:6], onto_ref[...])
        return carry

    lax.fori_loop(0, code_ref.shape[1] // width, step_tile, 0)
    volume_ref[...] = dot3(stiff_high[...], stiff_low[...], x_ref[...])
    for copy in copies:
        copy.wait()


def norms_kernel(axis, sums_ref, out_ref, landing, send_sem, recv_sem):
    count = lax.axis_size(axis)
    me = lax.axis_index(axis)
    barrier = pltpu.get_barrier_semaphore()

    def greet(k, carry):
        peer = lax.rem(me + k, count)
        pl.semaphore_signal(barrier, inc=1, device_id=(peer,), device_id_type=pl.DeviceIdType.MESH)
        return carry

    def copy_to(k):
        return pltpu.make_async_remote_copy(
            src_ref=sums_ref,
            dst_ref=landing.at[k],
            send_sem=send_sem.at[k],
            recv_sem=recv_sem.at[k],
            device_id=(lax.rem(me + k, count),),
            device_id_type=pl.DeviceIdType.MESH,
        )

    def start(k, carry):
        copy_to(k).start()
        return carry

    def finish(k, carry):
        copy_to(k).wait()
        return carry

    lax.fori_loop(1, count, greet, 0)
    pl.semaphore_wait(barrier, count - 1)
    lax.fori_loop(1, count, start, 0)
    landing[0] = sums_ref[...]
    lax.fori_loop(1, count, finish, 0)

    def add(j, total):
        return total + landing[lax.rem(me + count - j, count)]

    total = lax.fori_loop(0, count, add, jnp.zeros(out_ref.shape, F32))
    out_ref[...] = jnp.broadcast_to(jnp.sum(total, axis=1, keepdims=True), out_ref.shape)


def apply_kernel(
    row_ref, coef_ref, x_ref, dirn_ref, rhs_ref, elem_ref, prec_ref, recv_ref, own_ref, near_ref,
    volume_ref, code_ref, rows_ref, size_ref, off_ref, weight_ref, lift_high, lift_low, prior_ref,
    x_out, dirn_out, sums_out, pool, total,
):
    peer_count = recv_ref.shape[0]

    @pl.when(pl.program_id(0) == 0)
    def _():
        for k in range(peer_count):
            high, low = split(recv_ref[k])
            pool[144 * k : 144 * k + 72] = high
            pool[144 * k + 72 : 144 * k + 144] = low
        total[...] = jnp.zeros_like(total)

    code = code_ref[...]
    direction, sub = code[1:2], code[2:3]
    bound = code[6:7] == -1
    width = sub.shape[1]
    own = own_ref[...]
    wide = dot(pool[...], one_hot(code[7:8], pool.shape[1]))
    partner = near_ref[...]
    for k in range(peer_count):
        both = wide[144 * k : 144 * k + 72] + wide[144 * k + 72 : 144 * k + 144]
        partner = jnp.where(code[6:7] == k, both, partner)
    own_value, own_slope = own[0:36], own[36:72]
    part_value = jnp.where(bound, 0.0, partner[0:36])
    part_slope = jnp.where(bound, -own_slope, partner[36:72])
    jump = own_value - part_value
    flux = 0.5 * (own_slope - part_slope)
    mortar = size_ref[0:1]
    area = mortar * mortar
    weight = weight_ref[...] * size_ref[1:2]
    term_value = weight * (PENALTY * mortar * jump - area * flux)
    term_slope = -weight * (jnp.where(bound, 1.0, 0.5) * area) * jump
    terms = jnp.concatenate([term_value, term_slope], axis=0)
    spread = jnp.concatenate([jnp.where(sub == s, terms, 0.0) for s in range(4)], axis=0)
    spread_high, spread_low = split(spread)
    back = dot(off_ref[...], jnp.concatenate([spread_high, spread_low, spread_high], axis=0))
    back = jnp.where(sub >= 4, terms, back)
    spread = jnp.concatenate([jnp.where(direction == d, back, 0.0) for d in range(6)], axis=0)
    wide_high, wide_low = split(spread)
    lanes = lax.broadcasted_iota(jnp.int32, (width, total.shape[1]), 1)
    hot = jnp.where(lanes == rows_ref[...], 1.0, 0.0).astype(BF16)
    total[...] += dot(wide_high, hot) + dot(wide_low, hot)

    @pl.when(pl.program_id(0) == pl.num_programs(0) - 1)
    def _():
        size, inv = elem_ref[0:1], elem_ref[1:2]
        field = x_ref[...]
        row = lax.broadcasted_iota(jnp.int32, total.shape, 0)
        faces = jnp.where(lax.rem(row, 72) >= 36, total[...] * inv, total[...])
        applied = size * volume_ref[...]
        applied = applied + dot3(lift_high[...], lift_low[...], faces)
        residual = jnp.where(size > 0.0, rhs_ref[...] - applied, 0.0)
        scaled = residual * (inv * prec_ref[...])
        step = coef_ref[0] * dirn_ref[...] + coef_ref[1] * scaled
        dirn_out[...] = step
        x_out[...] = field + step
        squares = jnp.sum(residual * residual, axis=0, keepdims=True)
        products = jnp.sum(residual * scaled, axis=0, keepdims=True)
        fold = lambda line: sum(line[:, k : k + 128] for k in range(0, line.shape[1], 128))
        row = lax.broadcasted_iota(jnp.int32, sums_out.shape, 0)
        row_index = row_ref[0]
        later = jnp.where(row == 2 * row_index + 1, fold(products), prior_ref[...])
        sums_out[...] = jnp.where(row == 2 * row_index, fold(squares), later)


def take_small(tables, index):
    rows = tables.shape[1] // 128
    fine = (jnp.arange(128, dtype=jnp.int32)[:, None] == (index % 128)[None, :]).astype(BF16)
    wide = jnp.dot(tables.reshape(-1, 128).astype(BF16), fine, preferred_element_type=F32)
    wide = wide.reshape(tables.shape[0], rows, -1)
    coarse = jnp.arange(rows, dtype=jnp.int32)[:, None] == (index // 128)[None, :]
    return jnp.sum(jnp.where(coarse[None], wide, 0.0), axis=1).astype(jnp.int32)


def tile(count):
    for width in (512, 256, 128):
        if count % width == 0:
            return width
    return count


def whole(shape):
    return pl.BlockSpec(shape, lambda i: (0,) * len(shape))


def general_path(
    rhs, start, spectrum_top, elem_code, rec_elem, rec_dir, rec_sub, rec_peer, rec_index, send_rec
):
    traces, stiffness, interp, face_weight, stiff_diag = operators()
    part_count = lax.axis_size("parts")
    own_index = lax.axis_index("parts")
    elem_count = rhs.shape[1]
    record_count = rec_elem.shape[0]
    capacity = send_rec.shape[0] // part_count
    far_reach = 2 * LD - 1
    code_float = elem_code.astype(F32)
    elem_size = 0.5 * code_float
    inv_size = jnp.where(elem_code > 0, 2.0 / jnp.maximum(code_float, 1.0), 0.0)
    elem_rows = jnp.stack([elem_size, inv_size])
    is_bound = rec_peer < 0
    is_local = rec_peer == own_index
    is_remote = jnp.logical_and(jnp.logical_not(is_bound), jnp.logical_not(is_local))
    offset = own_index - rec_peer
    position = jnp.where(offset < 0, offset + far_reach, offset + far_reach - 1)
    block = jnp.where(is_remote, position, jnp.where(is_bound, -1, -2))
    steps = list(range(-far_reach, 0)) + list(range(1, far_reach + 1))
    lists = send_rec.reshape(part_count, capacity)
    lists = jnp.concatenate([lists[part_count - far_reach :], lists, lists[:far_reach]], axis=0)
    lists = lax.dynamic_slice_in_dim(lists, own_index, 2 * far_reach + 1, 0)
    send_cols = jnp.concatenate([lists[:far_reach], lists[far_reach + 1 :]], axis=0).reshape(-1)
    send_count = send_cols.shape[0]

    own_size = 0.5 * take_small(elem_code[None], rec_elem)[0].astype(F32)
    mortar_size = jnp.where(rec_sub < 4, 0.5 * own_size, own_size)
    size_rows = jnp.stack([mortar_size, (rec_sub < 5).astype(F32)])
    tables = jnp.stack([rec_elem // 256, rec_elem % 256, rec_dir * 8 + rec_sub])
    found = take_small(tables, jnp.concatenate([send_cols, rec_index]))
    found = jnp.stack([found[0] * 256 + found[1], found[2] // 8, found[2] % 8])
    send_code = found[:, :send_count]
    near = jnp.where(is_local[None], found[:, send_count:], -1)
    rec_code = jnp.concatenate(
        [jnp.stack([rec_elem, rec_dir, rec_sub]), near, block[None], rec_index[None]],
        axis=0,
    )
    rec_rows = rec_elem[:, None]

    mat_high, mat_low = split_np(traces)
    lift_high, lift_low = split_np(traces.T)
    stiff_high, stiff_low = split_np(stiffness)
    onto_high, onto_low = split_np(interp)
    onto = np.concatenate([onto_high, onto_high, onto_low], axis=1)
    flat = np.concatenate([interp[72 * s : 72 * s + 72].T for s in range(4)], axis=1)
    off_high, off_low = split_np(flat)
    off = np.concatenate([off_high, off_high, off_low], axis=1)
    prec = jnp.asarray((1.0 / stiff_diag).reshape(216, 1), F32)
    weight = jnp.asarray(face_weight, F32)

    send_tile, rec_tile, peer_count = 2 * capacity, tile(record_count), len(steps)
    params = pltpu.CompilerParams(vmem_limit_bytes=60 * 1024 * 1024)
    field = (216, elem_count)

    def send_call(x):
        return pl.pallas_call(
            send_kernel,
            grid=(send_count // send_tile,),
            in_specs=[
                whole(field),
                whole((1, elem_count)),
                pl.BlockSpec((3, send_tile), lambda i: (0, i)),
                whole((432, 216)),
                whole((432, 216)),
                whole((288, 216)),
            ],
            out_specs=[pl.BlockSpec((2, 72, capacity), lambda i: (i, 0, 0)), whole((864, elem_count))],
            out_shape=[
                jax.ShapeDtypeStruct((peer_count, 72, capacity), F32),
                jax.ShapeDtypeStruct((864, elem_count), BF16),
            ],
            compiler_params=params,
            name="send_traces",
        )(x, inv_size[None], send_code, jnp.asarray(mat_high), jnp.asarray(mat_low), jnp.asarray(onto))

    vmem = pl.BlockSpec(memory_space=pltpu.VMEM)

    def exchange(outgoing, x, element_traces):
        return pl.pallas_call(
            functools.partial(exchange_kernel, steps, "parts", rec_tile),
            in_specs=[pl.BlockSpec(memory_space=pl.ANY)] + [vmem] * 6,
            out_specs=[pl.BlockSpec(memory_space=pl.ANY)] + [vmem] * 3,
            out_shape=[
                jax.ShapeDtypeStruct((peer_count, 72, capacity), F32),
                jax.ShapeDtypeStruct((72, record_count), F32),
                jax.ShapeDtypeStruct((72, record_count), F32),
                jax.ShapeDtypeStruct(field, F32),
            ],
            scratch_shapes=[
                pltpu.SemaphoreType.DMA((peer_count,)),
                pltpu.SemaphoreType.DMA((peer_count,)),
            ],
            compiler_params=pltpu.CompilerParams(
                collective_id=0, has_side_effects=True, vmem_limit_bytes=60 * 1024 * 1024
            ),
            name="exchange",
        )(
            outgoing, x, element_traces, rec_code, jnp.asarray(onto),
            jnp.asarray(stiff_high), jnp.asarray(stiff_low),
        )

    def all_sums(sums):
        return pl.pallas_call(
            functools.partial(norms_kernel, "parts"),
            in_specs=[vmem],
            out_specs=vmem,
            out_shape=jax.ShapeDtypeStruct((8, 128), F32),
            scratch_shapes=[
                pltpu.VMEM((part_count, 8, 128), F32),
                pltpu.SemaphoreType.DMA((part_count,)),
                pltpu.SemaphoreType.DMA((part_count,)),
            ],
            compiler_params=pltpu.CompilerParams(collective_id=1, has_side_effects=True),
            name="all_sums",
        )(sums)

    def apply_call(row_index, coef, x, dirn, received, own, near_traces, volume, sums):
        tiles = lambda rows: pl.BlockSpec((rows, rec_tile), lambda i: (0, i))
        return pl.pallas_call(
            apply_kernel,
            grid=(record_count // rec_tile,),
            in_specs=[
                pl.BlockSpec(memory_space=pltpu.SMEM),
                pl.BlockSpec(memory_space=pltpu.SMEM),
                whole(field),
                whole(field),
                whole(field),
                whole((2, elem_count)),
                whole((216, 1)),
                whole((peer_count, 72, capacity)),
                tiles(72),
                tiles(72),
                whole(field),
                tiles(8),
                pl.BlockSpec((rec_tile, 1), lambda i: (i, 0)),
                tiles(2),
                whole((72, 864)),
                whole((36, 1)),
                whole((216, 432)),
                whole((216, 432)),
                whole((8, 128)),
            ],
            out_specs=[whole(field), whole(field), whole((8, 128))],
            out_shape=[
                jax.ShapeDtypeStruct(field, F32),
                jax.ShapeDtypeStruct(field, F32),
                jax.ShapeDtypeStruct((8, 128), F32),
            ],
            scratch_shapes=[
                pltpu.VMEM((144 * peer_count, capacity), BF16),
                pltpu.VMEM((432, elem_count), F32),
            ],
            compiler_params=params,
            name="apply_operator",
        )(
            row_index[None], coef, x, dirn, rhs, elem_rows, prec, received, own, near_traces, volume, rec_code, rec_rows,
            size_rows, jnp.asarray(off), weight, jnp.asarray(lift_high), jnp.asarray(lift_low), sums,
        )

    scale_total = 216.0 * elem_count * part_count
    top_value = spectrum_top[0]
    bottom = top_value / BOTTOM_RATIO
    center = 0.5 * (top_value + bottom)
    radius = 0.5 * (top_value - bottom)
    sigma_ratio = center / radius
    rho_prev = 1.0 / sigma_ratio
    coefs = [jnp.stack([jnp.zeros_like(center), 1.0 / center])]
    for step_index in range(1, ITERS):
        rho_next = 1.0 / (2.0 * sigma_ratio - rho_prev)
        coefs.append(jnp.stack([rho_next * rho_prev, 2.0 * rho_next / radius]))
        rho_prev = rho_next
    coefs = jnp.stack(coefs)

    def one_step(step_index, state):
        x, dirn, sums = state
        outgoing, element_traces = send_call(x)
        moved = exchange(outgoing, x, element_traces)
        coef = lax.dynamic_index_in_dim(coefs, step_index, 0, False)
        return tuple(apply_call(step_index, coef, x, dirn, *moved, sums))

    x, dirn, sums = lax.fori_loop(0, ITERS, one_step, (start, start, jnp.zeros((8, 128), F32)))
    norms = 0.5 * jnp.log(all_sums(sums)[: 2 * ITERS, 0].reshape(ITERS, 2) / scale_total)
    return (x, norms)


LATERAL = 128
FIELDS = 9


def iota(shape, axis):
    return lax.broadcasted_iota(jnp.int32, shape, axis)


def sum_rows(value):
    return jnp.sum(value, axis=0, keepdims=True)


def total_of(value):
    return jnp.sum(value, axis=1, keepdims=True)


def look_up(tables, rows, index):
    hot = jnp.where(iota((128, index.shape[1]), 0) == (index & 127), 1.0, 0.0).astype(BF16)
    wide = dot(tables, hot)
    mask = iota((rows, index.shape[1]), 0) == (index >> 7)
    count = tables.shape[0] // rows
    return [sum_rows(jnp.where(mask, wide[k * rows : (k + 1) * rows], 0.0)) for k in range(count)]


def regroup(columns, position, rows):
    mask = iota((rows, position.shape[1]), 0) == (position >> 7)
    left = jnp.concatenate([jnp.where(mask, column, 0.0) for column in columns], axis=0).astype(BF16)
    hot = jnp.where(iota((128, position.shape[1]), 0) == (position & 127), 1.0, 0.0).astype(BF16)
    return lax.dot_general(left, hot, (((1,), (1,)), ((), ())), preferred_element_type=F32)


def setup_kernel(
    axis, capacity, code_ref, elem_ref, dir_ref, sub_ref, peer_ref, index_ref,
    code_line, elem_line, dir_line, sub_line, peer_line, index_line, lists_ref,
    rows_ref, col_ref, send_ref, flag_ref, elem_out,
):
    me = lax.axis_index(axis)
    count = lax.axis_size(axis)
    group, place = me // LD, lax.rem(me, LD)
    elem, direction, sub = elem_line[...], dir_line[...], sub_line[...]
    peer, index = peer_line[...], index_line[...]
    records, slots = elem.shape[1], code_line.shape[1]
    chunks, table_rows, slot_rows = records // 128, records // 128, 6 * slots // 128
    used = sub < 5
    local = used & (peer == me)
    bound = used & (peer < 0)
    remote = used & (peer >= 0) & (peer != me)

    kind = jnp.where(used, jnp.where(remote, direction, direction + 8), -1)
    member = jnp.where(iota((16, records), 0) == kind, 1.0, 0.0)
    stacked = jnp.concatenate([member[:, 128 * k : 128 * k + 128] for k in range(chunks)], axis=0)
    upper = jnp.where(iota((128, 128), 0) < iota((128, 128), 1), 1.0, 0.0)
    counted = dot(
        stacked.astype(BF16), jnp.concatenate([upper, jnp.ones((128, 128), F32)], axis=1).astype(BF16)
    )
    carry = jnp.zeros((16, 128), F32)
    before = []
    for k in range(chunks):
        before.append(counted[16 * k : 16 * k + 16, :128] + carry)
        carry = carry + counted[16 * k : 16 * k + 16, 128:]
    base = jnp.concatenate([jnp.zeros((8, 128), F32), carry[:8]], axis=0)
    before = jnp.concatenate([part + base for part in before], axis=1)
    rank = sum_rows(before * member).astype(jnp.int32)
    in_range = used & (rank < slots)
    slot = jnp.where(in_range, direction * slots + rank, -1)

    tables = jnp.concatenate(
        [
            (elem_ref[...] & 127).astype(F32),
            ((elem_ref[...] >> 7) * 8 + sub_ref[...]).astype(F32),
            dir_ref[...].astype(F32),
        ],
        axis=0,
    ).astype(BF16)
    rows_per = capacity // 128
    list_rows = iota(lists_ref.shape, 0)
    lists = lists_ref[...].astype(F32)
    channel = []
    for d, other in ((1, group + 1), (0, group - 1)):
        here = remote & (direction == d)
        most = jnp.max(jnp.where(here, peer, -1), axis=1, keepdims=True)
        least = jnp.min(jnp.where(here, peer, count), axis=1, keepdims=True)
        wrong = here & (peer // LD != other)
        channel.append((most, jnp.where((most >= 0) & (most != least), 1.0, 0.0), wrong))
    wanted = []
    for most, _, _ in channel:
        for part in range(rows_per):
            wanted.append(sum_rows(jnp.where(list_rows == most * rows_per + part, lists, 0.0)))
    for pos in range(LD - 1):
        dest = group * LD + lax.rem(place + pos + 1, LD)
        wanted.append(sum_rows(jnp.where(list_rows == dest * rows_per, lists, 0.0)))
    wanted.append(jnp.zeros((1, LATERAL), F32))
    wanted = jnp.concatenate(wanted, axis=1).astype(jnp.int32)
    wanted_count = wanted.shape[1]
    low, high, found_dir = look_up(tables, table_rows, jnp.concatenate([wanted, index], axis=1))
    high = high.astype(jnp.int32)
    found_elem = low.astype(jnp.int32) + 128 * (high >> 3)
    found_sub = high & 7
    send_ref[0:1] = found_elem[:, :wanted_count]
    send_ref[1:2] = found_dir[:, :wanted_count].astype(jnp.int32)
    send_ref[2:3] = found_sub[:, :wanted_count]
    send_ref[3:8] = jnp.zeros((5, wanted_count), jnp.int32)
    near_elem, near_sub = found_elem[:, wanted_count:], found_sub[:, wanted_count:]

    code_rows = -(-slots // 1024) * 8
    code_table = code_ref[...].astype(F32)
    if code_rows > code_table.shape[0]:
        pad = jnp.zeros((code_rows - code_table.shape[0], 128), F32)
        code_table = jnp.concatenate([code_table, pad], axis=0)
    code = look_up(code_table.astype(BF16), code_rows, elem)[0]
    size = 0.5 * code
    mortar = jnp.where(sub < 4, 0.5 * size, size)

    turn = lax.rem(place - lax.rem(peer, LD) + LD, LD) - 1
    landed = jnp.where(direction < 2, index, turn * LATERAL + index)
    split_near = jnp.where(sub < 4, sub, jnp.where(near_sub < 4, near_sub + 4, 8))
    split_far = jnp.minimum(sub, 4)
    real = lambda value: value.astype(F32)
    columns = [
        real(elem & 127),
        real((elem >> 7) + 1),
        real(near_elem & 127),
        jnp.where(local, real((near_elem >> 7) + 1), 0.0),
        jnp.where(remote, real(landed & 127), 0.0),
        jnp.where(remote, real((landed >> 7) + 1), 0.0),
        real(split_near),
        real(split_far),
        mortar,
    ]
    moved = regroup(columns, slot, slot_rows)
    part = lambda k: moved[k * slot_rows : (k + 1) * slot_rows]
    join = lambda k: jnp.where(part(k + 1) > 0.0, part(k) + 128.0 * (part(k + 1) - 1.0), -1.0)
    own = join(0)
    spare = col_ref.shape[1] - slot_rows
    own_all = jnp.concatenate([own, jnp.zeros((spare, 128), F32)], axis=0)
    col_ref[...] = jnp.transpose(own_all).astype(jnp.int32)
    mort = part(8)
    fields = [join(2), join(4), part(6), part(7), 36.0 * mort, 0.5 * mort * mort]

    face = jnp.where(used, direction * slots + elem, -1)
    marks = [jnp.where(used & (sub == s), 1.0, 0.0) for s in range(5)]
    marks.append(jnp.where(bound & (sub == 4), 1.0, 0.0))
    tally = regroup(marks, face, slot_rows)
    fields += [tally[k * slot_rows : (k + 1) * slot_rows] for k in range(6)]
    per = slots // 128
    lines = []
    for value in fields:
        pieces = []
        for d in range(6):
            pieces.append(
                jnp.concatenate([value[per * d + q : per * d + q + 1] for q in range(per)], axis=1)
            )
        pieces.append(jnp.zeros((2, slots), F32))
        lines.append(jnp.concatenate(pieces, axis=0))
    code_all = code_line[...].astype(F32)
    size_all = 0.5 * code_all
    inv_all = jnp.where(code_all > 0.0, 2.0 / jnp.maximum(code_all, 1.0), 0.0)
    elem_out[0:1] = size_all
    elem_out[1:2] = inv_all
    elem_out[2:8] = jnp.zeros((6, slots), F32)
    half = 0.5 * size_all
    counts, bounds = lines[6:11], lines[11]
    lines = lines[:6]
    for s in range(5):
        lines.append(36.0 * (half if s < 4 else size_all) * counts[s])
    for s in range(4):
        lines.append(half * half * (0.5 * counts[s]))
    lines.append(size_all * size_all * (0.5 * (counts[4] + bounds)))
    for k, line in enumerate(lines):
        rows_ref[8 * k : 8 * k + 8] = line
    rows_ref[8 * len(lines) :] = jnp.zeros((rows_ref.shape[0] - 8 * len(lines), slots), F32)

    wrong = jnp.where(remote & (direction >= 2) & ((peer // LD != group) | (index >= LATERAL)), 1.0, 0.0)
    wrong = wrong + jnp.where(bound & (sub < 4), 1.0, 0.0)
    wrong = wrong + jnp.where(local & (sub < 4) & (near_sub < 4), 1.0, 0.0)
    wrong = wrong + jnp.where(used & (rank >= slots), 1.0, 0.0)
    for _, _, off in channel:
        wrong = wrong + jnp.where(off, 1.0, 0.0)
    faults = total_of(wrong) + channel[0][1] + channel[1][1]
    row = iota((8, 128), 0)
    allowed = jnp.where(row < 2, float(capacity), float(LATERAL))
    over = jnp.where((row < 6) & (carry[:8] > allowed), 1.0, 0.0)
    faults = faults + total_of(sum_rows(over))
    turns = [
        lax.rem(place - lax.rem(jnp.maximum(most, 0), LD) + LD, LD).astype(F32) for most, _, _ in channel
    ]
    flags = jnp.where(row == 0, faults, jnp.where(row == 1, turns[1], turns[0]))
    flag_ref[...] = flags


def stack2(value):
    high = value.astype(BF16).astype(F32)
    return jnp.concatenate([high, value - high], axis=0).astype(BF16)


def stack3(value):
    high = value.astype(BF16).astype(F32)
    return jnp.concatenate([high, value - high, high], axis=0).astype(BF16)


def fold_pair(value):
    half = value.shape[0] // 2
    return value[:half] + value[half:]


def choose(blocks, rows, code):
    last = blocks.shape[0] // rows - 1
    result = blocks[last * rows :]
    for q in range(last):
        result = jnp.where(code == q, blocks[q * rows : q * rows + rows], result)
    return result


def main_kernel(
    axis, iters, capacity,
    x_ref, rhs_ref, top_ref, rows_ref, col_ref, send_ref, flag_ref, elem_ref, prec_ref,
    trace_high, trace_low, stiff_high, stiff_low, lift_high, lift_low, onto_ref, own_ref, near_ref, far_ref,
    x_out, norm_out,
    dirn, volume, traces, pairs, faces, scatter, gather, gather_chan, gather_lat, send_chan, send_lat,
    far_rows, coefs, snd_chan, snd_lat, rcv_chan, rcv_lat, sums, landing,
    send_sem, recv_sem, sum_send, sum_recv,
):
    count = lax.axis_size(axis)
    me = lax.axis_index(axis)
    group, place = me // LD, lax.rem(me, LD)
    groups = count // LD
    slots = x_ref.shape[1]
    mesh_id = pl.DeviceIdType.MESH
    barrier = pltpu.get_barrier_semaphore()

    def greet(k, carry):
        peer = lax.rem(me + k, count)
        pl.semaphore_signal(barrier, inc=1, device_id=(peer,), device_id_type=mesh_id)
        return carry

    lax.fori_loop(1, count, greet, 0)

    def hot(mask):
        return jnp.where(mask, 1.0, 0.0).astype(BF16)

    per = slots // 128
    columns = col_ref[...]
    for d in range(6):
        line = rows_ref[d : d + 1].astype(jnp.int32)
        gather[d] = hot(iota((slots, slots), 0) == line)
        for q in range(per):
            column = columns[:, per * d + q : per * d + q + 1]
            scatter[d, 128 * q : 128 * q + 128] = hot(iota((128, slots), 1) == column)
        line = rows_ref[8 + d : 9 + d].astype(jnp.int32)
        if d < 2:
            gather_chan[d] = hot(iota((capacity, capacity), 0) == line[:, :capacity])
        else:
            gather_lat[d - 2] = hot(iota((LD * LATERAL, LATERAL), 0) == line[:, :LATERAL])
    send_elem = send_ref[0:1]
    send_chan[0] = hot(iota((slots, capacity), 0) == send_elem[:, :capacity])
    send_chan[1] = hot(iota((slots, capacity), 0) == send_elem[:, capacity : 2 * capacity])
    send_lat[...] = hot(iota((slots, LD * LATERAL), 0) == send_elem[:, 2 * capacity :])
    chosen = jnp.zeros(far_rows.shape, F32)
    for k, field in enumerate((3, 4, 5)):
        block = rows_ref[8 * field : 8 * field + 8]
        pieces = []
        for d in range(6):
            part = block[:, : capacity if d < 2 else LATERAL]
            pieces.append(sum_rows(jnp.where(iota(part.shape, 0) == d, part, 0.0)))
        chosen = jnp.where(iota(chosen.shape, 0) == k, jnp.concatenate(pieces, axis=1), chosen)
    far_rows[...] = chosen

    line = jnp.ones((1, 128), F32)
    top = top_ref[0] * line
    bottom = top / BOTTOM_RATIO
    center = 0.5 * (top + bottom)
    radius = 0.5 * (top - bottom)
    sigma = center / radius
    rho = 1.0 / sigma
    coefs[0:1] = 0.0 * line
    coefs[1:2] = 1.0 / center
    for k in range(1, iters):
        rho_next = 1.0 / (2.0 * sigma - rho)
        coefs[2 * k : 2 * k + 1] = rho_next * rho
        coefs[2 * k + 1 : 2 * k + 2] = 2.0 * rho_next / radius
        rho = rho_next
    x_out[...] = x_ref[...]
    dirn[...] = jnp.zeros_like(dirn)
    sums[...] = jnp.where(iota(sums.shape, 0) == 2 * iters, flag_ref[0:1], 0.0) * jnp.where(
        iota(sums.shape, 1) == 0, 1.0, 0.0
    )

    size, inv = elem_ref[0:1], elem_ref[1:2]
    pl.semaphore_wait(barrier, count - 1)

    def step(it, carry):
        field = x_out[...]
        raw = dot3(trace_high[...], trace_low[...], field)
        raw = jnp.where(lax.rem(iota(raw.shape, 0), 72) >= 36, raw * inv, raw)
        traces[...] = raw
        for d in range(6):
            pairs[d] = stack2(raw[72 * d : 72 * d + 72])

        send_dir = send_ref[1:2, 2 * capacity :]
        lateral = jnp.zeros((72, LD * LATERAL), F32)
        for d in range(2, 6):
            lateral = jnp.where(send_dir == d, fold_pair(dot(pairs[d], send_lat[...])), lateral)
        outgoing = jnp.concatenate(
            [fold_pair(dot(pairs[1], send_chan[0])), fold_pair(dot(pairs[0], send_chan[1])), lateral], axis=1
        )
        outgoing = choose(dot(onto_ref[...], stack3(outgoing)), 72, send_ref[2:3])
        snd_chan[0] = outgoing[:, :capacity]
        snd_chan[1] = outgoing[:, capacity : 2 * capacity]
        for pos in range(LD - 1):
            start = 2 * capacity + pos * LATERAL
            snd_lat[pos] = outgoing[:, start : start + LATERAL]

        copies = []
        for side in range(2):
            other = lax.rem(group + (1 if side == 0 else groups - 1), groups)
            for turn in range(LD):
                k = side * LD + turn
                copies.append(
                    pltpu.make_async_remote_copy(
                        src_ref=snd_chan.at[side],
                        dst_ref=rcv_chan.at[it, side, turn],
                        send_sem=send_sem.at[it, k],
                        recv_sem=recv_sem.at[it, k],
                        device_id=(other * LD + lax.rem(place + turn, LD),),
                        device_id_type=mesh_id,
                    )
                )
        for pos in range(LD - 1):
            k = 2 * LD + pos
            copies.append(
                pltpu.make_async_remote_copy(
                    src_ref=snd_lat.at[pos],
                    dst_ref=rcv_lat.at[it, pos],
                    send_sem=send_sem.at[it, k],
                    recv_sem=recv_sem.at[it, k],
                    device_id=(group * LD + lax.rem(place + pos + 1, LD),),
                    device_id_type=mesh_id,
                )
            )
        for copy in copies:
            copy.start()

        volume[...] = dot3(stiff_high[...], stiff_low[...], field) * size

        def local_faces(d, inner):
            line = lambda k: rows_ref[pl.ds(8 * k + d, 1)]
            mass = dot(own_ref[...], stack3(traces[pl.ds(pl.multiple_of(72 * d, 8), 72)]))
            value = jnp.zeros((40, slots), F32)
            slope = jnp.zeros((40, slots), F32)
            for s in range(5):
                mass_value, mass_slope = mass[80 * s : 80 * s + 40], mass[80 * s + 40 : 80 * s + 80]
                flux = line(11 + s)
                value = value + (line(6 + s) * mass_value - flux * mass_slope)
                slope = slope - flux * mass_value
            facing = d + 1 - 2 * lax.rem(d, 2)
            found = fold_pair(dot(pairs[facing], gather[d]))
            found = choose(dot(near_ref[...], stack3(found)), 80, line(2).astype(jnp.int32))
            jump, flux = line(4), line(5)
            terms = jnp.concatenate([flux * found[40:] - jump * found[:40], flux * found[:40]], axis=0)
            back = fold_pair(dot(stack2(terms), scatter[d]))
            faces[pl.ds(pl.multiple_of(80 * d, 8), 80)] = back + jnp.concatenate([value, slope], axis=0)
            return inner

        lax.fori_loop(0, 6, local_faces, 0)
        for copy in copies:
            copy.wait()

        pieces = []
        for side in range(2):
            turn = flag_ref[side + 1 : side + 2, 0:1]
            got = rcv_chan[it, side, 0]
            for k in range(1, LD):
                got = jnp.where(turn == float(k), rcv_chan[it, side, k], got)
            pieces.append(fold_pair(dot(stack2(got), gather_chan[side])))
        sides = [rcv_lat[it, pos] for pos in range(LD - 1)] + [jnp.zeros((72, LATERAL), F32)]
        got = stack2(jnp.concatenate(sides, axis=1))
        for d in range(4):
            pieces.append(fold_pair(dot(got, gather_lat[d])))
        found = jnp.concatenate(pieces, axis=1)
        found = choose(dot(far_ref[...], stack3(found)), 80, far_rows[0:1].astype(jnp.int32))
        jump, flux = far_rows[1:2], far_rows[2:3]
        terms = stack2(
            jnp.concatenate([flux * found[40:] - jump * found[:40], flux * found[:40]], axis=0)
        )
        for d in range(6):
            width = capacity if d < 2 else LATERAL
            start = d * capacity if d < 2 else 2 * capacity + (d - 2) * LATERAL
            faces[80 * d : 80 * d + 80] += fold_pair(
                dot(terms[:, start : start + width], scatter[d, :width])
            )
        total = faces[...]
        total = jnp.where(lax.rem(iota(total.shape, 0), 80) >= 40, total * inv, total)
        applied = volume[...] + dot3(lift_high[...], lift_low[...], total)
        residual = jnp.where(size > 0.0, rhs_ref[...] - applied, 0.0)
        scaled = residual * (inv * prec_ref[...])
        first = coefs[pl.ds(2 * it, 1), 0:1]
        second = coefs[pl.ds(2 * it + 1, 1), 0:1]
        change = first * dirn[...] + second * scaled
        dirn[...] = change
        x_out[...] = field + change
        squares = sum_rows(residual * residual)
        products = sum_rows(residual * scaled)
        fold = lambda row: sum(row[:, k : k + 128] for k in range(0, row.shape[1], 128))
        row = iota(sums.shape, 0)
        kept = jnp.where(row == 2 * it + 1, fold(products), sums[...])
        sums[...] = jnp.where(row == 2 * it, fold(squares), kept)
        return carry

    lax.fori_loop(0, iters, step, 0)

    def copy_to(k):
        return pltpu.make_async_remote_copy(
            src_ref=sums,
            dst_ref=landing.at[k],
            send_sem=sum_send.at[k],
            recv_sem=sum_recv.at[k],
            device_id=(lax.rem(me + k, count),),
            device_id_type=mesh_id,
        )

    def begin(k, carry):
        copy_to(k).start()
        return carry

    def finish(k, carry):
        copy_to(k).wait()
        return carry

    def add(j, total):
        return total + landing[lax.rem(me + count - j, count)]

    lax.fori_loop(1, count, begin, 0)
    landing[0] = sums[...]
    lax.fori_loop(1, count, finish, 0)
    total = total_of(lax.fori_loop(0, count, add, jnp.zeros(sums.shape, F32)))
    mean = total / (216.0 * slots * count)
    logs = 0.5 * jnp.log(jnp.where(iota(total.shape, 0) < 2 * iters, mean, 1.0))
    shown = jnp.where(iota(total.shape, 0) < 2 * iters, logs, total)
    norm_out[...] = jnp.broadcast_to(shown, norm_out.shape)


def wide_rows(blocks):
    padded = []
    for block in blocks:
        rows = np.zeros((80, block.shape[1]))
        rows[0:36], rows[40:76] = block[0:36], block[36:72]
        padded.append(rows)
    return np.concatenate(padded, axis=0)


def three(matrix):
    high, low = split_np(matrix)
    return np.concatenate([high, high, low], axis=1)


def set_up(slots, capacity, arrays, send_rec):
    slot_rows = 6 * slots // 128
    to_lines = lambda array: array.reshape(-1, 128)
    to_line = lambda array: array.reshape(1, -1)
    vmem = pl.BlockSpec(memory_space=pltpu.VMEM)
    columns = 2 * capacity + LD * LATERAL
    return pl.pallas_call(
        functools.partial(setup_kernel, "parts", capacity),
        in_specs=[vmem] * 13,
        out_specs=[vmem] * 5,
        out_shape=[
            jax.ShapeDtypeStruct((136, slots), F32),
            jax.ShapeDtypeStruct((128, 128 * -(-slot_rows // 128)), jnp.int32),
            jax.ShapeDtypeStruct((8, columns), jnp.int32),
            jax.ShapeDtypeStruct((8, 128), F32),
            jax.ShapeDtypeStruct((8, slots), F32),
        ],
        compiler_params=pltpu.CompilerParams(vmem_limit_bytes=60 * 1024 * 1024),
        name="set_up",
    )(*map(to_lines, arrays), *map(to_line, arrays), to_lines(send_rec))


def fast_path(
    rhs, start, spectrum_top, elem_code, rec_elem, rec_dir, rec_sub, rec_peer, rec_index, send_rec
):
    traces, stiffness, interp, face_weight, stiff_diag = operators()
    part_count = lax.axis_size("parts")
    slots = rhs.shape[1]
    capacity = send_rec.shape[0] // part_count
    arrays = (elem_code, rec_elem, rec_dir, rec_sub, rec_peer, rec_index)
    vmem = pl.BlockSpec(memory_space=pltpu.VMEM)
    rows, col, send, flag, elem = set_up(slots, capacity, arrays, send_rec)

    weight = np.concatenate([face_weight, face_weight], axis=0)
    quarters = [interp[72 * s : 72 * s + 72] for s in range(4)]
    eye = np.eye(72)
    onto = three(np.concatenate(quarters + [eye], axis=0))
    own = three(wide_rows([j.T @ (weight * j) for j in quarters] + [weight * eye]))
    back = [j.T * weight.T for j in quarters]
    near = three(wide_rows(back + [weight * j for j in quarters] + [weight * eye]))
    far = three(wide_rows(back + [weight * eye]))
    trace_high, trace_low = split_np(traces)
    stiff_high, stiff_low = split_np(stiffness)
    lift = np.zeros((216, 480))
    for d in range(6):
        lift[:, 80 * d : 80 * d + 36] = traces.T[:, 72 * d : 72 * d + 36]
        lift[:, 80 * d + 40 : 80 * d + 76] = traces.T[:, 72 * d + 36 : 72 * d + 72]
    lift_high, lift_low = split_np(lift)
    prec = (1.0 / stiff_diag).reshape(216, 1).astype(np.float32)
    constants = (
        prec, trace_high, trace_low, stiff_high, stiff_low, lift_high, lift_low, onto, own, near, far
    )
    copies = 2 * LD + LD - 1
    x, shown = pl.pallas_call(
        functools.partial(main_kernel, "parts", ITERS, capacity),
        in_specs=[vmem] * 2 + [pl.BlockSpec(memory_space=pltpu.SMEM)] + [vmem] * 16,
        out_specs=[vmem] * 2,
        out_shape=[jax.ShapeDtypeStruct((216, slots), F32), jax.ShapeDtypeStruct((8, 128), F32)],
        scratch_shapes=[
            pltpu.VMEM((216, slots), F32),
            pltpu.VMEM((216, slots), F32),
            pltpu.VMEM((432, slots), F32),
            pltpu.VMEM((6, 144, slots), BF16),
            pltpu.VMEM((480, slots), F32),
            pltpu.VMEM((6, slots, slots), BF16),
            pltpu.VMEM((6, slots, slots), BF16),
            pltpu.VMEM((2, capacity, capacity), BF16),
            pltpu.VMEM((4, LD * LATERAL, LATERAL), BF16),
            pltpu.VMEM((2, slots, capacity), BF16),
            pltpu.VMEM((slots, LD * LATERAL), BF16),
            pltpu.VMEM((8, 2 * capacity + 4 * LATERAL), F32),
            pltpu.VMEM((16, 128), F32),
            pltpu.VMEM((2, 72, capacity), F32),
            pltpu.VMEM((LD - 1, 72, LATERAL), F32),
            pltpu.VMEM((ITERS, 2, LD, 72, capacity), F32),
            pltpu.VMEM((ITERS, LD - 1, 72, LATERAL), F32),
            pltpu.VMEM((8, 128), F32),
            pltpu.VMEM((part_count, 8, 128), F32),
            pltpu.SemaphoreType.DMA((ITERS, copies)),
            pltpu.SemaphoreType.DMA((ITERS, copies)),
            pltpu.SemaphoreType.DMA((part_count,)),
            pltpu.SemaphoreType.DMA((part_count,)),
        ],
        compiler_params=pltpu.CompilerParams(
            collective_id=2, has_side_effects=True, vmem_limit_bytes=60 * 1024 * 1024
        ),
        name="smooth",
    )(
        start, rhs, spectrum_top, rows, col, send, flag, elem, *map(jnp.asarray, constants)
    )
    return x, shown


def on_device(*arguments):
    rhs, send_rec, rec_elem = arguments[0], arguments[9], arguments[4]
    part_count = lax.axis_size("parts")
    capacity, slots = send_rec.shape[0] // part_count, rhs.shape[1]
    suits = slots % 128 == 0 and rec_elem.shape[0] % 1024 == 0 and capacity % 128 == 0
    suits = suits and capacity <= slots <= 4096 and part_count % LD == 0 and part_count >= 3 * LD
    if not suits:
        return general_path(*arguments)
    x, shown = fast_path(*arguments)
    norms = shown[: 2 * ITERS, 0].reshape(ITERS, 2)
    return lax.cond(
        shown[2 * ITERS, 0] > 0.0, lambda: general_path(*arguments), lambda: (x, norms)
    )


def solution(mesh):
    placed = (
        P(None, "parts"),
        P(None, "parts"),
        P(),
        P("parts"),
        P("parts"),
        P("parts"),
        P("parts"),
        P("parts"),
        P("parts"),
        P("parts"),
    )
    return jax.shard_map(
        on_device, mesh=mesh, in_specs=placed, out_specs=(P(None, "parts"), P()), check_vma=False
    )
```

```python
import functools
import math

import jax
import jax.numpy as jnp
import numpy as np
from jax import lax
from jax.experimental import pallas as pl
from jax.experimental.pallas import tpu as pltpu
from jax.sharding import PartitionSpec as P

LD = 4
ITERS = 3


PENALTY = 36.0
BOTTOM_RATIO = 8.0


def lobatto_tables():
    root_seven = math.sqrt(7.0)
    inner_root = math.sqrt(1.0 / 3.0 - 2.0 * root_seven / 21.0)
    outer_root = math.sqrt(1.0 / 3.0 + 2.0 * root_seven / 21.0)
    points = (np.array([-1.0, -outer_root, -inner_root, inner_root, outer_root, 1.0]) + 1.0) / 2.0
    weights = (
        np.array(
            [
                1.0 / 15.0,
                (14.0 - root_seven) / 30.0,
                (14.0 + root_seven) / 30.0,
                (14.0 + root_seven) / 30.0,
                (14.0 - root_seven) / 30.0,
                1.0 / 15.0,
            ]
        )
        / 2.0
    )
    barycentric = np.array(
        [1.0 / np.prod([points[j] - points[k] for k in range(6) if k != j]) for j in range(6)]
    )
    derivative = np.zeros((6, 6))
    for i in range(6):
        for j in range(6):
            if i != j:
                derivative[i, j] = barycentric[j] / barycentric[i] / (points[i] - points[j])
        derivative[i, i] = -np.sum(derivative[i])
    halves = np.zeros((2, 6, 6))
    for which_half in range(2):
        targets = (points + which_half) / 2.0
        for i in range(6):
            for j in range(6):
                halves[which_half, i, j] = np.prod(
                    [(targets[i] - points[k]) / (points[j] - points[k]) for k in range(6) if k != j]
                )
    column_sums = np.sum(derivative * derivative * weights[:, None], axis=0)
    stiff_diag = (
        column_sums[:, None, None] * weights[None, :, None] * weights[None, None, :]
        + weights[:, None, None] * column_sums[None, :, None] * weights[None, None, :]
        + weights[:, None, None] * weights[None, :, None] * column_sums[None, None, :]
    )
    return (weights, derivative, halves, stiff_diag.reshape(216))


BF16 = jnp.bfloat16
F32 = jnp.float32


def split_np(matrix):
    high = np.asarray(matrix, np.float32).astype(BF16)
    low = (np.asarray(matrix, np.float64) - high.astype(np.float64)).astype(np.float32).astype(BF16)
    return high, low


def operators():
    weights, derivative, halves, stiff_diag = lobatto_tables()
    eye = np.eye(6)
    trace_rows = []
    for direction in range(6):
        axis_index = direction // 2
        layer_index = 5 * (direction % 2)
        orientation = 2.0 * (direction % 2) - 1.0
        for row in (eye[layer_index], orientation * derivative[layer_index]):
            factors = [eye, eye, eye]
            factors[axis_index] = row[None, :]
            trace_rows.append(np.kron(np.kron(factors[0], factors[1]), factors[2]))
    traces = np.concatenate(trace_rows, axis=0)
    stiff_1d = derivative.T @ (weights[:, None] * derivative)
    mass = np.diag(weights)
    stiffness = (
        np.kron(np.kron(stiff_1d, mass), mass)
        + np.kron(np.kron(mass, stiff_1d), mass)
        + np.kron(np.kron(mass, mass), stiff_1d)
    )
    blocks = []
    for sub in range(4):
        quarter = np.kron(halves[sub % 2], halves[sub // 2])
        blocks.append(np.kron(np.eye(2), quarter))
    return traces, stiffness, np.concatenate(blocks, axis=0), np.outer(weights, weights).reshape(36, 1), stiff_diag


def split(value):
    high = value.astype(BF16)
    return high, (value - high.astype(F32)).astype(BF16)


def dot(left, right):
    return jnp.dot(left, right, preferred_element_type=F32)


def dot3(left_high, left_low, right):
    high, low = split(right)
    return dot(left_high, high) + (dot(left_high, low) + dot(left_low, high))


def one_hot(index_row, rows, base=0):
    count = index_row.shape[1]
    position = lax.broadcasted_iota(jnp.int32, (rows, count), 0)
    return jnp.where(position == index_row - base, 1.0, 0.0).astype(BF16)


def pick(traces, elem, direction, sub, onto):
    wide = dot(traces, one_hot(elem, traces.shape[1]))
    face = jnp.zeros((72, elem.shape[1]), F32)
    for d in range(6):
        both = wide[72 * d : 72 * d + 72] + wide[432 + 72 * d : 432 + 72 * d + 72]
        face = jnp.where(direction == d, both, face)
    high, low = split(face)
    quarters = dot(onto, jnp.concatenate([high, low, high], axis=0))
    result = face
    for s in range(4):
        result = jnp.where(sub == s, quarters[72 * s : 72 * s + 72], result)
    return result


def send_kernel(x_ref, inv_ref, code_ref, mat_high, mat_low, onto_ref, out_ref, traces_ref):
    @pl.when(pl.program_id(0) == 0)
    def _():
        raw = dot3(mat_high[...], mat_low[...], x_ref[...])
        row = lax.broadcasted_iota(jnp.int32, raw.shape, 0)
        raw = jnp.where(lax.rem(row, 72) >= 36, raw * inv_ref[...], raw)
        high, low = split(raw)
        traces_ref[0:432] = high
        traces_ref[432:864] = low

    code = code_ref[...]
    picked = pick(traces_ref[...], code[0:1], code[1:2], code[2:3], onto_ref[...])
    capacity = out_ref.shape[2]
    for k in range(out_ref.shape[0]):
        out_ref[k] = picked[:, k * capacity : (k + 1) * capacity]


def exchange_kernel(
    steps, axis, width, src_ref, x_ref, traces_ref, code_ref, onto_ref, stiff_high, stiff_low,
    dst_ref, own_ref, near_ref, volume_ref, send_sem, recv_sem,
):
    count = lax.axis_size(axis)
    me = lax.axis_index(axis)
    barrier = pltpu.get_barrier_semaphore()
    peers = [lax.rem(me + step + count, count) for step in steps]
    for peer in peers:
        pl.semaphore_signal(barrier, inc=1, device_id=(peer,), device_id_type=pl.DeviceIdType.MESH)
    pl.semaphore_wait(barrier, len(steps))
    copies = []
    for k, peer in enumerate(peers):
        copy = pltpu.make_async_remote_copy(
            src_ref=src_ref.at[k],
            dst_ref=dst_ref.at[k],
            send_sem=send_sem.at[k],
            recv_sem=recv_sem.at[k],
            device_id=(peer,),
            device_id_type=pl.DeviceIdType.MESH,
        )
        copy.start()
        copies.append(copy)

    def step_tile(i, carry):
        part = pl.ds(pl.multiple_of(i * width, width), width)
        code = code_ref[:, part]
        own_ref[:, part] = pick(traces_ref[...], code[0:1], code[1:2], code[2:3], onto_ref[...])
        near_ref[:, part] = pick(traces_ref[...], code[3:4], code[4:5], code[5:6], onto_ref[...])
        return carry

    lax.fori_loop(0, code_ref.shape[1] // width, step_tile, 0)
    volume_ref[...] = dot3(stiff_high[...], stiff_low[...], x_ref[...])
    for copy in copies:
        copy.wait()


def norms_kernel(axis, sums_ref, out_ref, landing, send_sem, recv_sem):
    count = lax.axis_size(axis)
    me = lax.axis_index(axis)
    barrier = pltpu.get_barrier_semaphore()

    def greet(k, carry):
        peer = lax.rem(me + k, count)
        pl.semaphore_signal(barrier, inc=1, device_id=(peer,), device_id_type=pl.DeviceIdType.MESH)
        return carry

    def copy_to(k):
        return pltpu.make_async_remote_copy(
            src_ref=sums_ref,
            dst_ref=landing.at[k],
            send_sem=send_sem.at[k],
            recv_sem=recv_sem.at[k],
            device_id=(lax.rem(me + k, count),),
            device_id_type=pl.DeviceIdType.MESH,
        )

    def start(k, carry):
        copy_to(k).start()
        return carry

    def finish(k, carry):
        copy_to(k).wait()
        return carry

    lax.fori_loop(1, count, greet, 0)
    pl.semaphore_wait(barrier, count - 1)
    lax.fori_loop(1, count, start, 0)
    landing[0] = sums_ref[...]
    lax.fori_loop(1, count, finish, 0)

    def add(j, total):
        return total + landing[lax.rem(me + count - j, count)]

    total = lax.fori_loop(0, count, add, jnp.zeros(out_ref.shape, F32))
    out_ref[...] = jnp.broadcast_to(jnp.sum(total, axis=1, keepdims=True), out_ref.shape)


def apply_kernel(
    row_ref, coef_ref, x_ref, dirn_ref, rhs_ref, elem_ref, prec_ref, recv_ref, own_ref, near_ref,
    volume_ref, code_ref, rows_ref, size_ref, off_ref, weight_ref, lift_high, lift_low, prior_ref,
    x_out, dirn_out, sums_out, pool, total,
):
    peer_count = recv_ref.shape[0]

    @pl.when(pl.program_id(0) == 0)
    def _():
        for k in range(peer_count):
            high, low = split(recv_ref[k])
            pool[144 * k : 144 * k + 72] = high
            pool[144 * k + 72 : 144 * k + 144] = low
        total[...] = jnp.zeros_like(total)

    code = code_ref[...]
    direction, sub = code[1:2], code[2:3]
    bound = code[6:7] == -1
    width = sub.shape[1]
    own = own_ref[...]
    wide = dot(pool[...], one_hot(code[7:8], pool.shape[1]))
    partner = near_ref[...]
    for k in range(peer_count):
        both = wide[144 * k : 144 * k + 72] + wide[144 * k + 72 : 144 * k + 144]
        partner = jnp.where(code[6:7] == k, both, partner)
    own_value, own_slope = own[0:36], own[36:72]
    part_value = jnp.where(bound, 0.0, partner[0:36])
    part_slope = jnp.where(bound, -own_slope, partner[36:72])
    jump = own_value - part_value
    flux = 0.5 * (own_slope - part_slope)
    mortar = size_ref[0:1]
    area = mortar * mortar
    weight = weight_ref[...] * size_ref[1:2]
    term_value = weight * (PENALTY * mortar * jump - area * flux)
    term_slope = -weight * (jnp.where(bound, 1.0, 0.5) * area) * jump
    terms = jnp.concatenate([term_value, term_slope], axis=0)
    spread = jnp.concatenate([jnp.where(sub == s, terms, 0.0) for s in range(4)], axis=0)
    spread_high, spread_low = split(spread)
    back = dot(off_ref[...], jnp.concatenate([spread_high, spread_low, spread_high], axis=0))
    back = jnp.where(sub >= 4, terms, back)
    spread = jnp.concatenate([jnp.where(direction == d, back, 0.0) for d in range(6)], axis=0)
    wide_high, wide_low = split(spread)
    lanes = lax.broadcasted_iota(jnp.int32, (width, total.shape[1]), 1)
    hot = jnp.where(lanes == rows_ref[...], 1.0, 0.0).astype(BF16)
    total[...] += dot(wide_high, hot) + dot(wide_low, hot)

    @pl.when(pl.program_id(0) == pl.num_programs(0) - 1)
    def _():
        size, inv = elem_ref[0:1], elem_ref[1:2]
        field = x_ref[...]
        row = lax.broadcasted_iota(jnp.int32, total.shape, 0)
        faces = jnp.where(lax.rem(row, 72) >= 36, total[...] * inv, total[...])
        applied = size * volume_ref[...]
        applied = applied + dot3(lift_high[...], lift_low[...], faces)
        residual = jnp.where(size > 0.0, rhs_ref[...] - applied, 0.0)
        scaled = residual * (inv * prec_ref[...])
        step = coef_ref[0] * dirn_ref[...] + coef_ref[1] * scaled
        dirn_out[...] = step
        x_out[...] = field + step
        squares = jnp.sum(residual * residual, axis=0, keepdims=True)
        products = jnp.sum(residual * scaled, axis=0, keepdims=True)
        fold = lambda line: sum(line[:, k : k + 128] for k in range(0, line.shape[1], 128))
        row = lax.broadcasted_iota(jnp.int32, sums_out.shape, 0)
        row_index = row_ref[0]
        later = jnp.where(row == 2 * row_index + 1, fold(products), prior_ref[...])
        sums_out[...] = jnp.where(row == 2 * row_index, fold(squares), later)


def take_small(tables, index):
    rows = tables.shape[1] // 128
    fine = (jnp.arange(128, dtype=jnp.int32)[:, None] == (index % 128)[None, :]).astype(BF16)
    wide = jnp.dot(tables.reshape(-1, 128).astype(BF16), fine, preferred_element_type=F32)
    wide = wide.reshape(tables.shape[0], rows, -1)
    coarse = jnp.arange(rows, dtype=jnp.int32)[:, None] == (index // 128)[None, :]
    return jnp.sum(jnp.where(coarse[None], wide, 0.0), axis=1).astype(jnp.int32)


def tile(count):
    for width in (512, 256, 128):
        if count % width == 0:
            return width
    return count


def whole(shape):
    return pl.BlockSpec(shape, lambda i: (0,) * len(shape))


def general_path(
    rhs, start, spectrum_top, elem_code, rec_elem, rec_dir, rec_sub, rec_peer, rec_index, send_rec
):
    traces, stiffness, interp, face_weight, stiff_diag = operators()
    part_count = lax.axis_size("parts")
    own_index = lax.axis_index("parts")
    elem_count = rhs.shape[1]
    record_count = rec_elem.shape[0]
    capacity = send_rec.shape[0] // part_count
    far_reach = 2 * LD - 1
    code_float = elem_code.astype(F32)
    elem_size = 0.5 * code_float
    inv_size = jnp.where(elem_code > 0, 2.0 / jnp.maximum(code_float, 1.0), 0.0)
    elem_rows = jnp.stack([elem_size, inv_size])
    is_bound = rec_peer < 0
    is_local = rec_peer == own_index
    is_remote = jnp.logical_and(jnp.logical_not(is_bound), jnp.logical_not(is_local))
    offset = own_index - rec_peer
    position = jnp.where(offset < 0, offset + far_reach, offset + far_reach - 1)
    block = jnp.where(is_remote, position, jnp.where(is_bound, -1, -2))
    steps = list(range(-far_reach, 0)) + list(range(1, far_reach + 1))
    lists = send_rec.reshape(part_count, capacity)
    lists = jnp.concatenate([lists[part_count - far_reach :], lists, lists[:far_reach]], axis=0)
    lists = lax.dynamic_slice_in_dim(lists, own_index, 2 * far_reach + 1, 0)
    send_cols = jnp.concatenate([lists[:far_reach], lists[far_reach + 1 :]], axis=0).reshape(-1)
    send_count = send_cols.shape[0]

    own_size = 0.5 * take_small(elem_code[None], rec_elem)[0].astype(F32)
    mortar_size = jnp.where(rec_sub < 4, 0.5 * own_size, own_size)
    size_rows = jnp.stack([mortar_size, (rec_sub < 5).astype(F32)])
    tables = jnp.stack([rec_elem // 256, rec_elem % 256, rec_dir * 8 + rec_sub])
    found = take_small(tables, jnp.concatenate([send_cols, rec_index]))
    found = jnp.stack([found[0] * 256 + found[1], found[2] // 8, found[2] % 8])
    send_code = found[:, :send_count]
    near = jnp.where(is_local[None], found[:, send_count:], -1)
    rec_code = jnp.concatenate(
        [jnp.stack([rec_elem, rec_dir, rec_sub]), near, block[None], rec_index[None]],
        axis=0,
    )
    rec_rows = rec_elem[:, None]

    mat_high, mat_low = split_np(traces)
    lift_high, lift_low = split_np(traces.T)
    stiff_high, stiff_low = split_np(stiffness)
    onto_high, onto_low = split_np(interp)
    onto = np.concatenate([onto_high, onto_high, onto_low], axis=1)
    flat = np.concatenate([interp[72 * s : 72 * s + 72].T for s in range(4)], axis=1)
    off_high, off_low = split_np(flat)
    off = np.concatenate([off_high, off_high, off_low], axis=1)
    prec = jnp.asarray((1.0 / stiff_diag).reshape(216, 1), F32)
    weight = jnp.asarray(face_weight, F32)

    send_tile, rec_tile, peer_count = 2 * capacity, tile(record_count), len(steps)
    params = pltpu.CompilerParams(vmem_limit_bytes=60 * 1024 * 1024)
    field = (216, elem_count)

    def send_call(x):
        return pl.pallas_call(
            send_kernel,
            grid=(send_count // send_tile,),
            in_specs=[
                whole(field),
                whole((1, elem_count)),
                pl.BlockSpec((3, send_tile), lambda i: (0, i)),
                whole((432, 216)),
                whole((432, 216)),
                whole((288, 216)),
            ],
            out_specs=[pl.BlockSpec((2, 72, capacity), lambda i: (i, 0, 0)), whole((864, elem_count))],
            out_shape=[
                jax.ShapeDtypeStruct((peer_count, 72, capacity), F32),
                jax.ShapeDtypeStruct((864, elem_count), BF16),
            ],
            compiler_params=params,
            name="send_traces",
        )(x, inv_size[None], send_code, jnp.asarray(mat_high), jnp.asarray(mat_low), jnp.asarray(onto))

    vmem = pl.BlockSpec(memory_space=pltpu.VMEM)

    def exchange(outgoing, x, element_traces):
        return pl.pallas_call(
            functools.partial(exchange_kernel, steps, "parts", rec_tile),
            in_specs=[pl.BlockSpec(memory_space=pl.ANY)] + [vmem] * 6,
            out_specs=[pl.BlockSpec(memory_space=pl.ANY)] + [vmem] * 3,
            out_shape=[
                jax.ShapeDtypeStruct((peer_count, 72, capacity), F32),
                jax.ShapeDtypeStruct((72, record_count), F32),
                jax.ShapeDtypeStruct((72, record_count), F32),
                jax.ShapeDtypeStruct(field, F32),
            ],
            scratch_shapes=[
                pltpu.SemaphoreType.DMA((peer_count,)),
                pltpu.SemaphoreType.DMA((peer_count,)),
            ],
            compiler_params=pltpu.CompilerParams(
                collective_id=0, has_side_effects=True, vmem_limit_bytes=60 * 1024 * 1024
            ),
            name="exchange",
        )(
            outgoing, x, element_traces, rec_code, jnp.asarray(onto),
            jnp.asarray(stiff_high), jnp.asarray(stiff_low),
        )

    def all_sums(sums):
        return pl.pallas_call(
            functools.partial(norms_kernel, "parts"),
            in_specs=[vmem],
            out_specs=vmem,
            out_shape=jax.ShapeDtypeStruct((8, 128), F32),
            scratch_shapes=[
                pltpu.VMEM((part_count, 8, 128), F32),
                pltpu.SemaphoreType.DMA((part_count,)),
                pltpu.SemaphoreType.DMA((part_count,)),
            ],
            compiler_params=pltpu.CompilerParams(collective_id=1, has_side_effects=True),
            name="all_sums",
        )(sums)

    def apply_call(row_index, coef, x, dirn, received, own, near_traces, volume, sums):
        tiles = lambda rows: pl.BlockSpec((rows, rec_tile), lambda i: (0, i))
        return pl.pallas_call(
            apply_kernel,
            grid=(record_count // rec_tile,),
            in_specs=[
                pl.BlockSpec(memory_space=pltpu.SMEM),
                pl.BlockSpec(memory_space=pltpu.SMEM),
                whole(field),
                whole(field),
                whole(field),
                whole((2, elem_count)),
                whole((216, 1)),
                whole((peer_count, 72, capacity)),
                tiles(72),
                tiles(72),
                whole(field),
                tiles(8),
                pl.BlockSpec((rec_tile, 1), lambda i: (i, 0)),
                tiles(2),
                whole((72, 864)),
                whole((36, 1)),
                whole((216, 432)),
                whole((216, 432)),
                whole((8, 128)),
            ],
            out_specs=[whole(field), whole(field), whole((8, 128))],
            out_shape=[
                jax.ShapeDtypeStruct(field, F32),
                jax.ShapeDtypeStruct(field, F32),
                jax.ShapeDtypeStruct((8, 128), F32),
            ],
            scratch_shapes=[
                pltpu.VMEM((144 * peer_count, capacity), BF16),
                pltpu.VMEM((432, elem_count), F32),
            ],
            compiler_params=params,
            name="apply_operator",
        )(
            row_index[None], coef, x, dirn, rhs, elem_rows, prec, received, own, near_traces, volume, rec_code, rec_rows,
            size_rows, jnp.asarray(off), weight, jnp.asarray(lift_high), jnp.asarray(lift_low), sums,
        )

    scale_total = 216.0 * elem_count * part_count
    top_value = spectrum_top[0]
    bottom = top_value / BOTTOM_RATIO
    center = 0.5 * (top_value + bottom)
    radius = 0.5 * (top_value - bottom)
    sigma_ratio = center / radius
    rho_prev = 1.0 / sigma_ratio
    coefs = [jnp.stack([jnp.zeros_like(center), 1.0 / center])]
    for step_index in range(1, ITERS):
        rho_next = 1.0 / (2.0 * sigma_ratio - rho_prev)
        coefs.append(jnp.stack([rho_next * rho_prev, 2.0 * rho_next / radius]))
        rho_prev = rho_next
    coefs = jnp.stack(coefs)

    def one_step(step_index, state):
        x, dirn, sums = state
        outgoing, element_traces = send_call(x)
        moved = exchange(outgoing, x, element_traces)
        coef = lax.dynamic_index_in_dim(coefs, step_index, 0, False)
        return tuple(apply_call(step_index, coef, x, dirn, *moved, sums))

    x, dirn, sums = lax.fori_loop(0, ITERS, one_step, (start, start, jnp.zeros((8, 128), F32)))
    norms = 0.5 * jnp.log(all_sums(sums)[: 2 * ITERS, 0].reshape(ITERS, 2) / scale_total)
    return (x, norms)


LATERAL = 128
FIELDS = 9


def iota(shape, axis):
    return lax.broadcasted_iota(jnp.int32, shape, axis)


def sum_rows(value):
    return jnp.sum(value, axis=0, keepdims=True)


def total_of(value):
    return jnp.sum(value, axis=1, keepdims=True)


def look_up(tables, rows, index):
    hot = jnp.where(iota((128, index.shape[1]), 0) == (index & 127), 1.0, 0.0).astype(BF16)
    wide = dot(tables, hot)
    mask = iota((rows, index.shape[1]), 0) == (index >> 7)
    count = tables.shape[0] // rows
    return [sum_rows(jnp.where(mask, wide[k * rows : (k + 1) * rows], 0.0)) for k in range(count)]


def regroup(columns, position, rows):
    mask = iota((rows, position.shape[1]), 0) == (position >> 7)
    left = jnp.concatenate([jnp.where(mask, column, 0.0) for column in columns], axis=0).astype(BF16)
    hot = jnp.where(iota((128, position.shape[1]), 0) == (position & 127), 1.0, 0.0).astype(BF16)
    return lax.dot_general(left, hot, (((1,), (1,)), ((), ())), preferred_element_type=F32)


def setup_kernel(
    axis, capacity, code_ref, elem_ref, dir_ref, sub_ref, peer_ref, index_ref,
    code_line, elem_line, dir_line, sub_line, peer_line, index_line, lists_ref,
    rows_ref, col_ref, send_ref, flag_ref, elem_out,
):
    me = lax.axis_index(axis)
    count = lax.axis_size(axis)
    group, place = me // LD, lax.rem(me, LD)
    elem, direction, sub = elem_line[...], dir_line[...], sub_line[...]
    peer, index = peer_line[...], index_line[...]
    records, slots = elem.shape[1], code_line.shape[1]
    chunks, table_rows, slot_rows = records // 128, records // 128, 6 * slots // 128
    used = sub < 5
    local = used & (peer == me)
    bound = used & (peer < 0)
    remote = used & (peer >= 0) & (peer != me)

    kind = jnp.where(used, jnp.where(remote, direction, direction + 8), -1)
    member = jnp.where(iota((16, records), 0) == kind, 1.0, 0.0)
    stacked = jnp.concatenate([member[:, 128 * k : 128 * k + 128] for k in range(chunks)], axis=0)
    upper = jnp.where(iota((128, 128), 0) < iota((128, 128), 1), 1.0, 0.0)
    counted = dot(
        stacked.astype(BF16), jnp.concatenate([upper, jnp.ones((128, 128), F32)], axis=1).astype(BF16)
    )
    carry = jnp.zeros((16, 128), F32)
    before = []
    for k in range(chunks):
        before.append(counted[16 * k : 16 * k + 16, :128] + carry)
        carry = carry + counted[16 * k : 16 * k + 16, 128:]
    base = jnp.concatenate([jnp.zeros((8, 128), F32), carry[:8]], axis=0)
    before = jnp.concatenate([part + base for part in before], axis=1)
    rank = sum_rows(before * member).astype(jnp.int32)
    in_range = used & (rank < slots)
    slot = jnp.where(in_range, direction * slots + rank, -1)

    tables = jnp.concatenate(
        [
            (elem_ref[...] & 127).astype(F32),
            ((elem_ref[...] >> 7) * 8 + sub_ref[...]).astype(F32),
            dir_ref[...].astype(F32),
        ],
        axis=0,
    ).astype(BF16)
    rows_per = capacity // 128
    list_rows = iota(lists_ref.shape, 0)
    lists = lists_ref[...].astype(F32)
    channel = []
    for d, other in ((1, group + 1), (0, group - 1)):
        here = remote & (direction == d)
        most = jnp.max(jnp.where(here, peer, -1), axis=1, keepdims=True)
        least = jnp.min(jnp.where(here, peer, count), axis=1, keepdims=True)
        wrong = here & (peer // LD != other)
        channel.append((most, jnp.where((most >= 0) & (most != least), 1.0, 0.0), wrong))
    wanted = []
    for most, _, _ in channel:
        for part in range(rows_per):
            wanted.append(sum_rows(jnp.where(list_rows == most * rows_per + part, lists, 0.0)))
    for pos in range(LD - 1):
        dest = group * LD + lax.rem(place + pos + 1, LD)
        wanted.append(sum_rows(jnp.where(list_rows == dest * rows_per, lists, 0.0)))
    wanted.append(jnp.zeros((1, LATERAL), F32))
    wanted = jnp.concatenate(wanted, axis=1).astype(jnp.int32)
    wanted_count = wanted.shape[1]
    low, high, found_dir = look_up(tables, table_rows, jnp.concatenate([wanted, index], axis=1))
    high = high.astype(jnp.int32)
    found_elem = low.astype(jnp.int32) + 128 * (high >> 3)
    found_sub = high & 7
    send_ref[0:1] = found_elem[:, :wanted_count]
    send_ref[1:2] = found_dir[:, :wanted_count].astype(jnp.int32)
    send_ref[2:3] = found_sub[:, :wanted_count]
    send_ref[3:8] = jnp.zeros((5, wanted_count), jnp.int32)
    near_elem, near_sub = found_elem[:, wanted_count:], found_sub[:, wanted_count:]

    code_rows = -(-slots // 1024) * 8
    code_table = code_ref[...].astype(F32)
    if code_rows > code_table.shape[0]:
        pad = jnp.zeros((code_rows - code_table.shape[0], 128), F32)
        code_table = jnp.concatenate([code_table, pad], axis=0)
    code = look_up(code_table.astype(BF16), code_rows, elem)[0]
    size = 0.5 * code
    mortar = jnp.where(sub < 4, 0.5 * size, size)

    turn = lax.rem(place - lax.rem(peer, LD) + LD, LD) - 1
    landed = jnp.where(direction < 2, index, turn * LATERAL + index)
    split_near = jnp.where(sub < 4, sub, jnp.where(near_sub < 4, near_sub + 4, 8))
    split_far = jnp.minimum(sub, 4)
    real = lambda value: value.astype(F32)
    columns = [
        real(elem & 127),
        real((elem >> 7) + 1),
        real(near_elem & 127),
        jnp.where(local, real((near_elem >> 7) + 1), 0.0),
        jnp.where(remote, real(landed & 127), 0.0),
        jnp.where(remote, real((landed >> 7) + 1), 0.0),
        real(split_near),
        real(split_far),
        mortar,
    ]
    moved = regroup(columns, slot, slot_rows)
    part = lambda k: moved[k * slot_rows : (k + 1) * slot_rows]
    join = lambda k: jnp.where(part(k + 1) > 0.0, part(k) + 128.0 * (part(k + 1) - 1.0), -1.0)
    own = join(0)
    spare = col_ref.shape[1] - slot_rows
    own_all = jnp.concatenate([own, jnp.zeros((spare, 128), F32)], axis=0)
    col_ref[...] = jnp.transpose(own_all).astype(jnp.int32)
    mort = part(8)
    fields = [join(2), join(4), part(6), part(7), 36.0 * mort, 0.5 * mort * mort]

    face = jnp.where(used, direction * slots + elem, -1)
    marks = [jnp.where(used & (sub == s), 1.0, 0.0) for s in range(5)]
    marks.append(jnp.where(bound & (sub == 4), 1.0, 0.0))
    tally = regroup(marks, face, slot_rows)
    fields += [tally[k * slot_rows : (k + 1) * slot_rows] for k in range(6)]
    per = slots // 128
    lines = []
    for value in fields:
        pieces = []
        for d in range(6):
            pieces.append(
                jnp.concatenate([value[per * d + q : per * d + q + 1] for q in range(per)], axis=1)
            )
        pieces.append(jnp.zeros((2, slots), F32))
        lines.append(jnp.concatenate(pieces, axis=0))
    code_all = code_line[...].astype(F32)
    size_all = 0.5 * code_all
    inv_all = jnp.where(code_all > 0.0, 2.0 / jnp.maximum(code_all, 1.0), 0.0)
    elem_out[0:1] = size_all
    elem_out[1:2] = inv_all
    elem_out[2:8] = jnp.zeros((6, slots), F32)
    half = 0.5 * size_all
    counts, bounds = lines[6:11], lines[11]
    lines = lines[:6]
    for s in range(5):
        lines.append(36.0 * (half if s < 4 else size_all) * counts[s])
    for s in range(4):
        lines.append(half * half * (0.5 * counts[s]))
    lines.append(size_all * size_all * (0.5 * (counts[4] + bounds)))
    for k, line in enumerate(lines):
        rows_ref[8 * k : 8 * k + 8] = line
    rows_ref[8 * len(lines) :] = jnp.zeros((rows_ref.shape[0] - 8 * len(lines), slots), F32)

    wrong = jnp.where(remote & (direction >= 2) & ((peer // LD != group) | (index >= LATERAL)), 1.0, 0.0)
    wrong = wrong + jnp.where(bound & (sub < 4), 1.0, 0.0)
    wrong = wrong + jnp.where(local & (sub < 4) & (near_sub < 4), 1.0, 0.0)
    wrong = wrong + jnp.where(used & (rank >= slots), 1.0, 0.0)
    for _, _, off in channel:
        wrong = wrong + jnp.where(off, 1.0, 0.0)
    faults = total_of(wrong) + channel[0][1] + channel[1][1]
    row = iota((8, 128), 0)
    allowed = jnp.where(row < 2, float(capacity), float(LATERAL))
    over = jnp.where((row < 6) & (carry[:8] > allowed), 1.0, 0.0)
    faults = faults + total_of(sum_rows(over))
    turns = [
        lax.rem(place - lax.rem(jnp.maximum(most, 0), LD) + LD, LD).astype(F32) for most, _, _ in channel
    ]
    ahead = [
        jnp.where(most >= 0, lax.rem(jnp.maximum(most, 0) % LD - place + LD, LD), -1).astype(F32)
        for most, _, _ in channel
    ]
    flags = jnp.where(row == 0, faults, jnp.where(row == 1, turns[1], turns[0]))
    flag_ref[...] = jnp.where(row == 3, ahead[0], jnp.where(row == 4, ahead[1], flags))


def stack2(value):
    high = value.astype(BF16).astype(F32)
    return jnp.concatenate([high, value - high], axis=0).astype(BF16)


def stack3(value):
    high = value.astype(BF16).astype(F32)
    return jnp.concatenate([high, value - high, high], axis=0).astype(BF16)


def fold_pair(value):
    half = value.shape[0] // 2
    return value[:half] + value[half:]


def choose(blocks, rows, code):
    last = blocks.shape[0] // rows - 1
    result = blocks[last * rows :]
    for q in range(last):
        result = jnp.where(code == q, blocks[q * rows : q * rows + rows], result)
    return result


def main_kernel(
    axis, iters, capacity,
    x_ref, rhs_ref, top_ref, rows_ref, col_ref, send_ref, flag_ref, elem_ref, prec_ref,
    trace_high, trace_low, stiff_high, stiff_low, lift_high, lift_low, onto_ref, own_ref, near_ref, far_ref,
    x_out, norm_out,
    dirn, volume, traces, pairs, faces, scatter, gather, gather_chan, gather_lat, send_chan, send_lat,
    far_rows, coefs, snd_chan, snd_lat, snd_pass, kept_pass, rcv_chan, rcv_lat, rcv_pass, turns, sums, landing,
    send_sem, recv_sem, turn_send, turn_recv, sum_send, sum_recv,
):
    count = lax.axis_size(axis)
    me = lax.axis_index(axis)
    group, place = me // LD, lax.rem(me, LD)
    groups = count // LD
    slots, half = x_ref.shape[1], capacity // 2
    mesh_id = pl.DeviceIdType.MESH
    barrier = pltpu.get_barrier_semaphore()

    def greet(k, carry):
        peer = lax.rem(me + k, count)
        pl.semaphore_signal(barrier, inc=1, device_id=(peer,), device_id_type=mesh_id)
        return carry

    lax.fori_loop(1, count, greet, 0)

    def hot(mask):
        return jnp.where(mask, 1.0, 0.0).astype(BF16)

    per = slots // 128
    columns = col_ref[...]
    for d in range(6):
        line = rows_ref[d : d + 1].astype(jnp.int32)
        gather[d] = hot(iota((slots, slots), 0) == line)
        for q in range(per):
            column = columns[:, per * d + q : per * d + q + 1]
            scatter[d, 128 * q : 128 * q + 128] = hot(iota((128, slots), 1) == column)
        line = rows_ref[8 + d : 9 + d].astype(jnp.int32)
        if d < 2:
            gather_chan[d] = hot(iota((capacity, capacity), 0) == line[:, :capacity])
        else:
            gather_lat[d - 2] = hot(iota((LD * LATERAL, LATERAL), 0) == line[:, :LATERAL])
    size, inv = elem_ref[0:1], elem_ref[1:2]
    pl.semaphore_wait(barrier, count - 1)

    def across(side, turn):
        other = lax.rem(group + (1 if side == 0 else groups - 1), groups)
        return (other * LD + lax.rem(place + turn, LD),)

    told = [
        pltpu.make_async_remote_copy(
            src_ref=flag_ref,
            dst_ref=turns.at[side, turn],
            send_sem=turn_send.at[side * LD + turn],
            recv_sem=turn_recv.at[side * LD + turn],
            device_id=across(side, turn),
            device_id_type=mesh_id,
        )
        for side in range(2)
        for turn in range(LD)
    ]
    for copy in told:
        copy.start()
    send_elem = send_ref[0:1]
    send_chan[0] = hot(iota((slots, capacity), 0) == send_elem[:, :capacity])
    send_chan[1] = hot(iota((slots, capacity), 0) == send_elem[:, capacity : 2 * capacity])
    send_lat[...] = hot(iota((slots, LD * LATERAL), 0) == send_elem[:, 2 * capacity :])
    chosen = jnp.zeros(far_rows.shape, F32)
    for k, field in enumerate((3, 4, 5)):
        block = rows_ref[8 * field : 8 * field + 8]
        pieces = []
        for d in range(6):
            part = block[:, : capacity if d < 2 else LATERAL]
            pieces.append(sum_rows(jnp.where(iota(part.shape, 0) == d, part, 0.0)))
        chosen = jnp.where(iota(chosen.shape, 0) == k, jnp.concatenate(pieces, axis=1), chosen)
    far_rows[...] = chosen

    line = jnp.ones((1, 128), F32)
    top = top_ref[0] * line
    bottom = top / BOTTOM_RATIO
    center = 0.5 * (top + bottom)
    radius = 0.5 * (top - bottom)
    sigma = center / radius
    rho = 1.0 / sigma
    coefs[0:1] = 0.0 * line
    coefs[1:2] = 1.0 / center
    for k in range(1, iters):
        rho_next = 1.0 / (2.0 * sigma - rho)
        coefs[2 * k : 2 * k + 1] = rho_next * rho
        coefs[2 * k + 1 : 2 * k + 2] = 2.0 * rho_next / radius
        rho = rho_next
    x_out[...] = x_ref[...]
    dirn[...] = jnp.zeros_like(dirn)
    sums[...] = jnp.where(iota(sums.shape, 0) == 2 * iters, flag_ref[0:1], 0.0) * jnp.where(
        iota(sums.shape, 1) == 0, 1.0, 0.0
    )

    for copy in told:
        copy.wait()

    def step(it, carry):
        field = x_out[...]
        raw = dot3(trace_high[...], trace_low[...], field)
        raw = jnp.where(lax.rem(iota(raw.shape, 0), 72) >= 36, raw * inv, raw)
        traces[...] = raw
        for d in range(6):
            pairs[d] = stack2(raw[72 * d : 72 * d + 72])

        send_dir = send_ref[1:2, 2 * capacity :]
        lateral = jnp.zeros((72, LD * LATERAL), F32)
        for d in range(2, 6):
            lateral = jnp.where(send_dir == d, fold_pair(dot(pairs[d], send_lat[...])), lateral)
        outgoing = jnp.concatenate(
            [fold_pair(dot(pairs[1], send_chan[0])), fold_pair(dot(pairs[0], send_chan[1])), lateral], axis=1
        )
        outgoing = choose(dot(onto_ref[...], stack3(outgoing)), 80, send_ref[2:3])
        for side in range(2):
            for turn in range(LD):
                low, left = 40 * (turn // 2), side * capacity + half * (turn % 2)
                snd_chan[side, turn] = outgoing[low : low + 40, left : left + half]
        for pos in range(LD - 1):
            start = 2 * capacity + pos * LATERAL
            snd_lat[pos] = outgoing[:, start : start + LATERAL]

        def send(source, target, k, place_of):
            return pltpu.make_async_remote_copy(
                src_ref=source,
                dst_ref=target,
                send_sem=send_sem.at[it, k],
                recv_sem=recv_sem.at[it, k],
                device_id=place_of,
                device_id_type=mesh_id,
            )

        def beside(turn):
            return (group * LD + lax.rem(place + turn, LD),)

        pairs_of = [(side, turn) for side in range(2) for turn in range(LD)]
        channel = [
            send(snd_chan.at[side, turn], rcv_chan.at[it, side, turn], side * LD + turn, across(side, turn))
            for side, turn in pairs_of
        ]
        lateral = [
            send(snd_lat.at[pos], rcv_lat.at[it, pos], 2 * LD + pos, beside(pos + 1)) for pos in range(LD - 1)
        ]
        passed = [
            send(
                snd_pass.at[side, turn - 1],
                rcv_pass.at[it, side, turn - 1],
                (3 + side) * LD + turn - 1,
                beside(turn),
            )
            for side, turn in pairs_of
            if turn
        ]
        for copy in channel + lateral:
            copy.start()

        volume[...] = dot3(stiff_high[...], stiff_low[...], field) * size

        def local_faces(d, inner):
            line = lambda k: rows_ref[pl.ds(8 * k + d, 1)]
            mass = dot(own_ref[...], stack3(traces[pl.ds(pl.multiple_of(72 * d, 8), 72)]))
            value = jnp.zeros((40, slots), F32)
            slope = jnp.zeros((40, slots), F32)
            for s in range(5):
                mass_value, mass_slope = mass[80 * s : 80 * s + 40], mass[80 * s + 40 : 80 * s + 80]
                flux = line(11 + s)
                value = value + (line(6 + s) * mass_value - flux * mass_slope)
                slope = slope - flux * mass_value
            facing = d + 1 - 2 * lax.rem(d, 2)
            found = fold_pair(dot(pairs[facing], gather[d]))
            found = choose(dot(near_ref[...], stack3(found)), 80, line(2).astype(jnp.int32))
            jump, flux = line(4), line(5)
            terms = jnp.concatenate([flux * found[40:] - jump * found[:40], flux * found[:40]], axis=0)
            back = fold_pair(dot(stack2(terms), scatter[d]))
            faces[pl.ds(pl.multiple_of(80 * d, 8), 80)] = back + jnp.concatenate([value, slope], axis=0)
            return inner

        lax.fori_loop(0, 4, local_faces, 0)
        for copy in channel:
            copy.wait()
        for side in range(2):
            for turn in range(LD):
                chunk = jnp.zeros((40, half), F32)
                for k in range(LD):
                    mine = turns[side, k, 3 + side : 4 + side, 0:1] == float((turn + k) % LD)
                    chunk = jnp.where(mine, rcv_chan[it, side, k], chunk)
                if turn:
                    snd_pass[side, turn - 1] = chunk
                else:
                    kept_pass[side] = chunk
        for copy in passed:
            copy.start()
        lax.fori_loop(4, 6, local_faces, 0)
        for copy in passed + lateral:
            copy.wait()

        pieces = []
        for side in range(2):
            turn = flag_ref[side + 1 : side + 2, 0:1]
            landed = [kept_pass[side]] + [rcv_pass[it, side, k] for k in range(LD - 1)]
            chunks = []
            for k in range(LD):
                chunk = landed[(-k) % LD]
                for t in range(1, LD):
                    chunk = jnp.where(turn == float(t), landed[(t - k) % LD], chunk)
                chunks.append(chunk)
            got = jnp.concatenate(
                [jnp.concatenate(chunks[:2], axis=1), jnp.concatenate(chunks[2:], axis=1)], axis=0
            )
            pieces.append(fold_pair(dot(stack2(got), gather_chan[side])))
        sides = [rcv_lat[it, pos] for pos in range(LD - 1)] + [jnp.zeros((80, LATERAL), F32)]
        got = stack2(jnp.concatenate(sides, axis=1))
        for d in range(4):
            pieces.append(fold_pair(dot(got, gather_lat[d])))
        found = jnp.concatenate(pieces, axis=1)
        found = choose(dot(far_ref[...], stack3(found)), 80, far_rows[0:1].astype(jnp.int32))
        jump, flux = far_rows[1:2], far_rows[2:3]
        terms = stack2(
            jnp.concatenate([flux * found[40:] - jump * found[:40], flux * found[:40]], axis=0)
        )
        for d in range(6):
            width = capacity if d < 2 else LATERAL
            start = d * capacity if d < 2 else 2 * capacity + (d - 2) * LATERAL
            faces[80 * d : 80 * d + 80] += fold_pair(
                dot(terms[:, start : start + width], scatter[d, :width])
            )
        total = faces[...]
        total = jnp.where(lax.rem(iota(total.shape, 0), 80) >= 40, total * inv, total)
        applied = volume[...] + dot3(lift_high[...], lift_low[...], total)
        residual = jnp.where(size > 0.0, rhs_ref[...] - applied, 0.0)
        scaled = residual * (inv * prec_ref[...])
        first = coefs[pl.ds(2 * it, 1), 0:1]
        second = coefs[pl.ds(2 * it + 1, 1), 0:1]
        change = first * dirn[...] + second * scaled
        dirn[...] = change
        x_out[...] = field + change
        squares = sum_rows(residual * residual)
        products = sum_rows(residual * scaled)
        fold = lambda row: sum(row[:, k : k + 128] for k in range(0, row.shape[1], 128))
        row = iota(sums.shape, 0)
        kept = jnp.where(row == 2 * it + 1, fold(products), sums[...])
        sums[...] = jnp.where(row == 2 * it, fold(squares), kept)
        return carry

    lax.fori_loop(0, iters, step, 0)

    def copy_to(k):
        return pltpu.make_async_remote_copy(
            src_ref=sums,
            dst_ref=landing.at[k],
            send_sem=sum_send.at[k],
            recv_sem=sum_recv.at[k],
            device_id=(lax.rem(me + k, count),),
            device_id_type=mesh_id,
        )

    def begin(k, carry):
        copy_to(k).start()
        return carry

    def finish(k, carry):
        copy_to(k).wait()
        return carry

    def add(j, total):
        return total + landing[lax.rem(me + count - j, count)]

    lax.fori_loop(1, count, begin, 0)
    landing[0] = sums[...]
    lax.fori_loop(1, count, finish, 0)
    total = total_of(lax.fori_loop(0, count, add, jnp.zeros(sums.shape, F32)))
    mean = total / (216.0 * slots * count)
    logs = 0.5 * jnp.log(jnp.where(iota(total.shape, 0) < 2 * iters, mean, 1.0))
    shown = jnp.where(iota(total.shape, 0) < 2 * iters, logs, total)
    norm_out[...] = jnp.broadcast_to(shown, norm_out.shape)


def wide_rows(blocks):
    padded = []
    for block in blocks:
        rows = np.zeros((80, block.shape[1]))
        rows[0:36], rows[40:76] = block[0:36], block[36:72]
        padded.append(rows)
    return np.concatenate(padded, axis=0)


def three(matrix):
    high, low = split_np(matrix)
    return np.concatenate([high, high, low], axis=1)


def set_up(slots, capacity, arrays, send_rec):
    slot_rows = 6 * slots // 128
    to_lines = lambda array: array.reshape(-1, 128)
    to_line = lambda array: array.reshape(1, -1)
    vmem = pl.BlockSpec(memory_space=pltpu.VMEM)
    columns = 2 * capacity + LD * LATERAL
    return pl.pallas_call(
        functools.partial(setup_kernel, "parts", capacity),
        in_specs=[vmem] * 13,
        out_specs=[vmem] * 5,
        out_shape=[
            jax.ShapeDtypeStruct((136, slots), F32),
            jax.ShapeDtypeStruct((128, 128 * -(-slot_rows // 128)), jnp.int32),
            jax.ShapeDtypeStruct((8, columns), jnp.int32),
            jax.ShapeDtypeStruct((8, 128), F32),
            jax.ShapeDtypeStruct((8, slots), F32),
        ],
        compiler_params=pltpu.CompilerParams(vmem_limit_bytes=60 * 1024 * 1024),
        name="set_up",
    )(*map(to_lines, arrays), *map(to_line, arrays), to_lines(send_rec))


def fast_path(
    rhs, start, spectrum_top, elem_code, rec_elem, rec_dir, rec_sub, rec_peer, rec_index, send_rec
):
    traces, stiffness, interp, face_weight, stiff_diag = operators()
    part_count = lax.axis_size("parts")
    slots = rhs.shape[1]
    capacity = send_rec.shape[0] // part_count
    arrays = (elem_code, rec_elem, rec_dir, rec_sub, rec_peer, rec_index)
    vmem = pl.BlockSpec(memory_space=pltpu.VMEM)
    rows, col, send, flag, elem = set_up(slots, capacity, arrays, send_rec)

    weight = np.concatenate([face_weight, face_weight], axis=0)
    quarters = [interp[72 * s : 72 * s + 72] for s in range(4)]
    eye = np.eye(72)
    onto = three(wide_rows(quarters + [eye]))
    own = three(wide_rows([j.T @ (weight * j) for j in quarters] + [weight * eye]))
    back = [j.T * weight.T for j in quarters]
    near = three(wide_rows(back + [weight * j for j in quarters] + [weight * eye]))
    far = wide_rows(back + [weight * eye])
    far = three(wide_rows([far.T]).T)
    trace_high, trace_low = split_np(traces)
    stiff_high, stiff_low = split_np(stiffness)
    lift = np.zeros((216, 480))
    for d in range(6):
        lift[:, 80 * d : 80 * d + 36] = traces.T[:, 72 * d : 72 * d + 36]
        lift[:, 80 * d + 40 : 80 * d + 76] = traces.T[:, 72 * d + 36 : 72 * d + 72]
    lift_high, lift_low = split_np(lift)
    prec = (1.0 / stiff_diag).reshape(216, 1).astype(np.float32)
    constants = (
        prec, trace_high, trace_low, stiff_high, stiff_low, lift_high, lift_low, onto, own, near, far
    )
    copies, half = 5 * LD, capacity // 2
    x, shown = pl.pallas_call(
        functools.partial(main_kernel, "parts", ITERS, capacity),
        in_specs=[vmem] * 2 + [pl.BlockSpec(memory_space=pltpu.SMEM)] + [vmem] * 16,
        out_specs=[vmem] * 2,
        out_shape=[jax.ShapeDtypeStruct((216, slots), F32), jax.ShapeDtypeStruct((8, 128), F32)],
        scratch_shapes=[
            pltpu.VMEM((216, slots), F32),
            pltpu.VMEM((216, slots), F32),
            pltpu.VMEM((432, slots), F32),
            pltpu.VMEM((6, 144, slots), BF16),
            pltpu.VMEM((480, slots), F32),
            pltpu.VMEM((6, slots, slots), BF16),
            pltpu.VMEM((6, slots, slots), BF16),
            pltpu.VMEM((2, capacity, capacity), BF16),
            pltpu.VMEM((4, LD * LATERAL, LATERAL), BF16),
            pltpu.VMEM((2, slots, capacity), BF16),
            pltpu.VMEM((slots, LD * LATERAL), BF16),
            pltpu.VMEM((8, 2 * capacity + 4 * LATERAL), F32),
            pltpu.VMEM((16, 128), F32),
            pltpu.VMEM((2, LD, 40, half), F32),
            pltpu.VMEM((LD - 1, 80, LATERAL), F32),
            pltpu.VMEM((2, LD - 1, 40, half), F32),
            pltpu.VMEM((2, 40, half), F32),
            pltpu.VMEM((ITERS, 2, LD, 40, half), F32),
            pltpu.VMEM((ITERS, LD - 1, 80, LATERAL), F32),
            pltpu.VMEM((ITERS, 2, LD - 1, 40, half), F32),
            pltpu.VMEM((2, LD, 8, 128), F32),
            pltpu.VMEM((8, 128), F32),
            pltpu.VMEM((part_count, 8, 128), F32),
            pltpu.SemaphoreType.DMA((ITERS, copies)),
            pltpu.SemaphoreType.DMA((ITERS, copies)),
            pltpu.SemaphoreType.DMA((2 * LD,)),
            pltpu.SemaphoreType.DMA((2 * LD,)),
            pltpu.SemaphoreType.DMA((part_count,)),
            pltpu.SemaphoreType.DMA((part_count,)),
        ],
        compiler_params=pltpu.CompilerParams(
            collective_id=2, has_side_effects=True, vmem_limit_bytes=60 * 1024 * 1024
        ),
        name="smooth",
    )(
        start, rhs, spectrum_top, rows, col, send, flag, elem, *map(jnp.asarray, constants)
    )
    return x, shown


def on_device(*arguments):
    rhs, send_rec, rec_elem = arguments[0], arguments[9], arguments[4]
    part_count = lax.axis_size("parts")
    capacity, slots = send_rec.shape[0] // part_count, rhs.shape[1]
    suits = slots % 128 == 0 and rec_elem.shape[0] % 1024 == 0 and capacity % 256 == 0
    suits = suits and capacity <= slots <= 4096 and part_count % LD == 0 and part_count >= 3 * LD
    if not suits:
        return general_path(*arguments)
    x, shown = fast_path(*arguments)
    norms = shown[: 2 * ITERS, 0].reshape(ITERS, 2)
    return lax.cond(
        shown[2 * ITERS, 0] > 0.0, lambda: general_path(*arguments), lambda: (x, norms)
    )


def solution(mesh):
    placed = (
        P(None, "parts"),
        P(None, "parts"),
        P(),
        P("parts"),
        P("parts"),
        P("parts"),
        P("parts"),
        P("parts"),
        P("parts"),
        P("parts"),
    )
    return jax.shard_map(
        on_device, mesh=mesh, in_specs=placed, out_specs=(P(None, "parts"), P()), check_vma=False
    )
```

```python
import functools
import math

import jax
import jax.numpy as jnp
import numpy as np
from jax import lax
from jax.experimental import pallas as pl
from jax.experimental.pallas import tpu as pltpu
from jax.sharding import PartitionSpec as P

LD = 4
ITERS = 3


PENALTY = 36.0
BOTTOM_RATIO = 8.0


def lobatto_tables():
    root_seven = math.sqrt(7.0)
    inner_root = math.sqrt(1.0 / 3.0 - 2.0 * root_seven / 21.0)
    outer_root = math.sqrt(1.0 / 3.0 + 2.0 * root_seven / 21.0)
    points = (np.array([-1.0, -outer_root, -inner_root, inner_root, outer_root, 1.0]) + 1.0) / 2.0
    weights = (
        np.array(
            [
                1.0 / 15.0,
                (14.0 - root_seven) / 30.0,
                (14.0 + root_seven) / 30.0,
                (14.0 + root_seven) / 30.0,
                (14.0 - root_seven) / 30.0,
                1.0 / 15.0,
            ]
        )
        / 2.0
    )
    barycentric = np.array(
        [1.0 / np.prod([points[j] - points[k] for k in range(6) if k != j]) for j in range(6)]
    )
    derivative = np.zeros((6, 6))
    for i in range(6):
        for j in range(6):
            if i != j:
                derivative[i, j] = barycentric[j] / barycentric[i] / (points[i] - points[j])
        derivative[i, i] = -np.sum(derivative[i])
    halves = np.zeros((2, 6, 6))
    for which_half in range(2):
        targets = (points + which_half) / 2.0
        for i in range(6):
            for j in range(6):
                halves[which_half, i, j] = np.prod(
                    [(targets[i] - points[k]) / (points[j] - points[k]) for k in range(6) if k != j]
                )
    column_sums = np.sum(derivative * derivative * weights[:, None], axis=0)
    stiff_diag = (
        column_sums[:, None, None] * weights[None, :, None] * weights[None, None, :]
        + weights[:, None, None] * column_sums[None, :, None] * weights[None, None, :]
        + weights[:, None, None] * weights[None, :, None] * column_sums[None, None, :]
    )
    return (weights, derivative, halves, stiff_diag.reshape(216))


BF16 = jnp.bfloat16
F32 = jnp.float32


def split_np(matrix):
    high = np.asarray(matrix, np.float32).astype(BF16)
    low = (np.asarray(matrix, np.float64) - high.astype(np.float64)).astype(np.float32).astype(BF16)
    return high, low


def operators():
    weights, derivative, halves, stiff_diag = lobatto_tables()
    eye = np.eye(6)
    trace_rows = []
    for direction in range(6):
        axis_index = direction // 2
        layer_index = 5 * (direction % 2)
        orientation = 2.0 * (direction % 2) - 1.0
        for row in (eye[layer_index], orientation * derivative[layer_index]):
            factors = [eye, eye, eye]
            factors[axis_index] = row[None, :]
            trace_rows.append(np.kron(np.kron(factors[0], factors[1]), factors[2]))
    traces = np.concatenate(trace_rows, axis=0)
    stiff_1d = derivative.T @ (weights[:, None] * derivative)
    mass = np.diag(weights)
    stiffness = (
        np.kron(np.kron(stiff_1d, mass), mass)
        + np.kron(np.kron(mass, stiff_1d), mass)
        + np.kron(np.kron(mass, mass), stiff_1d)
    )
    blocks = []
    for sub in range(4):
        quarter = np.kron(halves[sub % 2], halves[sub // 2])
        blocks.append(np.kron(np.eye(2), quarter))
    return traces, stiffness, np.concatenate(blocks, axis=0), np.outer(weights, weights).reshape(36, 1), stiff_diag


def split(value):
    high = value.astype(BF16)
    return high, (value - high.astype(F32)).astype(BF16)


def dot(left, right):
    return jnp.dot(left, right, preferred_element_type=F32)


def dot3(left_high, left_low, right):
    high, low = split(right)
    return dot(left_high, high) + (dot(left_high, low) + dot(left_low, high))


def one_hot(index_row, rows, base=0):
    count = index_row.shape[1]
    position = lax.broadcasted_iota(jnp.int32, (rows, count), 0)
    return jnp.where(position == index_row - base, 1.0, 0.0).astype(BF16)


def pick(traces, elem, direction, sub, onto):
    wide = dot(traces, one_hot(elem, traces.shape[1]))
    face = jnp.zeros((72, elem.shape[1]), F32)
    for d in range(6):
        both = wide[72 * d : 72 * d + 72] + wide[432 + 72 * d : 432 + 72 * d + 72]
        face = jnp.where(direction == d, both, face)
    high, low = split(face)
    quarters = dot(onto, jnp.concatenate([high, low, high], axis=0))
    result = face
    for s in range(4):
        result = jnp.where(sub == s, quarters[72 * s : 72 * s + 72], result)
    return result


def send_kernel(x_ref, inv_ref, code_ref, mat_high, mat_low, onto_ref, out_ref, traces_ref):
    @pl.when(pl.program_id(0) == 0)
    def _():
        raw = dot3(mat_high[...], mat_low[...], x_ref[...])
        row = lax.broadcasted_iota(jnp.int32, raw.shape, 0)
        raw = jnp.where(lax.rem(row, 72) >= 36, raw * inv_ref[...], raw)
        high, low = split(raw)
        traces_ref[0:432] = high
        traces_ref[432:864] = low

    code = code_ref[...]
    picked = pick(traces_ref[...], code[0:1], code[1:2], code[2:3], onto_ref[...])
    capacity = out_ref.shape[2]
    for k in range(out_ref.shape[0]):
        out_ref[k] = picked[:, k * capacity : (k + 1) * capacity]


def exchange_kernel(
    steps, axis, width, src_ref, x_ref, traces_ref, code_ref, onto_ref, stiff_high, stiff_low,
    dst_ref, own_ref, near_ref, volume_ref, send_sem, recv_sem,
):
    count = lax.axis_size(axis)
    me = lax.axis_index(axis)
    barrier = pltpu.get_barrier_semaphore()
    peers = [lax.rem(me + step + count, count) for step in steps]
    for peer in peers:
        pl.semaphore_signal(barrier, inc=1, device_id=(peer,), device_id_type=pl.DeviceIdType.MESH)
    pl.semaphore_wait(barrier, len(steps))
    copies = []
    for k, peer in enumerate(peers):
        copy = pltpu.make_async_remote_copy(
            src_ref=src_ref.at[k],
            dst_ref=dst_ref.at[k],
            send_sem=send_sem.at[k],
            recv_sem=recv_sem.at[k],
            device_id=(peer,),
            device_id_type=pl.DeviceIdType.MESH,
        )
        copy.start()
        copies.append(copy)

    def step_tile(i, carry):
        part = pl.ds(pl.multiple_of(i * width, width), width)
        code = code_ref[:, part]
        own_ref[:, part] = pick(traces_ref[...], code[0:1], code[1:2], code[2:3], onto_ref[...])
        near_ref[:, part] = pick(traces_ref[...], code[3:4], code[4:5], code[5:6], onto_ref[...])
        return carry

    lax.fori_loop(0, code_ref.shape[1] // width, step_tile, 0)
    volume_ref[...] = dot3(stiff_high[...], stiff_low[...], x_ref[...])
    for copy in copies:
        copy.wait()


def norms_kernel(axis, sums_ref, out_ref, landing, send_sem, recv_sem):
    count = lax.axis_size(axis)
    me = lax.axis_index(axis)
    barrier = pltpu.get_barrier_semaphore()

    def greet(k, carry):
        peer = lax.rem(me + k, count)
        pl.semaphore_signal(barrier, inc=1, device_id=(peer,), device_id_type=pl.DeviceIdType.MESH)
        return carry

    def copy_to(k):
        return pltpu.make_async_remote_copy(
            src_ref=sums_ref,
            dst_ref=landing.at[k],
            send_sem=send_sem.at[k],
            recv_sem=recv_sem.at[k],
            device_id=(lax.rem(me + k, count),),
            device_id_type=pl.DeviceIdType.MESH,
        )

    def start(k, carry):
        copy_to(k).start()
        return carry

    def finish(k, carry):
        copy_to(k).wait()
        return carry

    lax.fori_loop(1, count, greet, 0)
    pl.semaphore_wait(barrier, count - 1)
    lax.fori_loop(1, count, start, 0)
    landing[0] = sums_ref[...]
    lax.fori_loop(1, count, finish, 0)

    def add(j, total):
        return total + landing[lax.rem(me + count - j, count)]

    total = lax.fori_loop(0, count, add, jnp.zeros(out_ref.shape, F32))
    out_ref[...] = jnp.broadcast_to(jnp.sum(total, axis=1, keepdims=True), out_ref.shape)


def apply_kernel(
    row_ref, coef_ref, x_ref, dirn_ref, rhs_ref, elem_ref, prec_ref, recv_ref, own_ref, near_ref,
    volume_ref, code_ref, rows_ref, size_ref, off_ref, weight_ref, lift_high, lift_low, prior_ref,
    x_out, dirn_out, sums_out, pool, total,
):
    peer_count = recv_ref.shape[0]

    @pl.when(pl.program_id(0) == 0)
    def _():
        for k in range(peer_count):
            high, low = split(recv_ref[k])
            pool[144 * k : 144 * k + 72] = high
            pool[144 * k + 72 : 144 * k + 144] = low
        total[...] = jnp.zeros_like(total)

    code = code_ref[...]
    direction, sub = code[1:2], code[2:3]
    bound = code[6:7] == -1
    width = sub.shape[1]
    own = own_ref[...]
    wide = dot(pool[...], one_hot(code[7:8], pool.shape[1]))
    partner = near_ref[...]
    for k in range(peer_count):
        both = wide[144 * k : 144 * k + 72] + wide[144 * k + 72 : 144 * k + 144]
        partner = jnp.where(code[6:7] == k, both, partner)
    own_value, own_slope = own[0:36], own[36:72]
    part_value = jnp.where(bound, 0.0, partner[0:36])
    part_slope = jnp.where(bound, -own_slope, partner[36:72])
    jump = own_value - part_value
    flux = 0.5 * (own_slope - part_slope)
    mortar = size_ref[0:1]
    area = mortar * mortar
    weight = weight_ref[...] * size_ref[1:2]
    term_value = weight * (PENALTY * mortar * jump - area * flux)
    term_slope = -weight * (jnp.where(bound, 1.0, 0.5) * area) * jump
    terms = jnp.concatenate([term_value, term_slope], axis=0)
    spread = jnp.concatenate([jnp.where(sub == s, terms, 0.0) for s in range(4)], axis=0)
    spread_high, spread_low = split(spread)
    back = dot(off_ref[...], jnp.concatenate([spread_high, spread_low, spread_high], axis=0))
    back = jnp.where(sub >= 4, terms, back)
    spread = jnp.concatenate([jnp.where(direction == d, back, 0.0) for d in range(6)], axis=0)
    wide_high, wide_low = split(spread)
    lanes = lax.broadcasted_iota(jnp.int32, (width, total.shape[1]), 1)
    hot = jnp.where(lanes == rows_ref[...], 1.0, 0.0).astype(BF16)
    total[...] += dot(wide_high, hot) + dot(wide_low, hot)

    @pl.when(pl.program_id(0) == pl.num_programs(0) - 1)
    def _():
        size, inv = elem_ref[0:1], elem_ref[1:2]
        field = x_ref[...]
        row = lax.broadcasted_iota(jnp.int32, total.shape, 0)
        faces = jnp.where(lax.rem(row, 72) >= 36, total[...] * inv, total[...])
        applied = size * volume_ref[...]
        applied = applied + dot3(lift_high[...], lift_low[...], faces)
        residual = jnp.where(size > 0.0, rhs_ref[...] - applied, 0.0)
        scaled = residual * (inv * prec_ref[...])
        step = coef_ref[0] * dirn_ref[...] + coef_ref[1] * scaled
        dirn_out[...] = step
        x_out[...] = field + step
        squares = jnp.sum(residual * residual, axis=0, keepdims=True)
        products = jnp.sum(residual * scaled, axis=0, keepdims=True)
        fold = lambda line: sum(line[:, k : k + 128] for k in range(0, line.shape[1], 128))
        row = lax.broadcasted_iota(jnp.int32, sums_out.shape, 0)
        row_index = row_ref[0]
        later = jnp.where(row == 2 * row_index + 1, fold(products), prior_ref[...])
        sums_out[...] = jnp.where(row == 2 * row_index, fold(squares), later)


def take_small(tables, index):
    rows = tables.shape[1] // 128
    fine = (jnp.arange(128, dtype=jnp.int32)[:, None] == (index % 128)[None, :]).astype(BF16)
    wide = jnp.dot(tables.reshape(-1, 128).astype(BF16), fine, preferred_element_type=F32)
    wide = wide.reshape(tables.shape[0], rows, -1)
    coarse = jnp.arange(rows, dtype=jnp.int32)[:, None] == (index // 128)[None, :]
    return jnp.sum(jnp.where(coarse[None], wide, 0.0), axis=1).astype(jnp.int32)


def tile(count):
    for width in (512, 256, 128):
        if count % width == 0:
            return width
    return count


def whole(shape):
    return pl.BlockSpec(shape, lambda i: (0,) * len(shape))


def general_path(
    rhs, start, spectrum_top, elem_code, rec_elem, rec_dir, rec_sub, rec_peer, rec_index, send_rec
):
    traces, stiffness, interp, face_weight, stiff_diag = operators()
    part_count = lax.axis_size("parts")
    own_index = lax.axis_index("parts")
    elem_count = rhs.shape[1]
    record_count = rec_elem.shape[0]
    capacity = send_rec.shape[0] // part_count
    far_reach = 2 * LD - 1
    code_float = elem_code.astype(F32)
    elem_size = 0.5 * code_float
    inv_size = jnp.where(elem_code > 0, 2.0 / jnp.maximum(code_float, 1.0), 0.0)
    elem_rows = jnp.stack([elem_size, inv_size])
    is_bound = rec_peer < 0
    is_local = rec_peer == own_index
    is_remote = jnp.logical_and(jnp.logical_not(is_bound), jnp.logical_not(is_local))
    offset = own_index - rec_peer
    position = jnp.where(offset < 0, offset + far_reach, offset + far_reach - 1)
    block = jnp.where(is_remote, position, jnp.where(is_bound, -1, -2))
    steps = list(range(-far_reach, 0)) + list(range(1, far_reach + 1))
    lists = send_rec.reshape(part_count, capacity)
    lists = jnp.concatenate([lists[part_count - far_reach :], lists, lists[:far_reach]], axis=0)
    lists = lax.dynamic_slice_in_dim(lists, own_index, 2 * far_reach + 1, 0)
    send_cols = jnp.concatenate([lists[:far_reach], lists[far_reach + 1 :]], axis=0).reshape(-1)
    send_count = send_cols.shape[0]

    own_size = 0.5 * take_small(elem_code[None], rec_elem)[0].astype(F32)
    mortar_size = jnp.where(rec_sub < 4, 0.5 * own_size, own_size)
    size_rows = jnp.stack([mortar_size, (rec_sub < 5).astype(F32)])
    tables = jnp.stack([rec_elem // 256, rec_elem % 256, rec_dir * 8 + rec_sub])
    found = take_small(tables, jnp.concatenate([send_cols, rec_index]))
    found = jnp.stack([found[0] * 256 + found[1], found[2] // 8, found[2] % 8])
    send_code = found[:, :send_count]
    near = jnp.where(is_local[None], found[:, send_count:], -1)
    rec_code = jnp.concatenate(
        [jnp.stack([rec_elem, rec_dir, rec_sub]), near, block[None], rec_index[None]],
        axis=0,
    )
    rec_rows = rec_elem[:, None]

    mat_high, mat_low = split_np(traces)
    lift_high, lift_low = split_np(traces.T)
    stiff_high, stiff_low = split_np(stiffness)
    onto_high, onto_low = split_np(interp)
    onto = np.concatenate([onto_high, onto_high, onto_low], axis=1)
    flat = np.concatenate([interp[72 * s : 72 * s + 72].T for s in range(4)], axis=1)
    off_high, off_low = split_np(flat)
    off = np.concatenate([off_high, off_high, off_low], axis=1)
    prec = jnp.asarray((1.0 / stiff_diag).reshape(216, 1), F32)
    weight = jnp.asarray(face_weight, F32)

    send_tile, rec_tile, peer_count = 2 * capacity, tile(record_count), len(steps)
    params = pltpu.CompilerParams(vmem_limit_bytes=60 * 1024 * 1024)
    field = (216, elem_count)

    def send_call(x):
        return pl.pallas_call(
            send_kernel,
            grid=(send_count // send_tile,),
            in_specs=[
                whole(field),
                whole((1, elem_count)),
                pl.BlockSpec((3, send_tile), lambda i: (0, i)),
                whole((432, 216)),
                whole((432, 216)),
                whole((288, 216)),
            ],
            out_specs=[pl.BlockSpec((2, 72, capacity), lambda i: (i, 0, 0)), whole((864, elem_count))],
            out_shape=[
                jax.ShapeDtypeStruct((peer_count, 72, capacity), F32),
                jax.ShapeDtypeStruct((864, elem_count), BF16),
            ],
            compiler_params=params,
            name="send_traces",
        )(x, inv_size[None], send_code, jnp.asarray(mat_high), jnp.asarray(mat_low), jnp.asarray(onto))

    vmem = pl.BlockSpec(memory_space=pltpu.VMEM)

    def exchange(outgoing, x, element_traces):
        return pl.pallas_call(
            functools.partial(exchange_kernel, steps, "parts", rec_tile),
            in_specs=[pl.BlockSpec(memory_space=pl.ANY)] + [vmem] * 6,
            out_specs=[pl.BlockSpec(memory_space=pl.ANY)] + [vmem] * 3,
            out_shape=[
                jax.ShapeDtypeStruct((peer_count, 72, capacity), F32),
                jax.ShapeDtypeStruct((72, record_count), F32),
                jax.ShapeDtypeStruct((72, record_count), F32),
                jax.ShapeDtypeStruct(field, F32),
            ],
            scratch_shapes=[
                pltpu.SemaphoreType.DMA((peer_count,)),
                pltpu.SemaphoreType.DMA((peer_count,)),
            ],
            compiler_params=pltpu.CompilerParams(
                collective_id=0, has_side_effects=True, vmem_limit_bytes=60 * 1024 * 1024
            ),
            name="exchange",
        )(
            outgoing, x, element_traces, rec_code, jnp.asarray(onto),
            jnp.asarray(stiff_high), jnp.asarray(stiff_low),
        )

    def all_sums(sums):
        return pl.pallas_call(
            functools.partial(norms_kernel, "parts"),
            in_specs=[vmem],
            out_specs=vmem,
            out_shape=jax.ShapeDtypeStruct((8, 128), F32),
            scratch_shapes=[
                pltpu.VMEM((part_count, 8, 128), F32),
                pltpu.SemaphoreType.DMA((part_count,)),
                pltpu.SemaphoreType.DMA((part_count,)),
            ],
            compiler_params=pltpu.CompilerParams(collective_id=1, has_side_effects=True),
            name="all_sums",
        )(sums)

    def apply_call(row_index, coef, x, dirn, received, own, near_traces, volume, sums):
        tiles = lambda rows: pl.BlockSpec((rows, rec_tile), lambda i: (0, i))
        return pl.pallas_call(
            apply_kernel,
            grid=(record_count // rec_tile,),
            in_specs=[
                pl.BlockSpec(memory_space=pltpu.SMEM),
                pl.BlockSpec(memory_space=pltpu.SMEM),
                whole(field),
                whole(field),
                whole(field),
                whole((2, elem_count)),
                whole((216, 1)),
                whole((peer_count, 72, capacity)),
                tiles(72),
                tiles(72),
                whole(field),
                tiles(8),
                pl.BlockSpec((rec_tile, 1), lambda i: (i, 0)),
                tiles(2),
                whole((72, 864)),
                whole((36, 1)),
                whole((216, 432)),
                whole((216, 432)),
                whole((8, 128)),
            ],
            out_specs=[whole(field), whole(field), whole((8, 128))],
            out_shape=[
                jax.ShapeDtypeStruct(field, F32),
                jax.ShapeDtypeStruct(field, F32),
                jax.ShapeDtypeStruct((8, 128), F32),
            ],
            scratch_shapes=[
                pltpu.VMEM((144 * peer_count, capacity), BF16),
                pltpu.VMEM((432, elem_count), F32),
            ],
            compiler_params=params,
            name="apply_operator",
        )(
            row_index[None], coef, x, dirn, rhs, elem_rows, prec, received, own, near_traces, volume, rec_code, rec_rows,
            size_rows, jnp.asarray(off), weight, jnp.asarray(lift_high), jnp.asarray(lift_low), sums,
        )

    scale_total = 216.0 * elem_count * part_count
    top_value = spectrum_top[0]
    bottom = top_value / BOTTOM_RATIO
    center = 0.5 * (top_value + bottom)
    radius = 0.5 * (top_value - bottom)
    sigma_ratio = center / radius
    rho_prev = 1.0 / sigma_ratio
    coefs = [jnp.stack([jnp.zeros_like(center), 1.0 / center])]
    for step_index in range(1, ITERS):
        rho_next = 1.0 / (2.0 * sigma_ratio - rho_prev)
        coefs.append(jnp.stack([rho_next * rho_prev, 2.0 * rho_next / radius]))
        rho_prev = rho_next
    coefs = jnp.stack(coefs)

    def one_step(step_index, state):
        x, dirn, sums = state
        outgoing, element_traces = send_call(x)
        moved = exchange(outgoing, x, element_traces)
        coef = lax.dynamic_index_in_dim(coefs, step_index, 0, False)
        return tuple(apply_call(step_index, coef, x, dirn, *moved, sums))

    x, dirn, sums = lax.fori_loop(0, ITERS, one_step, (start, start, jnp.zeros((8, 128), F32)))
    norms = 0.5 * jnp.log(all_sums(sums)[: 2 * ITERS, 0].reshape(ITERS, 2) / scale_total)
    return (x, norms)


LATERAL = 128
FIELDS = 9


def iota(shape, axis):
    return lax.broadcasted_iota(jnp.int32, shape, axis)


def sum_rows(value):
    return jnp.sum(value, axis=0, keepdims=True)


def total_of(value):
    return jnp.sum(value, axis=1, keepdims=True)


def look_up(tables, rows, index):
    hot = jnp.where(iota((128, index.shape[1]), 0) == (index & 127), 1.0, 0.0).astype(BF16)
    wide = dot(tables, hot)
    mask = iota((rows, index.shape[1]), 0) == (index >> 7)
    count = tables.shape[0] // rows
    return [sum_rows(jnp.where(mask, wide[k * rows : (k + 1) * rows], 0.0)) for k in range(count)]


def regroup(columns, position, rows):
    mask = iota((rows, position.shape[1]), 0) == (position >> 7)
    left = jnp.concatenate([jnp.where(mask, column, 0.0) for column in columns], axis=0).astype(BF16)
    hot = jnp.where(iota((128, position.shape[1]), 0) == (position & 127), 1.0, 0.0).astype(BF16)
    return lax.dot_general(left, hot, (((1,), (1,)), ((), ())), preferred_element_type=F32)


def setup_kernel(
    axis, capacity, code_ref, elem_ref, dir_ref, sub_ref, peer_ref, index_ref,
    code_line, elem_line, dir_line, sub_line, peer_line, index_line, lists_ref,
    rows_ref, col_ref, send_ref, flag_ref, elem_out,
):
    me = lax.axis_index(axis)
    count = lax.axis_size(axis)
    group, place = me // LD, lax.rem(me, LD)
    elem, direction, sub = elem_line[...], dir_line[...], sub_line[...]
    peer, index = peer_line[...], index_line[...]
    records, slots = elem.shape[1], code_line.shape[1]
    chunks, table_rows, slot_rows = records // 128, records // 128, 6 * slots // 128
    used = sub < 5
    local = used & (peer == me)
    bound = used & (peer < 0)
    remote = used & (peer >= 0) & (peer != me)

    kind = jnp.where(used, jnp.where(remote, direction, direction + 8), -1)
    member = jnp.where(iota((16, records), 0) == kind, 1.0, 0.0)
    stacked = jnp.concatenate([member[:, 128 * k : 128 * k + 128] for k in range(chunks)], axis=0)
    upper = jnp.where(iota((128, 128), 0) < iota((128, 128), 1), 1.0, 0.0)
    counted = dot(
        stacked.astype(BF16), jnp.concatenate([upper, jnp.ones((128, 128), F32)], axis=1).astype(BF16)
    )
    carry = jnp.zeros((16, 128), F32)
    before = []
    for k in range(chunks):
        before.append(counted[16 * k : 16 * k + 16, :128] + carry)
        carry = carry + counted[16 * k : 16 * k + 16, 128:]
    base = jnp.concatenate([jnp.zeros((8, 128), F32), carry[:8]], axis=0)
    before = jnp.concatenate([part + base for part in before], axis=1)
    rank = sum_rows(before * member).astype(jnp.int32)
    in_range = used & (rank < slots)
    slot = jnp.where(in_range, direction * slots + rank, -1)

    tables = jnp.concatenate(
        [
            (elem_ref[...] & 127).astype(F32),
            ((elem_ref[...] >> 7) * 8 + sub_ref[...]).astype(F32),
            dir_ref[...].astype(F32),
        ],
        axis=0,
    ).astype(BF16)
    rows_per = capacity // 128
    list_rows = iota(lists_ref.shape, 0)
    lists = lists_ref[...].astype(F32)
    channel = []
    for d, other in ((1, group + 1), (0, group - 1)):
        here = remote & (direction == d)
        most = jnp.max(jnp.where(here, peer, -1), axis=1, keepdims=True)
        least = jnp.min(jnp.where(here, peer, count), axis=1, keepdims=True)
        wrong = here & (peer // LD != other)
        channel.append((most, jnp.where((most >= 0) & (most != least), 1.0, 0.0), wrong))
    wanted = []
    for most, _, _ in channel:
        for part in range(rows_per):
            wanted.append(sum_rows(jnp.where(list_rows == most * rows_per + part, lists, 0.0)))
    for pos in range(LD - 1):
        dest = group * LD + lax.rem(place + pos + 1, LD)
        wanted.append(sum_rows(jnp.where(list_rows == dest * rows_per, lists, 0.0)))
    wanted.append(jnp.zeros((1, LATERAL), F32))
    wanted = jnp.concatenate(wanted, axis=1).astype(jnp.int32)
    wanted_count = wanted.shape[1]
    low, high, found_dir = look_up(tables, table_rows, jnp.concatenate([wanted, index], axis=1))
    high = high.astype(jnp.int32)
    found_elem = low.astype(jnp.int32) + 128 * (high >> 3)
    found_sub = high & 7
    send_ref[0:1] = found_elem[:, :wanted_count]
    send_ref[1:2] = found_dir[:, :wanted_count].astype(jnp.int32)
    send_ref[2:3] = found_sub[:, :wanted_count]
    send_ref[3:8] = jnp.zeros((5, wanted_count), jnp.int32)
    near_elem, near_sub = found_elem[:, wanted_count:], found_sub[:, wanted_count:]

    code_rows = -(-slots // 1024) * 8
    code_table = code_ref[...].astype(F32)
    if code_rows > code_table.shape[0]:
        pad = jnp.zeros((code_rows - code_table.shape[0], 128), F32)
        code_table = jnp.concatenate([code_table, pad], axis=0)
    code = look_up(code_table.astype(BF16), code_rows, elem)[0]
    size = 0.5 * code
    mortar = jnp.where(sub < 4, 0.5 * size, size)

    turn = lax.rem(place - lax.rem(peer, LD) + LD, LD) - 1
    landed = jnp.where(direction < 2, index, turn * LATERAL + index)
    split_near = jnp.where(sub < 4, sub, jnp.where(near_sub < 4, near_sub + 4, 8))
    split_far = jnp.minimum(sub, 4)
    real = lambda value: value.astype(F32)
    columns = [
        real(elem & 127),
        real((elem >> 7) + 1),
        real(near_elem & 127),
        jnp.where(local, real((near_elem >> 7) + 1), 0.0),
        jnp.where(remote, real(landed & 127), 0.0),
        jnp.where(remote, real((landed >> 7) + 1), 0.0),
        real(split_near),
        real(split_far),
        mortar,
    ]
    moved = regroup(columns, slot, slot_rows)
    part = lambda k: moved[k * slot_rows : (k + 1) * slot_rows]
    join = lambda k: jnp.where(part(k + 1) > 0.0, part(k) + 128.0 * (part(k + 1) - 1.0), -1.0)
    own = join(0)
    spare = col_ref.shape[1] - slot_rows
    own_all = jnp.concatenate([own, jnp.zeros((spare, 128), F32)], axis=0)
    col_ref[...] = jnp.transpose(own_all).astype(jnp.int32)
    mort = part(8)
    fields = [join(2), join(4), part(6), part(7), 36.0 * mort, 0.5 * mort * mort]

    face = jnp.where(used, direction * slots + elem, -1)
    marks = [jnp.where(used & (sub == s), 1.0, 0.0) for s in range(5)]
    marks.append(jnp.where(bound & (sub == 4), 1.0, 0.0))
    tally = regroup(marks, face, slot_rows)
    fields += [tally[k * slot_rows : (k + 1) * slot_rows] for k in range(6)]
    per = slots // 128
    lines = []
    for value in fields:
        pieces = []
        for d in range(6):
            pieces.append(
                jnp.concatenate([value[per * d + q : per * d + q + 1] for q in range(per)], axis=1)
            )
        pieces.append(jnp.zeros((2, slots), F32))
        lines.append(jnp.concatenate(pieces, axis=0))
    code_all = code_line[...].astype(F32)
    size_all = 0.5 * code_all
    inv_all = jnp.where(code_all > 0.0, 2.0 / jnp.maximum(code_all, 1.0), 0.0)
    elem_out[0:1] = size_all
    elem_out[1:2] = inv_all
    elem_out[2:8] = jnp.zeros((6, slots), F32)
    half = 0.5 * size_all
    counts, bounds = lines[6:11], lines[11]
    lines = lines[:6]
    for s in range(5):
        lines.append(36.0 * (half if s < 4 else size_all) * counts[s])
    for s in range(4):
        lines.append(half * half * (0.5 * counts[s]))
    lines.append(size_all * size_all * (0.5 * (counts[4] + bounds)))
    for k, line in enumerate(lines):
        rows_ref[8 * k : 8 * k + 8] = line
    rows_ref[8 * len(lines) :] = jnp.zeros((rows_ref.shape[0] - 8 * len(lines), slots), F32)

    wrong = jnp.where(remote & (direction >= 2) & ((peer // LD != group) | (index >= LATERAL)), 1.0, 0.0)
    wrong = wrong + jnp.where(bound & (sub < 4), 1.0, 0.0)
    wrong = wrong + jnp.where(local & (sub < 4) & (near_sub < 4), 1.0, 0.0)
    wrong = wrong + jnp.where(used & (rank >= slots), 1.0, 0.0)
    for _, _, off in channel:
        wrong = wrong + jnp.where(off, 1.0, 0.0)
    faults = total_of(wrong) + channel[0][1] + channel[1][1]
    row = iota((8, 128), 0)
    allowed = jnp.where(row < 2, float(capacity), float(LATERAL))
    over = jnp.where((row < 6) & (carry[:8] > allowed), 1.0, 0.0)
    faults = faults + total_of(sum_rows(over))
    turns = [
        lax.rem(place - lax.rem(jnp.maximum(most, 0), LD) + LD, LD).astype(F32) for most, _, _ in channel
    ]
    ahead = [
        jnp.where(most >= 0, lax.rem(jnp.maximum(most, 0) % LD - place + LD, LD), -1).astype(F32)
        for most, _, _ in channel
    ]
    flags = jnp.where(row == 0, faults, jnp.where(row == 1, turns[1], turns[0]))
    flag_ref[...] = jnp.where(row == 3, ahead[0], jnp.where(row == 4, ahead[1], flags))


def stack2(value):
    high = value.astype(BF16).astype(F32)
    return jnp.concatenate([high, value - high], axis=0).astype(BF16)


def stack3(value):
    high = value.astype(BF16).astype(F32)
    return jnp.concatenate([high, value - high, high], axis=0).astype(BF16)


def fold_pair(value):
    half = value.shape[0] // 2
    return value[:half] + value[half:]


def choose(blocks, rows, code):
    last = blocks.shape[0] // rows - 1
    result = blocks[last * rows :]
    for q in range(last):
        result = jnp.where(code == q, blocks[q * rows : q * rows + rows], result)
    return result


def main_kernel(
    axis, iters, capacity,
    x_ref, rhs_hbm, top_ref, rows_ref, col_ref, send_ref, flag_ref, elem_ref, prec_ref,
    trace_high_hbm, trace_low_hbm, stiff_high_hbm, stiff_low_hbm, lift_high_hbm, lift_low_hbm,
    onto_hbm, own_hbm, near_hbm, far_hbm,
    x_out, norm_out,
    rhs_ref, trace_high, trace_low, stiff_high, stiff_low, lift_high, lift_low,
    onto_ref, own_ref, near_ref, far_ref, load_sem,
    dirn, volume, traces, pairs, faces, scatter, gather, gather_chan, gather_lat, send_chan, send_lat,
    far_rows, coefs, snd_chan, snd_lat, snd_pass, kept_pass, rcv_chan, rcv_lat, rcv_pass, sums, landing,
    send_sem, recv_sem, sum_send, sum_recv,
):
    count = lax.axis_size(axis)
    me = lax.axis_index(axis)
    group, place = me // LD, lax.rem(me, LD)
    groups = count // LD
    slots, half = x_ref.shape[1], capacity // 2
    mesh_id = pl.DeviceIdType.MESH
    barrier = pltpu.get_barrier_semaphore()

    def greet(k, carry):
        peer = lax.rem(me + k, count)
        pl.semaphore_signal(barrier, inc=1, device_id=(peer,), device_id_type=mesh_id)
        return carry

    lax.fori_loop(1, count, greet, 0)
    held = [
        (x_ref, x_out),
        (trace_high_hbm, trace_high),
        (trace_low_hbm, trace_low),
        (onto_hbm, onto_ref),
        (stiff_high_hbm, stiff_high),
        (stiff_low_hbm, stiff_low),
        (own_hbm, own_ref),
        (near_hbm, near_ref),
        (far_hbm, far_ref),
        (lift_high_hbm, lift_high),
        (lift_low_hbm, lift_low),
        (rhs_hbm, rhs_ref),
    ]
    loads = [pltpu.make_async_copy(src, dst, load_sem.at[k]) for k, (src, dst) in enumerate(held)]
    for load in loads:
        load.start()

    def hot(mask):
        return jnp.where(mask, 1.0, 0.0).astype(BF16)

    per = slots // 128
    columns = col_ref[...]
    for d in range(6):
        line = rows_ref[d : d + 1].astype(jnp.int32)
        gather[d] = hot(iota((slots, slots), 0) == line)
        for q in range(per):
            column = columns[:, per * d + q : per * d + q + 1]
            scatter[d, 128 * q : 128 * q + 128] = hot(iota((128, slots), 1) == column)
        line = rows_ref[8 + d : 9 + d].astype(jnp.int32)
        if d < 2:
            gather_chan[d] = hot(iota((capacity, capacity), 0) == line[:, :capacity])
        else:
            gather_lat[d - 2] = hot(iota((LD * LATERAL, LATERAL), 0) == line[:, :LATERAL])
    size, inv = elem_ref[0:1], elem_ref[1:2]
    def across(side, turn):
        other = lax.rem(group + (1 if side == 0 else groups - 1), groups)
        return (other * LD + lax.rem(place + turn, LD),)

    send_elem = send_ref[0:1]
    send_chan[0] = hot(iota((slots, capacity), 0) == send_elem[:, :capacity])
    send_chan[1] = hot(iota((slots, capacity), 0) == send_elem[:, capacity : 2 * capacity])
    send_lat[...] = hot(iota((slots, LD * LATERAL), 0) == send_elem[:, 2 * capacity :])
    chosen = jnp.zeros(far_rows.shape, F32)
    for k, field in enumerate((3, 4, 5)):
        block = rows_ref[8 * field : 8 * field + 8]
        pieces = []
        for d in range(6):
            part = block[:, : capacity if d < 2 else LATERAL]
            pieces.append(sum_rows(jnp.where(iota(part.shape, 0) == d, part, 0.0)))
        chosen = jnp.where(iota(chosen.shape, 0) == k, jnp.concatenate(pieces, axis=1), chosen)
    far_rows[...] = chosen

    line = jnp.ones((1, 128), F32)
    top = top_ref[0] * line
    bottom = top / BOTTOM_RATIO
    center = 0.5 * (top + bottom)
    radius = 0.5 * (top - bottom)
    sigma = center / radius
    rho = 1.0 / sigma
    coefs[0:1] = 0.0 * line
    coefs[1:2] = 1.0 / center
    for k in range(1, iters):
        rho_next = 1.0 / (2.0 * sigma - rho)
        coefs[2 * k : 2 * k + 1] = rho_next * rho
        coefs[2 * k + 1 : 2 * k + 2] = 2.0 * rho_next / radius
        rho = rho_next
    dirn[...] = jnp.zeros_like(dirn)
    sums[...] = jnp.where(iota(sums.shape, 0) == 2 * iters, flag_ref[0:1], 0.0) * jnp.where(
        iota(sums.shape, 1) == 0, 1.0, 0.0
    )

    for load in loads:
        load.wait()
    pl.semaphore_wait(barrier, count - 1)

    def step(it, carry):
        field = x_out[...]
        field_high, field_low = split(field)

        def trace(first, last):
            high, low = trace_high[first:last], trace_low[first:last]
            raw = dot(high, field_high) + (dot(high, field_low) + dot(low, field_high))
            raw = jnp.where(lax.rem(iota(raw.shape, 0), 72) >= 36, raw * inv, raw)
            traces[first:last] = raw
            for d in range(first // 72, last // 72):
                pairs[d] = stack2(raw[72 * d - first : 72 * d + 72 - first])

        trace(0, 144)
        outgoing = jnp.concatenate(
            [fold_pair(dot(pairs[1], send_chan[0])), fold_pair(dot(pairs[0], send_chan[1]))], axis=1
        )
        outgoing = choose(dot(onto_ref[...], stack3(outgoing)), 80, send_ref[2:3, : 2 * capacity])
        spare = iota((40, half), 0) >= 36
        for side in range(2):
            ahead = flag_ref[3 + side : 4 + side, 0:1]
            for turn in range(LD):
                low, left = 40 * (turn // 2), side * capacity + half * (turn % 2)
                snd_chan[side, turn] = jnp.where(spare, ahead, outgoing[low : low + 40, left : left + half])

        def send(source, target, k, place_of):
            return pltpu.make_async_remote_copy(
                src_ref=source,
                dst_ref=target,
                send_sem=send_sem.at[it, k],
                recv_sem=recv_sem.at[it, k],
                device_id=place_of,
                device_id_type=mesh_id,
            )

        def beside(turn):
            return (group * LD + lax.rem(place + turn, LD),)

        pairs_of = [(side, turn) for side in range(2) for turn in range(LD)]
        channel = [
            send(snd_chan.at[side, turn], rcv_chan.at[it, side, turn], side * LD + turn, across(side, turn))
            for side, turn in pairs_of
        ]
        lateral = [
            send(snd_lat.at[pos], rcv_lat.at[it, pos], 2 * LD + pos, beside(pos + 1)) for pos in range(LD - 1)
        ]
        passed = [
            send(
                snd_pass.at[side, turn - 1],
                rcv_pass.at[it, side, turn - 1],
                (3 + side) * LD + turn - 1,
                beside(turn),
            )
            for side, turn in pairs_of
            if turn
        ]
        for copy in channel:
            copy.start()

        trace(144, 432)
        send_dir = send_ref[1:2, 2 * capacity :]
        outgoing = jnp.zeros((72, LD * LATERAL), F32)
        for d in range(2, 6):
            outgoing = jnp.where(send_dir == d, fold_pair(dot(pairs[d], send_lat[...])), outgoing)
        outgoing = choose(dot(onto_ref[...], stack3(outgoing)), 80, send_ref[2:3, 2 * capacity :])
        for pos in range(LD - 1):
            snd_lat[pos] = outgoing[:, pos * LATERAL : (pos + 1) * LATERAL]
        for copy in lateral:
            copy.start()

        volume[...] = dot3(stiff_high[...], stiff_low[...], field) * size

        def local_faces(d, inner):
            line = lambda k: rows_ref[pl.ds(8 * k + d, 1)]
            mass = dot(own_ref[...], stack3(traces[pl.ds(pl.multiple_of(72 * d, 8), 72)]))
            value = jnp.zeros((40, slots), F32)
            slope = jnp.zeros((40, slots), F32)
            for s in range(5):
                mass_value, mass_slope = mass[80 * s : 80 * s + 40], mass[80 * s + 40 : 80 * s + 80]
                flux = line(11 + s)
                value = value + (line(6 + s) * mass_value - flux * mass_slope)
                slope = slope - flux * mass_value
            facing = d + 1 - 2 * lax.rem(d, 2)
            found = fold_pair(dot(pairs[facing], gather[d]))
            found = choose(dot(near_ref[...], stack3(found)), 80, line(2).astype(jnp.int32))
            jump, flux = line(4), line(5)
            terms = jnp.concatenate([flux * found[40:] - jump * found[:40], flux * found[:40]], axis=0)
            back = fold_pair(dot(stack2(terms), scatter[d]))
            faces[pl.ds(pl.multiple_of(80 * d, 8), 80)] = back + jnp.concatenate([value, slope], axis=0)
            return inner

        lax.fori_loop(2, 6, local_faces, 0)
        for copy in channel:
            copy.wait()
        for side in range(2):
            for turn in range(LD):
                chunk = jnp.zeros((40, half), F32)
                for k in range(LD):
                    mine = rcv_chan[it, side, k][36:37, 0:1] == float((turn + k) % LD)
                    chunk = jnp.where(mine, rcv_chan[it, side, k], chunk)
                if turn:
                    snd_pass[side, turn - 1] = chunk
                else:
                    kept_pass[side] = chunk
        for copy in passed:
            copy.start()
        lax.fori_loop(0, 2, local_faces, 0)
        for copy in lateral:
            copy.wait()

        def add_far(pieces, first, last, width):
            found = jnp.concatenate(pieces, axis=1)
            left = first * capacity if first < 2 else 2 * capacity
            part = slice(left, left + width * (last - first))
            found = choose(dot(far_ref[...], stack3(found)), 80, far_rows[0:1, part].astype(jnp.int32))
            jump, flux = far_rows[1:2, part], far_rows[2:3, part]
            terms = stack2(
                jnp.concatenate([flux * found[40:] - jump * found[:40], flux * found[:40]], axis=0)
            )
            for d in range(first, last):
                start = (d - first) * width
                faces[80 * d : 80 * d + 80] += fold_pair(
                    dot(terms[:, start : start + width], scatter[d, :width])
                )

        def lifted(first, last):
            total = faces[80 * first : 80 * last]
            total = jnp.where(lax.rem(iota(total.shape, 0), 80) >= 40, total * inv, total)
            high, low = split(total)
            left, rest = lift_high[:, 80 * first : 80 * last], lift_low[:, 80 * first : 80 * last]
            return dot(left, high) + (dot(left, low) + dot(rest, high))

        sides = [rcv_lat[it, pos] for pos in range(LD - 1)] + [jnp.zeros((80, LATERAL), F32)]
        got = stack2(jnp.concatenate(sides, axis=1))
        add_far([fold_pair(dot(got, gather_lat[d])) for d in range(4)], 2, 6, LATERAL)
        volume[...] += lifted(2, 6)
        for copy in passed:
            copy.wait()

        pieces = []
        for side in range(2):
            turn = flag_ref[side + 1 : side + 2, 0:1]
            landed = [kept_pass[side]] + [rcv_pass[it, side, k] for k in range(LD - 1)]
            chunks = []
            for k in range(LD):
                chunk = landed[(-k) % LD]
                for t in range(1, LD):
                    chunk = jnp.where(turn == float(t), landed[(t - k) % LD], chunk)
                chunks.append(chunk)
            got = jnp.concatenate(
                [jnp.concatenate(chunks[:2], axis=1), jnp.concatenate(chunks[2:], axis=1)], axis=0
            )
            pieces.append(fold_pair(dot(stack2(got), gather_chan[side])))
        add_far(pieces, 0, 2, capacity)
        applied = volume[...] + lifted(0, 2)
        residual = jnp.where(size > 0.0, rhs_ref[...] - applied, 0.0)
        scaled = residual * (inv * prec_ref[...])
        first = coefs[pl.ds(2 * it, 1), 0:1]
        second = coefs[pl.ds(2 * it + 1, 1), 0:1]
        change = first * dirn[...] + second * scaled
        dirn[...] = change
        x_out[...] = field + change
        squares = sum_rows(residual * residual)
        products = sum_rows(residual * scaled)
        fold = lambda row: sum(row[:, k : k + 128] for k in range(0, row.shape[1], 128))
        row = iota(sums.shape, 0)
        kept = jnp.where(row == 2 * it + 1, fold(products), sums[...])
        sums[...] = jnp.where(row == 2 * it, fold(squares), kept)
        return carry

    lax.fori_loop(0, iters, step, 0)

    def copy_to(k):
        return pltpu.make_async_remote_copy(
            src_ref=sums,
            dst_ref=landing.at[k],
            send_sem=sum_send.at[k],
            recv_sem=sum_recv.at[k],
            device_id=(lax.rem(me + k, count),),
            device_id_type=mesh_id,
        )

    def begin(k, carry):
        copy_to(k).start()
        return carry

    def finish(k, carry):
        copy_to(k).wait()
        return carry

    def add(j, total):
        return total + landing[lax.rem(me + count - j, count)]

    lax.fori_loop(1, count, begin, 0)
    landing[0] = sums[...]
    lax.fori_loop(1, count, finish, 0)
    total = total_of(lax.fori_loop(0, count, add, jnp.zeros(sums.shape, F32)))
    mean = total / (216.0 * slots * count)
    logs = 0.5 * jnp.log(jnp.where(iota(total.shape, 0) < 2 * iters, mean, 1.0))
    shown = jnp.where(iota(total.shape, 0) < 2 * iters, logs, total)
    norm_out[...] = jnp.broadcast_to(shown, norm_out.shape)


def wide_rows(blocks):
    padded = []
    for block in blocks:
        rows = np.zeros((80, block.shape[1]))
        rows[0:36], rows[40:76] = block[0:36], block[36:72]
        padded.append(rows)
    return np.concatenate(padded, axis=0)


def three(matrix):
    high, low = split_np(matrix)
    return np.concatenate([high, high, low], axis=1)


def set_up(slots, capacity, arrays, send_rec):
    slot_rows = 6 * slots // 128
    to_lines = lambda array: array.reshape(-1, 128)
    to_line = lambda array: array.reshape(1, -1)
    vmem = pl.BlockSpec(memory_space=pltpu.VMEM)
    columns = 2 * capacity + LD * LATERAL
    return pl.pallas_call(
        functools.partial(setup_kernel, "parts", capacity),
        in_specs=[vmem] * 13,
        out_specs=[vmem] * 5,
        out_shape=[
            jax.ShapeDtypeStruct((136, slots), F32),
            jax.ShapeDtypeStruct((128, 128 * -(-slot_rows // 128)), jnp.int32),
            jax.ShapeDtypeStruct((8, columns), jnp.int32),
            jax.ShapeDtypeStruct((8, 128), F32),
            jax.ShapeDtypeStruct((8, slots), F32),
        ],
        compiler_params=pltpu.CompilerParams(vmem_limit_bytes=60 * 1024 * 1024),
        name="set_up",
    )(*map(to_lines, arrays), *map(to_line, arrays), to_lines(send_rec))


def fast_path(
    rhs, start, spectrum_top, elem_code, rec_elem, rec_dir, rec_sub, rec_peer, rec_index, send_rec
):
    traces, stiffness, interp, face_weight, stiff_diag = operators()
    part_count = lax.axis_size("parts")
    slots = rhs.shape[1]
    capacity = send_rec.shape[0] // part_count
    arrays = (elem_code, rec_elem, rec_dir, rec_sub, rec_peer, rec_index)
    vmem = pl.BlockSpec(memory_space=pltpu.VMEM)
    rows, col, send, flag, elem = set_up(slots, capacity, arrays, send_rec)

    weight = np.concatenate([face_weight, face_weight], axis=0)
    quarters = [interp[72 * s : 72 * s + 72] for s in range(4)]
    eye = np.eye(72)
    onto = three(wide_rows(quarters + [eye]))
    own = three(wide_rows([j.T @ (weight * j) for j in quarters] + [weight * eye]))
    back = [j.T * weight.T for j in quarters]
    near = three(wide_rows(back + [weight * j for j in quarters] + [weight * eye]))
    far = wide_rows(back + [weight * eye])
    far = three(wide_rows([far.T]).T)
    trace_high, trace_low = split_np(traces)
    stiff_high, stiff_low = split_np(stiffness)
    lift = np.zeros((216, 480))
    for d in range(6):
        lift[:, 80 * d : 80 * d + 36] = traces.T[:, 72 * d : 72 * d + 36]
        lift[:, 80 * d + 40 : 80 * d + 76] = traces.T[:, 72 * d + 36 : 72 * d + 72]
    lift_high, lift_low = split_np(lift)
    prec = (1.0 / stiff_diag).reshape(216, 1).astype(np.float32)
    constants = (
        prec, trace_high, trace_low, stiff_high, stiff_low, lift_high, lift_low, onto, own, near, far
    )
    copies, half = 5 * LD, capacity // 2
    hbm = pl.BlockSpec(memory_space=pltpu.HBM)
    x, shown = pl.pallas_call(
        functools.partial(main_kernel, "parts", ITERS, capacity),
        in_specs=[hbm] * 2 + [pl.BlockSpec(memory_space=pltpu.SMEM)] + [vmem] * 6 + [hbm] * 10,
        out_specs=[vmem] * 2,
        out_shape=[jax.ShapeDtypeStruct((216, slots), F32), jax.ShapeDtypeStruct((8, 128), F32)],
        scratch_shapes=[
            pltpu.VMEM((216, slots), F32),
            *[pltpu.VMEM(array.shape, BF16) for array in constants[1:]],
            pltpu.SemaphoreType.DMA((12,)),
            pltpu.VMEM((216, slots), F32),
            pltpu.VMEM((216, slots), F32),
            pltpu.VMEM((432, slots), F32),
            pltpu.VMEM((6, 144, slots), BF16),
            pltpu.VMEM((480, slots), F32),
            pltpu.VMEM((6, slots, slots), BF16),
            pltpu.VMEM((6, slots, slots), BF16),
            pltpu.VMEM((2, capacity, capacity), BF16),
            pltpu.VMEM((4, LD * LATERAL, LATERAL), BF16),
            pltpu.VMEM((2, slots, capacity), BF16),
            pltpu.VMEM((slots, LD * LATERAL), BF16),
            pltpu.VMEM((8, 2 * capacity + 4 * LATERAL), F32),
            pltpu.VMEM((16, 128), F32),
            pltpu.VMEM((2, LD, 40, half), F32),
            pltpu.VMEM((LD - 1, 80, LATERAL), F32),
            pltpu.VMEM((2, LD - 1, 40, half), F32),
            pltpu.VMEM((2, 40, half), F32),
            pltpu.VMEM((ITERS, 2, LD, 40, half), F32),
            pltpu.VMEM((ITERS, LD - 1, 80, LATERAL), F32),
            pltpu.VMEM((ITERS, 2, LD - 1, 40, half), F32),
            pltpu.VMEM((8, 128), F32),
            pltpu.VMEM((part_count, 8, 128), F32),
            pltpu.SemaphoreType.DMA((ITERS, copies)),
            pltpu.SemaphoreType.DMA((ITERS, copies)),
            pltpu.SemaphoreType.DMA((part_count,)),
            pltpu.SemaphoreType.DMA((part_count,)),
        ],
        compiler_params=pltpu.CompilerParams(
            collective_id=2, has_side_effects=True, vmem_limit_bytes=60 * 1024 * 1024
        ),
        name="smooth",
    )(
        start, rhs, spectrum_top, rows, col, send, flag, elem, *map(jnp.asarray, constants)
    )
    return x, shown


def on_device(*arguments):
    rhs, send_rec, rec_elem = arguments[0], arguments[9], arguments[4]
    part_count = lax.axis_size("parts")
    capacity, slots = send_rec.shape[0] // part_count, rhs.shape[1]
    suits = slots % 128 == 0 and rec_elem.shape[0] % 1024 == 0 and capacity % 256 == 0
    suits = suits and capacity <= slots <= 4096 and part_count % LD == 0 and part_count >= 3 * LD
    if not suits:
        return general_path(*arguments)
    x, shown = fast_path(*arguments)
    norms = shown[: 2 * ITERS, 0].reshape(ITERS, 2)
    return lax.cond(
        shown[2 * ITERS, 0] > 0.0, lambda: general_path(*arguments), lambda: (x, norms)
    )


def solution(mesh):
    placed = (
        P(None, "parts"),
        P(None, "parts"),
        P(),
        P("parts"),
        P("parts"),
        P("parts"),
        P("parts"),
        P("parts"),
        P("parts"),
        P("parts"),
    )
    return jax.shard_map(
        on_device, mesh=mesh, in_specs=placed, out_specs=(P(None, "parts"), P()), check_vma=False
    )
```

```python
import functools
import math

import jax
import jax.numpy as jnp
import numpy as np
from jax import lax
from jax.experimental import pallas as pl
from jax.experimental.pallas import tpu as pltpu
from jax.sharding import PartitionSpec as P

LD = 4
ITERS = 3


PENALTY = 36.0
BOTTOM_RATIO = 8.0


def lobatto_tables():
    root_seven = math.sqrt(7.0)
    inner_root = math.sqrt(1.0 / 3.0 - 2.0 * root_seven / 21.0)
    outer_root = math.sqrt(1.0 / 3.0 + 2.0 * root_seven / 21.0)
    points = (np.array([-1.0, -outer_root, -inner_root, inner_root, outer_root, 1.0]) + 1.0) / 2.0
    weights = (
        np.array(
            [
                1.0 / 15.0,
                (14.0 - root_seven) / 30.0,
                (14.0 + root_seven) / 30.0,
                (14.0 + root_seven) / 30.0,
                (14.0 - root_seven) / 30.0,
                1.0 / 15.0,
            ]
        )
        / 2.0
    )
    barycentric = np.array(
        [1.0 / np.prod([points[j] - points[k] for k in range(6) if k != j]) for j in range(6)]
    )
    derivative = np.zeros((6, 6))
    for i in range(6):
        for j in range(6):
            if i != j:
                derivative[i, j] = barycentric[j] / barycentric[i] / (points[i] - points[j])
        derivative[i, i] = -np.sum(derivative[i])
    halves = np.zeros((2, 6, 6))
    for which_half in range(2):
        targets = (points + which_half) / 2.0
        for i in range(6):
            for j in range(6):
                halves[which_half, i, j] = np.prod(
                    [(targets[i] - points[k]) / (points[j] - points[k]) for k in range(6) if k != j]
                )
    column_sums = np.sum(derivative * derivative * weights[:, None], axis=0)
    stiff_diag = (
        column_sums[:, None, None] * weights[None, :, None] * weights[None, None, :]
        + weights[:, None, None] * column_sums[None, :, None] * weights[None, None, :]
        + weights[:, None, None] * weights[None, :, None] * column_sums[None, None, :]
    )
    return (weights, derivative, halves, stiff_diag.reshape(216))


BF16 = jnp.bfloat16
F32 = jnp.float32


def split_np(matrix):
    high = np.asarray(matrix, np.float32).astype(BF16)
    low = (np.asarray(matrix, np.float64) - high.astype(np.float64)).astype(np.float32).astype(BF16)
    return high, low


def operators():
    weights, derivative, halves, stiff_diag = lobatto_tables()
    eye = np.eye(6)
    trace_rows = []
    for direction in range(6):
        axis_index = direction // 2
        layer_index = 5 * (direction % 2)
        orientation = 2.0 * (direction % 2) - 1.0
        for row in (eye[layer_index], orientation * derivative[layer_index]):
            factors = [eye, eye, eye]
            factors[axis_index] = row[None, :]
            trace_rows.append(np.kron(np.kron(factors[0], factors[1]), factors[2]))
    traces = np.concatenate(trace_rows, axis=0)
    stiff_1d = derivative.T @ (weights[:, None] * derivative)
    mass = np.diag(weights)
    stiffness = (
        np.kron(np.kron(stiff_1d, mass), mass)
        + np.kron(np.kron(mass, stiff_1d), mass)
        + np.kron(np.kron(mass, mass), stiff_1d)
    )
    blocks = []
    for sub in range(4):
        quarter = np.kron(halves[sub % 2], halves[sub // 2])
        blocks.append(np.kron(np.eye(2), quarter))
    return traces, stiffness, np.concatenate(blocks, axis=0), np.outer(weights, weights).reshape(36, 1), stiff_diag


def split(value):
    high = value.astype(BF16)
    return high, (value - high.astype(F32)).astype(BF16)


def dot(left, right):
    return jnp.dot(left, right, preferred_element_type=F32)


def dot3(left_high, left_low, right):
    high, low = split(right)
    return dot(left_high, high) + (dot(left_high, low) + dot(left_low, high))


def one_hot(index_row, rows, base=0):
    count = index_row.shape[1]
    position = lax.broadcasted_iota(jnp.int32, (rows, count), 0)
    return jnp.where(position == index_row - base, 1.0, 0.0).astype(BF16)


def pick(traces, elem, direction, sub, onto):
    wide = dot(traces, one_hot(elem, traces.shape[1]))
    face = jnp.zeros((72, elem.shape[1]), F32)
    for d in range(6):
        both = wide[72 * d : 72 * d + 72] + wide[432 + 72 * d : 432 + 72 * d + 72]
        face = jnp.where(direction == d, both, face)
    high, low = split(face)
    quarters = dot(onto, jnp.concatenate([high, low, high], axis=0))
    result = face
    for s in range(4):
        result = jnp.where(sub == s, quarters[72 * s : 72 * s + 72], result)
    return result


def send_kernel(x_ref, inv_ref, code_ref, mat_high, mat_low, onto_ref, out_ref, traces_ref):
    @pl.when(pl.program_id(0) == 0)
    def _():
        raw = dot3(mat_high[...], mat_low[...], x_ref[...])
        row = lax.broadcasted_iota(jnp.int32, raw.shape, 0)
        raw = jnp.where(lax.rem(row, 72) >= 36, raw * inv_ref[...], raw)
        high, low = split(raw)
        traces_ref[0:432] = high
        traces_ref[432:864] = low

    code = code_ref[...]
    picked = pick(traces_ref[...], code[0:1], code[1:2], code[2:3], onto_ref[...])
    capacity = out_ref.shape[2]
    for k in range(out_ref.shape[0]):
        out_ref[k] = picked[:, k * capacity : (k + 1) * capacity]


def exchange_kernel(
    steps, axis, width, src_ref, x_ref, traces_ref, code_ref, onto_ref, stiff_high, stiff_low,
    dst_ref, own_ref, near_ref, volume_ref, send_sem, recv_sem,
):
    count = lax.axis_size(axis)
    me = lax.axis_index(axis)
    barrier = pltpu.get_barrier_semaphore()
    peers = [lax.rem(me + step + count, count) for step in steps]
    for peer in peers:
        pl.semaphore_signal(barrier, inc=1, device_id=(peer,), device_id_type=pl.DeviceIdType.MESH)
    pl.semaphore_wait(barrier, len(steps))
    copies = []
    for k, peer in enumerate(peers):
        copy = pltpu.make_async_remote_copy(
            src_ref=src_ref.at[k],
            dst_ref=dst_ref.at[k],
            send_sem=send_sem.at[k],
            recv_sem=recv_sem.at[k],
            device_id=(peer,),
            device_id_type=pl.DeviceIdType.MESH,
        )
        copy.start()
        copies.append(copy)

    def step_tile(i, carry):
        part = pl.ds(pl.multiple_of(i * width, width), width)
        code = code_ref[:, part]
        own_ref[:, part] = pick(traces_ref[...], code[0:1], code[1:2], code[2:3], onto_ref[...])
        near_ref[:, part] = pick(traces_ref[...], code[3:4], code[4:5], code[5:6], onto_ref[...])
        return carry

    lax.fori_loop(0, code_ref.shape[1] // width, step_tile, 0)
    volume_ref[...] = dot3(stiff_high[...], stiff_low[...], x_ref[...])
    for copy in copies:
        copy.wait()


def norms_kernel(axis, sums_ref, out_ref, landing, send_sem, recv_sem):
    count = lax.axis_size(axis)
    me = lax.axis_index(axis)
    barrier = pltpu.get_barrier_semaphore()

    def greet(k, carry):
        peer = lax.rem(me + k, count)
        pl.semaphore_signal(barrier, inc=1, device_id=(peer,), device_id_type=pl.DeviceIdType.MESH)
        return carry

    def copy_to(k):
        return pltpu.make_async_remote_copy(
            src_ref=sums_ref,
            dst_ref=landing.at[k],
            send_sem=send_sem.at[k],
            recv_sem=recv_sem.at[k],
            device_id=(lax.rem(me + k, count),),
            device_id_type=pl.DeviceIdType.MESH,
        )

    def start(k, carry):
        copy_to(k).start()
        return carry

    def finish(k, carry):
        copy_to(k).wait()
        return carry

    lax.fori_loop(1, count, greet, 0)
    pl.semaphore_wait(barrier, count - 1)
    lax.fori_loop(1, count, start, 0)
    landing[0] = sums_ref[...]
    lax.fori_loop(1, count, finish, 0)

    def add(j, total):
        return total + landing[lax.rem(me + count - j, count)]

    total = lax.fori_loop(0, count, add, jnp.zeros(out_ref.shape, F32))
    out_ref[...] = jnp.broadcast_to(jnp.sum(total, axis=1, keepdims=True), out_ref.shape)


def apply_kernel(
    row_ref, coef_ref, x_ref, dirn_ref, rhs_ref, elem_ref, prec_ref, recv_ref, own_ref, near_ref,
    volume_ref, code_ref, rows_ref, size_ref, off_ref, weight_ref, lift_high, lift_low, prior_ref,
    x_out, dirn_out, sums_out, pool, total,
):
    peer_count = recv_ref.shape[0]

    @pl.when(pl.program_id(0) == 0)
    def _():
        for k in range(peer_count):
            high, low = split(recv_ref[k])
            pool[144 * k : 144 * k + 72] = high
            pool[144 * k + 72 : 144 * k + 144] = low
        total[...] = jnp.zeros_like(total)

    code = code_ref[...]
    direction, sub = code[1:2], code[2:3]
    bound = code[6:7] == -1
    width = sub.shape[1]
    own = own_ref[...]
    wide = dot(pool[...], one_hot(code[7:8], pool.shape[1]))
    partner = near_ref[...]
    for k in range(peer_count):
        both = wide[144 * k : 144 * k + 72] + wide[144 * k + 72 : 144 * k + 144]
        partner = jnp.where(code[6:7] == k, both, partner)
    own_value, own_slope = own[0:36], own[36:72]
    part_value = jnp.where(bound, 0.0, partner[0:36])
    part_slope = jnp.where(bound, -own_slope, partner[36:72])
    jump = own_value - part_value
    flux = 0.5 * (own_slope - part_slope)
    mortar = size_ref[0:1]
    area = mortar * mortar
    weight = weight_ref[...] * size_ref[1:2]
    term_value = weight * (PENALTY * mortar * jump - area * flux)
    term_slope = -weight * (jnp.where(bound, 1.0, 0.5) * area) * jump
    terms = jnp.concatenate([term_value, term_slope], axis=0)
    spread = jnp.concatenate([jnp.where(sub == s, terms, 0.0) for s in range(4)], axis=0)
    spread_high, spread_low = split(spread)
    back = dot(off_ref[...], jnp.concatenate([spread_high, spread_low, spread_high], axis=0))
    back = jnp.where(sub >= 4, terms, back)
    spread = jnp.concatenate([jnp.where(direction == d, back, 0.0) for d in range(6)], axis=0)
    wide_high, wide_low = split(spread)
    lanes = lax.broadcasted_iota(jnp.int32, (width, total.shape[1]), 1)
    hot = jnp.where(lanes == rows_ref[...], 1.0, 0.0).astype(BF16)
    total[...] += dot(wide_high, hot) + dot(wide_low, hot)

    @pl.when(pl.program_id(0) == pl.num_programs(0) - 1)
    def _():
        size, inv = elem_ref[0:1], elem_ref[1:2]
        field = x_ref[...]
        row = lax.broadcasted_iota(jnp.int32, total.shape, 0)
        faces = jnp.where(lax.rem(row, 72) >= 36, total[...] * inv, total[...])
        applied = size * volume_ref[...]
        applied = applied + dot3(lift_high[...], lift_low[...], faces)
        residual = jnp.where(size > 0.0, rhs_ref[...] - applied, 0.0)
        scaled = residual * (inv * prec_ref[...])
        step = coef_ref[0] * dirn_ref[...] + coef_ref[1] * scaled
        dirn_out[...] = step
        x_out[...] = field + step
        squares = jnp.sum(residual * residual, axis=0, keepdims=True)
        products = jnp.sum(residual * scaled, axis=0, keepdims=True)
        fold = lambda line: sum(line[:, k : k + 128] for k in range(0, line.shape[1], 128))
        row = lax.broadcasted_iota(jnp.int32, sums_out.shape, 0)
        row_index = row_ref[0]
        later = jnp.where(row == 2 * row_index + 1, fold(products), prior_ref[...])
        sums_out[...] = jnp.where(row == 2 * row_index, fold(squares), later)


def take_small(tables, index):
    rows = tables.shape[1] // 128
    fine = (jnp.arange(128, dtype=jnp.int32)[:, None] == (index % 128)[None, :]).astype(BF16)
    wide = jnp.dot(tables.reshape(-1, 128).astype(BF16), fine, preferred_element_type=F32)
    wide = wide.reshape(tables.shape[0], rows, -1)
    coarse = jnp.arange(rows, dtype=jnp.int32)[:, None] == (index // 128)[None, :]
    return jnp.sum(jnp.where(coarse[None], wide, 0.0), axis=1).astype(jnp.int32)


def tile(count):
    for width in (512, 256, 128):
        if count % width == 0:
            return width
    return count


def whole(shape):
    return pl.BlockSpec(shape, lambda i: (0,) * len(shape))


def general_path(
    rhs, start, spectrum_top, elem_code, rec_elem, rec_dir, rec_sub, rec_peer, rec_index, send_rec
):
    traces, stiffness, interp, face_weight, stiff_diag = operators()
    part_count = lax.axis_size("parts")
    own_index = lax.axis_index("parts")
    elem_count = rhs.shape[1]
    record_count = rec_elem.shape[0]
    capacity = send_rec.shape[0] // part_count
    far_reach = 2 * LD - 1
    code_float = elem_code.astype(F32)
    elem_size = 0.5 * code_float
    inv_size = jnp.where(elem_code > 0, 2.0 / jnp.maximum(code_float, 1.0), 0.0)
    elem_rows = jnp.stack([elem_size, inv_size])
    is_bound = rec_peer < 0
    is_local = rec_peer == own_index
    is_remote = jnp.logical_and(jnp.logical_not(is_bound), jnp.logical_not(is_local))
    offset = own_index - rec_peer
    position = jnp.where(offset < 0, offset + far_reach, offset + far_reach - 1)
    block = jnp.where(is_remote, position, jnp.where(is_bound, -1, -2))
    steps = list(range(-far_reach, 0)) + list(range(1, far_reach + 1))
    lists = send_rec.reshape(part_count, capacity)
    lists = jnp.concatenate([lists[part_count - far_reach :], lists, lists[:far_reach]], axis=0)
    lists = lax.dynamic_slice_in_dim(lists, own_index, 2 * far_reach + 1, 0)
    send_cols = jnp.concatenate([lists[:far_reach], lists[far_reach + 1 :]], axis=0).reshape(-1)
    send_count = send_cols.shape[0]

    own_size = 0.5 * take_small(elem_code[None], rec_elem)[0].astype(F32)
    mortar_size = jnp.where(rec_sub < 4, 0.5 * own_size, own_size)
    size_rows = jnp.stack([mortar_size, (rec_sub < 5).astype(F32)])
    tables = jnp.stack([rec_elem // 256, rec_elem % 256, rec_dir * 8 + rec_sub])
    found = take_small(tables, jnp.concatenate([send_cols, rec_index]))
    found = jnp.stack([found[0] * 256 + found[1], found[2] // 8, found[2] % 8])
    send_code = found[:, :send_count]
    near = jnp.where(is_local[None], found[:, send_count:], -1)
    rec_code = jnp.concatenate(
        [jnp.stack([rec_elem, rec_dir, rec_sub]), near, block[None], rec_index[None]],
        axis=0,
    )
    rec_rows = rec_elem[:, None]

    mat_high, mat_low = split_np(traces)
    lift_high, lift_low = split_np(traces.T)
    stiff_high, stiff_low = split_np(stiffness)
    onto_high, onto_low = split_np(interp)
    onto = np.concatenate([onto_high, onto_high, onto_low], axis=1)
    flat = np.concatenate([interp[72 * s : 72 * s + 72].T for s in range(4)], axis=1)
    off_high, off_low = split_np(flat)
    off = np.concatenate([off_high, off_high, off_low], axis=1)
    prec = jnp.asarray((1.0 / stiff_diag).reshape(216, 1), F32)
    weight = jnp.asarray(face_weight, F32)

    send_tile, rec_tile, peer_count = 2 * capacity, tile(record_count), len(steps)
    params = pltpu.CompilerParams(vmem_limit_bytes=60 * 1024 * 1024)
    field = (216, elem_count)

    def send_call(x):
        return pl.pallas_call(
            send_kernel,
            grid=(send_count // send_tile,),
            in_specs=[
                whole(field),
                whole((1, elem_count)),
                pl.BlockSpec((3, send_tile), lambda i: (0, i)),
                whole((432, 216)),
                whole((432, 216)),
                whole((288, 216)),
            ],
            out_specs=[pl.BlockSpec((2, 72, capacity), lambda i: (i, 0, 0)), whole((864, elem_count))],
            out_shape=[
                jax.ShapeDtypeStruct((peer_count, 72, capacity), F32),
                jax.ShapeDtypeStruct((864, elem_count), BF16),
            ],
            compiler_params=params,
            name="send_traces",
        )(x, inv_size[None], send_code, jnp.asarray(mat_high), jnp.asarray(mat_low), jnp.asarray(onto))

    vmem = pl.BlockSpec(memory_space=pltpu.VMEM)

    def exchange(outgoing, x, element_traces):
        return pl.pallas_call(
            functools.partial(exchange_kernel, steps, "parts", rec_tile),
            in_specs=[pl.BlockSpec(memory_space=pl.ANY)] + [vmem] * 6,
            out_specs=[pl.BlockSpec(memory_space=pl.ANY)] + [vmem] * 3,
            out_shape=[
                jax.ShapeDtypeStruct((peer_count, 72, capacity), F32),
                jax.ShapeDtypeStruct((72, record_count), F32),
                jax.ShapeDtypeStruct((72, record_count), F32),
                jax.ShapeDtypeStruct(field, F32),
            ],
            scratch_shapes=[
                pltpu.SemaphoreType.DMA((peer_count,)),
                pltpu.SemaphoreType.DMA((peer_count,)),
            ],
            compiler_params=pltpu.CompilerParams(
                collective_id=0, has_side_effects=True, vmem_limit_bytes=60 * 1024 * 1024
            ),
            name="exchange",
        )(
            outgoing, x, element_traces, rec_code, jnp.asarray(onto),
            jnp.asarray(stiff_high), jnp.asarray(stiff_low),
        )

    def all_sums(sums):
        return pl.pallas_call(
            functools.partial(norms_kernel, "parts"),
            in_specs=[vmem],
            out_specs=vmem,
            out_shape=jax.ShapeDtypeStruct((8, 128), F32),
            scratch_shapes=[
                pltpu.VMEM((part_count, 8, 128), F32),
                pltpu.SemaphoreType.DMA((part_count,)),
                pltpu.SemaphoreType.DMA((part_count,)),
            ],
            compiler_params=pltpu.CompilerParams(collective_id=1, has_side_effects=True),
            name="all_sums",
        )(sums)

    def apply_call(row_index, coef, x, dirn, received, own, near_traces, volume, sums):
        tiles = lambda rows: pl.BlockSpec((rows, rec_tile), lambda i: (0, i))
        return pl.pallas_call(
            apply_kernel,
            grid=(record_count // rec_tile,),
            in_specs=[
                pl.BlockSpec(memory_space=pltpu.SMEM),
                pl.BlockSpec(memory_space=pltpu.SMEM),
                whole(field),
                whole(field),
                whole(field),
                whole((2, elem_count)),
                whole((216, 1)),
                whole((peer_count, 72, capacity)),
                tiles(72),
                tiles(72),
                whole(field),
                tiles(8),
                pl.BlockSpec((rec_tile, 1), lambda i: (i, 0)),
                tiles(2),
                whole((72, 864)),
                whole((36, 1)),
                whole((216, 432)),
                whole((216, 432)),
                whole((8, 128)),
            ],
            out_specs=[whole(field), whole(field), whole((8, 128))],
            out_shape=[
                jax.ShapeDtypeStruct(field, F32),
                jax.ShapeDtypeStruct(field, F32),
                jax.ShapeDtypeStruct((8, 128), F32),
            ],
            scratch_shapes=[
                pltpu.VMEM((144 * peer_count, capacity), BF16),
                pltpu.VMEM((432, elem_count), F32),
            ],
            compiler_params=params,
            name="apply_operator",
        )(
            row_index[None], coef, x, dirn, rhs, elem_rows, prec, received, own, near_traces, volume, rec_code, rec_rows,
            size_rows, jnp.asarray(off), weight, jnp.asarray(lift_high), jnp.asarray(lift_low), sums,
        )

    scale_total = 216.0 * elem_count * part_count
    top_value = spectrum_top[0]
    bottom = top_value / BOTTOM_RATIO
    center = 0.5 * (top_value + bottom)
    radius = 0.5 * (top_value - bottom)
    sigma_ratio = center / radius
    rho_prev = 1.0 / sigma_ratio
    coefs = [jnp.stack([jnp.zeros_like(center), 1.0 / center])]
    for step_index in range(1, ITERS):
        rho_next = 1.0 / (2.0 * sigma_ratio - rho_prev)
        coefs.append(jnp.stack([rho_next * rho_prev, 2.0 * rho_next / radius]))
        rho_prev = rho_next
    coefs = jnp.stack(coefs)

    def one_step(step_index, state):
        x, dirn, sums = state
        outgoing, element_traces = send_call(x)
        moved = exchange(outgoing, x, element_traces)
        coef = lax.dynamic_index_in_dim(coefs, step_index, 0, False)
        return tuple(apply_call(step_index, coef, x, dirn, *moved, sums))

    x, dirn, sums = lax.fori_loop(0, ITERS, one_step, (start + 0.0 * top_value, jnp.zeros_like(start), jnp.zeros((8, 128), F32)))
    norms = 0.5 * jnp.log(all_sums(sums)[: 2 * ITERS, 0].reshape(ITERS, 2) / scale_total)
    return (x, norms)


LATERAL = 128
FIELDS = 9


def iota(shape, axis):
    return lax.broadcasted_iota(jnp.int32, shape, axis)


def sum_rows(value):
    return jnp.sum(value, axis=0, keepdims=True)


def total_of(value):
    return jnp.sum(value, axis=1, keepdims=True)


def look_up(tables, rows, index):
    hot = jnp.where(iota((128, index.shape[1]), 0) == (index & 127), 1.0, 0.0).astype(BF16)
    wide = dot(tables, hot)
    mask = iota((rows, index.shape[1]), 0) == (index >> 7)
    count = tables.shape[0] // rows
    return [sum_rows(jnp.where(mask, wide[k * rows : (k + 1) * rows], 0.0)) for k in range(count)]


def regroup(columns, position, rows):
    mask = iota((rows, position.shape[1]), 0) == (position >> 7)
    left = jnp.concatenate([jnp.where(mask, column, 0.0) for column in columns], axis=0).astype(BF16)
    hot = jnp.where(iota((128, position.shape[1]), 0) == (position & 127), 1.0, 0.0).astype(BF16)
    return lax.dot_general(left, hot, (((1,), (1,)), ((), ())), preferred_element_type=F32)


def setup_kernel(
    axis, capacity, code_ref, elem_ref, dir_ref, sub_ref, peer_ref, index_ref,
    code_line, elem_line, dir_line, sub_line, peer_line, index_line, lists_ref,
    rows_ref, col_ref, send_ref, flag_ref, elem_out,
):
    me = lax.axis_index(axis)
    count = lax.axis_size(axis)
    group, place = me // LD, lax.rem(me, LD)
    elem, direction, sub = elem_line[...], dir_line[...], sub_line[...]
    peer, index = peer_line[...], index_line[...]
    records, slots = elem.shape[1], code_line.shape[1]
    chunks, table_rows, slot_rows = records // 128, records // 128, 6 * slots // 128
    used = sub < 5
    local = used & (peer == me)
    bound = used & (peer < 0)
    remote = used & (peer >= 0) & (peer != me)

    kind = jnp.where(used, jnp.where(remote, direction, direction + 8), -1)
    member = jnp.where(iota((16, records), 0) == kind, 1.0, 0.0)
    stacked = jnp.concatenate([member[:, 128 * k : 128 * k + 128] for k in range(chunks)], axis=0)
    upper = jnp.where(iota((128, 128), 0) < iota((128, 128), 1), 1.0, 0.0)
    counted = dot(
        stacked.astype(BF16), jnp.concatenate([upper, jnp.ones((128, 128), F32)], axis=1).astype(BF16)
    )
    carry = jnp.zeros((16, 128), F32)
    before = []
    for k in range(chunks):
        before.append(counted[16 * k : 16 * k + 16, :128] + carry)
        carry = carry + counted[16 * k : 16 * k + 16, 128:]
    base = jnp.concatenate([jnp.zeros((8, 128), F32), carry[:8]], axis=0)
    before = jnp.concatenate([part + base for part in before], axis=1)
    rank = sum_rows(before * member).astype(jnp.int32)
    in_range = used & (rank < slots)
    slot = jnp.where(in_range, direction * slots + rank, -1)

    tables = jnp.concatenate(
        [
            (elem_ref[...] & 127).astype(F32),
            ((elem_ref[...] >> 7) * 8 + sub_ref[...]).astype(F32),
            dir_ref[...].astype(F32),
        ],
        axis=0,
    ).astype(BF16)
    rows_per = capacity // 128
    list_rows = iota(lists_ref.shape, 0)
    lists = lists_ref[...].astype(F32)
    channel = []
    for d, other in ((1, group + 1), (0, group - 1)):
        here = remote & (direction == d)
        most = jnp.max(jnp.where(here, peer, -1), axis=1, keepdims=True)
        least = jnp.min(jnp.where(here, peer, count), axis=1, keepdims=True)
        wrong = here & (peer // LD != other)
        channel.append((most, jnp.where((most >= 0) & (most != least), 1.0, 0.0), wrong))
    wanted = []
    for most, _, _ in channel:
        for part in range(rows_per):
            wanted.append(sum_rows(jnp.where(list_rows == most * rows_per + part, lists, 0.0)))
    for pos in range(LD - 1):
        dest = group * LD + lax.rem(place + pos + 1, LD)
        wanted.append(sum_rows(jnp.where(list_rows == dest * rows_per, lists, 0.0)))
    wanted.append(jnp.zeros((1, LATERAL), F32))
    wanted = jnp.concatenate(wanted, axis=1).astype(jnp.int32)
    wanted_count = wanted.shape[1]
    low, high, found_dir = look_up(tables, table_rows, jnp.concatenate([wanted, index], axis=1))
    high = high.astype(jnp.int32)
    found_elem = low.astype(jnp.int32) + 128 * (high >> 3)
    found_sub = high & 7
    send_ref[0:1] = found_elem[:, :wanted_count]
    send_ref[1:2] = found_dir[:, :wanted_count].astype(jnp.int32)
    send_ref[2:3] = found_sub[:, :wanted_count]
    send_ref[3:8] = jnp.zeros((5, wanted_count), jnp.int32)
    near_elem, near_sub = found_elem[:, wanted_count:], found_sub[:, wanted_count:]

    code_rows = -(-slots // 1024) * 8
    code_table = code_ref[...].astype(F32)
    if code_rows > code_table.shape[0]:
        pad = jnp.zeros((code_rows - code_table.shape[0], 128), F32)
        code_table = jnp.concatenate([code_table, pad], axis=0)
    code = look_up(code_table.astype(BF16), code_rows, elem)[0]
    size = 0.5 * code
    mortar = jnp.where(sub < 4, 0.5 * size, size)

    turn = lax.rem(place - lax.rem(peer, LD) + LD, LD) - 1
    landed = jnp.where(direction < 2, index, turn * LATERAL + index)
    split_near = jnp.where(sub < 4, sub, jnp.where(near_sub < 4, near_sub + 4, 8))
    split_far = jnp.minimum(sub, 4)
    real = lambda value: value.astype(F32)
    columns = [
        real(elem & 127),
        real((elem >> 7) + 1),
        real(near_elem & 127),
        jnp.where(local, real((near_elem >> 7) + 1), 0.0),
        jnp.where(remote, real(landed & 127), 0.0),
        jnp.where(remote, real((landed >> 7) + 1), 0.0),
        real(split_near),
        real(split_far),
        mortar,
    ]
    moved = regroup(columns, slot, slot_rows)
    part = lambda k: moved[k * slot_rows : (k + 1) * slot_rows]
    join = lambda k: jnp.where(part(k + 1) > 0.0, part(k) + 128.0 * (part(k + 1) - 1.0), -1.0)
    own = join(0)
    spare = col_ref.shape[1] - slot_rows
    own_all = jnp.concatenate([own, jnp.zeros((spare, 128), F32)], axis=0)
    col_ref[...] = jnp.transpose(own_all).astype(jnp.int32)
    mort = part(8)
    fields = [join(2), join(4), part(6), part(7), 36.0 * mort, 0.5 * mort * mort]

    face = jnp.where(used, direction * slots + elem, -1)
    marks = [jnp.where(used & (sub == s), 1.0, 0.0) for s in range(5)]
    marks.append(jnp.where(bound & (sub == 4), 1.0, 0.0))
    tally = regroup(marks, face, slot_rows)
    fields += [tally[k * slot_rows : (k + 1) * slot_rows] for k in range(6)]
    per = slots // 128
    lines = []
    for value in fields:
        pieces = []
        for d in range(6):
            pieces.append(
                jnp.concatenate([value[per * d + q : per * d + q + 1] for q in range(per)], axis=1)
            )
        pieces.append(jnp.zeros((2, slots), F32))
        lines.append(jnp.concatenate(pieces, axis=0))
    code_all = code_line[...].astype(F32)
    size_all = 0.5 * code_all
    inv_all = jnp.where(code_all > 0.0, 2.0 / jnp.maximum(code_all, 1.0), 0.0)
    elem_out[0:1] = size_all
    elem_out[1:2] = inv_all
    elem_out[2:8] = jnp.zeros((6, slots), F32)
    half = 0.5 * size_all
    counts, bounds = lines[6:11], lines[11]
    lines = lines[:6]
    for s in range(5):
        lines.append(36.0 * (half if s < 4 else size_all) * counts[s])
    for s in range(4):
        lines.append(half * half * (0.5 * counts[s]))
    lines.append(size_all * size_all * (0.5 * (counts[4] + bounds)))
    for k, line in enumerate(lines):
        rows_ref[8 * k : 8 * k + 8] = line
    rows_ref[8 * len(lines) :] = jnp.zeros((rows_ref.shape[0] - 8 * len(lines), slots), F32)

    wrong = jnp.where(remote & (direction >= 2) & ((peer // LD != group) | (index >= LATERAL)), 1.0, 0.0)
    wrong = wrong + jnp.where(bound & (sub < 4), 1.0, 0.0)
    wrong = wrong + jnp.where(local & (sub < 4) & (near_sub < 4), 1.0, 0.0)
    wrong = wrong + jnp.where(used & (rank >= slots), 1.0, 0.0)
    for _, _, off in channel:
        wrong = wrong + jnp.where(off, 1.0, 0.0)
    faults = total_of(wrong) + channel[0][1] + channel[1][1]
    row = iota((8, 128), 0)
    allowed = jnp.where(row < 2, float(capacity), float(LATERAL))
    over = jnp.where((row < 6) & (carry[:8] > allowed), 1.0, 0.0)
    faults = faults + total_of(sum_rows(over))
    turns = [
        lax.rem(place - lax.rem(jnp.maximum(most, 0), LD) + LD, LD).astype(F32) for most, _, _ in channel
    ]
    ahead = [
        jnp.where(most >= 0, lax.rem(jnp.maximum(most, 0) % LD - place + LD, LD), -1).astype(F32)
        for most, _, _ in channel
    ]
    flags = jnp.where(row == 0, faults, jnp.where(row == 1, turns[1], turns[0]))
    flag_ref[...] = jnp.where(row == 3, ahead[0], jnp.where(row == 4, ahead[1], flags))


def stack2(value):
    high = value.astype(BF16).astype(F32)
    return jnp.concatenate([high, value - high], axis=0).astype(BF16)


def stack3(value):
    high = value.astype(BF16).astype(F32)
    return jnp.concatenate([high, value - high, high], axis=0).astype(BF16)


def fold_pair(value):
    half = value.shape[0] // 2
    return value[:half] + value[half:]


def choose(blocks, rows, code):
    last = blocks.shape[0] // rows - 1
    result = blocks[last * rows :]
    for q in range(last):
        result = jnp.where(code == q, blocks[q * rows : q * rows + rows], result)
    return result


def main_kernel(
    axis, iters, capacity,
    x_ref, rhs_hbm, top_ref, rows_ref, col_ref, send_ref, flag_ref, elem_ref, prec_ref,
    trace_high_hbm, trace_low_hbm, stiff_high_hbm, stiff_low_hbm, lift_high_hbm, lift_low_hbm,
    onto_hbm, own_hbm, near_hbm, far_hbm,
    x_out, norm_out,
    rhs_ref, trace_high, trace_low, stiff_high, stiff_low, lift_high, lift_low,
    onto_ref, own_ref, near_ref, far_ref, load_sem,
    dirn, volume, traces, pairs, faces, scatter, gather, gather_chan, gather_lat, send_chan, send_lat,
    far_rows, coefs, snd_chan, snd_lat, snd_pass, kept_pass, rcv_chan, rcv_lat, rcv_pass, sums, landing,
    send_sem, recv_sem, sum_send, sum_recv,
):
    count = lax.axis_size(axis)
    me = lax.axis_index(axis)
    group, place = me // LD, lax.rem(me, LD)
    groups = count // LD
    slots, half = x_ref.shape[1], capacity // 2
    mesh_id = pl.DeviceIdType.MESH
    barrier = pltpu.get_barrier_semaphore()

    def greet(k, carry):
        peer = lax.rem(me + k, count)
        pl.semaphore_signal(barrier, inc=1, device_id=(peer,), device_id_type=mesh_id)
        return carry

    lax.fori_loop(1, count, greet, 0)
    held = [
        (x_ref, x_out),
        (trace_high_hbm, trace_high),
        (trace_low_hbm, trace_low),
        (onto_hbm, onto_ref),
        (stiff_high_hbm, stiff_high),
        (stiff_low_hbm, stiff_low),
        (own_hbm, own_ref),
        (near_hbm, near_ref),
        (far_hbm, far_ref),
        (lift_high_hbm, lift_high),
        (lift_low_hbm, lift_low),
        (rhs_hbm, rhs_ref),
    ]
    loads = [pltpu.make_async_copy(src, dst, load_sem.at[k]) for k, (src, dst) in enumerate(held)]
    for load in loads:
        load.start()

    def hot(mask):
        return jnp.where(mask, 1.0, 0.0).astype(BF16)

    per = slots // 128
    columns = col_ref[...]
    for d in range(6):
        line = rows_ref[d : d + 1].astype(jnp.int32)
        gather[d] = hot(iota((slots, slots), 0) == line)
        for q in range(per):
            column = columns[:, per * d + q : per * d + q + 1]
            scatter[d, 128 * q : 128 * q + 128] = hot(iota((128, slots), 1) == column)
        line = rows_ref[8 + d : 9 + d].astype(jnp.int32)
        if d < 2:
            gather_chan[d] = hot(iota((capacity, capacity), 0) == line[:, :capacity])
        else:
            gather_lat[d - 2] = hot(iota((LD * LATERAL, LATERAL), 0) == line[:, :LATERAL])
    size, inv = elem_ref[0:1], elem_ref[1:2]
    def across(side, turn):
        other = lax.rem(group + (1 if side == 0 else groups - 1), groups)
        return (other * LD + lax.rem(place + turn, LD),)

    send_elem = send_ref[0:1]
    send_chan[0] = hot(iota((slots, capacity), 0) == send_elem[:, :capacity])
    send_chan[1] = hot(iota((slots, capacity), 0) == send_elem[:, capacity : 2 * capacity])
    send_lat[...] = hot(iota((slots, LD * LATERAL), 0) == send_elem[:, 2 * capacity :])
    chosen = jnp.zeros(far_rows.shape, F32)
    for k, field in enumerate((3, 4, 5)):
        block = rows_ref[8 * field : 8 * field + 8]
        pieces = []
        for d in range(6):
            part = block[:, : capacity if d < 2 else LATERAL]
            pieces.append(sum_rows(jnp.where(iota(part.shape, 0) == d, part, 0.0)))
        chosen = jnp.where(iota(chosen.shape, 0) == k, jnp.concatenate(pieces, axis=1), chosen)
    far_rows[...] = chosen

    line = jnp.ones((1, 128), F32)
    top = top_ref[0] * line
    bottom = top / BOTTOM_RATIO
    center = 0.5 * (top + bottom)
    radius = 0.5 * (top - bottom)
    sigma = center / radius
    rho = 1.0 / sigma
    coefs[0:1] = 0.0 * line
    coefs[1:2] = 1.0 / center
    for k in range(1, iters):
        rho_next = 1.0 / (2.0 * sigma - rho)
        coefs[2 * k : 2 * k + 1] = rho_next * rho
        coefs[2 * k + 1 : 2 * k + 2] = 2.0 * rho_next / radius
        rho = rho_next
    dirn[...] = jnp.zeros_like(dirn)
    sums[...] = jnp.where(iota(sums.shape, 0) == 2 * iters, flag_ref[0:1], 0.0) * jnp.where(
        iota(sums.shape, 1) == 0, 1.0, 0.0
    )

    for load in loads:
        load.wait()
    pl.semaphore_wait(barrier, count - 1)

    def step(it, carry):
        field = x_out[...]
        field_high, field_low = split(field)

        def trace(first, last):
            high, low = trace_high[first:last], trace_low[first:last]
            raw = dot(high, field_high) + (dot(high, field_low) + dot(low, field_high))
            raw = jnp.where(lax.rem(iota(raw.shape, 0), 72) >= 36, raw * inv, raw)
            traces[first:last] = raw
            for d in range(first // 72, last // 72):
                pairs[d] = stack2(raw[72 * d - first : 72 * d + 72 - first])

        trace(0, 144)
        outgoing = jnp.concatenate(
            [fold_pair(dot(pairs[1], send_chan[0])), fold_pair(dot(pairs[0], send_chan[1]))], axis=1
        )
        outgoing = choose(dot(onto_ref[...], stack3(outgoing)), 80, send_ref[2:3, : 2 * capacity])
        spare = iota((40, half), 0) >= 36
        for side in range(2):
            ahead = flag_ref[3 + side : 4 + side, 0:1]
            for turn in range(LD):
                low, left = 40 * (turn // 2), side * capacity + half * (turn % 2)
                snd_chan[side, turn] = jnp.where(spare, ahead, outgoing[low : low + 40, left : left + half])

        def send(source, target, k, place_of):
            return pltpu.make_async_remote_copy(
                src_ref=source,
                dst_ref=target,
                send_sem=send_sem.at[it, k],
                recv_sem=recv_sem.at[it, k],
                device_id=place_of,
                device_id_type=mesh_id,
            )

        def beside(turn):
            return (group * LD + lax.rem(place + turn, LD),)

        pairs_of = [(side, turn) for side in range(2) for turn in range(LD)]
        channel = [
            send(snd_chan.at[side, turn], rcv_chan.at[it, side, turn], side * LD + turn, across(side, turn))
            for side, turn in pairs_of
        ]
        lateral = [
            send(snd_lat.at[pos], rcv_lat.at[it, pos], 2 * LD + pos, beside(pos + 1)) for pos in range(LD - 1)
        ]
        passed = [
            send(
                snd_pass.at[side, turn - 1],
                rcv_pass.at[it, side, turn - 1],
                (3 + side) * LD + turn - 1,
                beside(turn),
            )
            for side, turn in pairs_of
            if turn
        ]
        for copy in channel:
            copy.start()

        trace(144, 432)
        send_dir = send_ref[1:2, 2 * capacity :]
        outgoing = jnp.zeros((72, LD * LATERAL), F32)
        for d in range(2, 6):
            outgoing = jnp.where(send_dir == d, fold_pair(dot(pairs[d], send_lat[...])), outgoing)
        outgoing = choose(dot(onto_ref[...], stack3(outgoing)), 80, send_ref[2:3, 2 * capacity :])
        for pos in range(LD - 1):
            snd_lat[pos] = outgoing[:, pos * LATERAL : (pos + 1) * LATERAL]
        for copy in lateral:
            copy.start()

        volume[...] = dot3(stiff_high[...], stiff_low[...], field) * size

        def local_faces(d, inner):
            line = lambda k: rows_ref[pl.ds(8 * k + d, 1)]
            mass = dot(own_ref[...], stack3(traces[pl.ds(pl.multiple_of(72 * d, 8), 72)]))
            value = jnp.zeros((40, slots), F32)
            slope = jnp.zeros((40, slots), F32)
            for s in range(5):
                mass_value, mass_slope = mass[80 * s : 80 * s + 40], mass[80 * s + 40 : 80 * s + 80]
                flux = line(11 + s)
                value = value + (line(6 + s) * mass_value - flux * mass_slope)
                slope = slope - flux * mass_value
            facing = d + 1 - 2 * lax.rem(d, 2)
            found = fold_pair(dot(pairs[facing], gather[d]))
            found = choose(dot(near_ref[...], stack3(found)), 80, line(2).astype(jnp.int32))
            jump, flux = line(4), line(5)
            terms = jnp.concatenate([flux * found[40:] - jump * found[:40], flux * found[:40]], axis=0)
            back = fold_pair(dot(stack2(terms), scatter[d]))
            faces[pl.ds(pl.multiple_of(80 * d, 8), 80)] = back + jnp.concatenate([value, slope], axis=0)
            return inner

        def pass_on(side):
            for copy in channel[side * LD : side * LD + LD]:
                copy.wait()
            for turn in range(LD):
                chunk = jnp.zeros((40, half), F32)
                for k in range(LD):
                    mine = rcv_chan[it, side, k][36:37, 0:1] == float((turn + k) % LD)
                    chunk = jnp.where(mine, rcv_chan[it, side, k], chunk)
                if turn:
                    snd_pass[side, turn - 1] = chunk
                else:
                    kept_pass[side] = chunk
            for copy in passed[side * (LD - 1) : (side + 1) * (LD - 1)]:
                copy.start()

        lax.fori_loop(2, 6, local_faces, 0)
        pass_on(0)
        pass_on(1)
        lax.fori_loop(0, 2, local_faces, 0)
        for copy in lateral:
            copy.wait()

        def add_far(pieces, first, last, width):
            found = jnp.concatenate(pieces, axis=1)
            left = first * capacity if first < 2 else 2 * capacity
            part = slice(left, left + width * (last - first))
            found = choose(dot(far_ref[...], stack3(found)), 80, far_rows[0:1, part].astype(jnp.int32))
            jump, flux = far_rows[1:2, part], far_rows[2:3, part]
            terms = stack2(
                jnp.concatenate([flux * found[40:] - jump * found[:40], flux * found[:40]], axis=0)
            )
            for d in range(first, last):
                start = (d - first) * width
                faces[80 * d : 80 * d + 80] += fold_pair(
                    dot(terms[:, start : start + width], scatter[d, :width])
                )

        def lifted(first, last):
            total = faces[80 * first : 80 * last]
            total = jnp.where(lax.rem(iota(total.shape, 0), 80) >= 40, total * inv, total)
            high, low = split(total)
            left, rest = lift_high[:, 80 * first : 80 * last], lift_low[:, 80 * first : 80 * last]
            return dot(left, high) + (dot(left, low) + dot(rest, high))

        sides = [rcv_lat[it, pos] for pos in range(LD - 1)] + [jnp.zeros((80, LATERAL), F32)]
        got = stack2(jnp.concatenate(sides, axis=1))
        add_far([fold_pair(dot(got, gather_lat[d])) for d in range(4)], 2, 6, LATERAL)
        volume[...] += lifted(2, 6)
        for copy in passed:
            copy.wait()

        pieces = []
        for side in range(2):
            turn = flag_ref[side + 1 : side + 2, 0:1]
            landed = [kept_pass[side]] + [rcv_pass[it, side, k] for k in range(LD - 1)]
            chunks = []
            for k in range(LD):
                chunk = landed[(-k) % LD]
                for t in range(1, LD):
                    chunk = jnp.where(turn == float(t), landed[(t - k) % LD], chunk)
                chunks.append(chunk)
            got = jnp.concatenate(
                [jnp.concatenate(chunks[:2], axis=1), jnp.concatenate(chunks[2:], axis=1)], axis=0
            )
            pieces.append(fold_pair(dot(stack2(got), gather_chan[side])))
        add_far(pieces, 0, 2, capacity)
        applied = volume[...] + lifted(0, 2)
        residual = jnp.where(size > 0.0, rhs_ref[...] - applied, 0.0)
        scaled = residual * (inv * prec_ref[...])
        first = coefs[pl.ds(2 * it, 1), 0:1]
        second = coefs[pl.ds(2 * it + 1, 1), 0:1]
        change = first * dirn[...] + second * scaled
        dirn[...] = change
        x_out[...] = field + change
        squares = sum_rows(residual * residual)
        products = sum_rows(residual * scaled)
        fold = lambda row: sum(row[:, k : k + 128] for k in range(0, row.shape[1], 128))
        row = iota(sums.shape, 0)
        kept = jnp.where(row == 2 * it + 1, fold(products), sums[...])
        sums[...] = jnp.where(row == 2 * it, fold(squares), kept)
        return carry

    lax.fori_loop(0, iters, step, 0)

    def copy_to(k):
        return pltpu.make_async_remote_copy(
            src_ref=sums,
            dst_ref=landing.at[k],
            send_sem=sum_send.at[k],
            recv_sem=sum_recv.at[k],
            device_id=(lax.rem(me + k, count),),
            device_id_type=mesh_id,
        )

    def begin(k, carry):
        copy_to(k).start()
        return carry

    def finish(k, carry):
        copy_to(k).wait()
        return carry

    def add(j, total):
        return total + landing[lax.rem(me + count - j, count)]

    lax.fori_loop(1, count, begin, 0)
    landing[0] = sums[...]
    lax.fori_loop(1, count, finish, 0)
    total = total_of(lax.fori_loop(0, count, add, jnp.zeros(sums.shape, F32)))
    mean = total / (216.0 * slots * count)
    logs = 0.5 * jnp.log(jnp.where(iota(total.shape, 0) < 2 * iters, mean, 1.0))
    shown = jnp.where(iota(total.shape, 0) < 2 * iters, logs, total)
    norm_out[...] = jnp.broadcast_to(shown, norm_out.shape)


def wide_rows(blocks):
    padded = []
    for block in blocks:
        rows = np.zeros((80, block.shape[1]))
        rows[0:36], rows[40:76] = block[0:36], block[36:72]
        padded.append(rows)
    return np.concatenate(padded, axis=0)


def three(matrix):
    high, low = split_np(matrix)
    return np.concatenate([high, high, low], axis=1)


def set_up(slots, capacity, arrays, send_rec):
    slot_rows = 6 * slots // 128
    to_lines = lambda array: array.reshape(-1, 128)
    to_line = lambda array: array.reshape(1, -1)
    vmem = pl.BlockSpec(memory_space=pltpu.VMEM)
    columns = 2 * capacity + LD * LATERAL
    return pl.pallas_call(
        functools.partial(setup_kernel, "parts", capacity),
        in_specs=[vmem] * 13,
        out_specs=[vmem] * 5,
        out_shape=[
            jax.ShapeDtypeStruct((136, slots), F32),
            jax.ShapeDtypeStruct((128, 128 * -(-slot_rows // 128)), jnp.int32),
            jax.ShapeDtypeStruct((8, columns), jnp.int32),
            jax.ShapeDtypeStruct((8, 128), F32),
            jax.ShapeDtypeStruct((8, slots), F32),
        ],
        compiler_params=pltpu.CompilerParams(vmem_limit_bytes=60 * 1024 * 1024),
        name="set_up",
    )(*map(to_lines, arrays), *map(to_line, arrays), to_lines(send_rec))


def fast_path(
    rhs, start, spectrum_top, elem_code, rec_elem, rec_dir, rec_sub, rec_peer, rec_index, send_rec
):
    traces, stiffness, interp, face_weight, stiff_diag = operators()
    part_count = lax.axis_size("parts")
    slots = rhs.shape[1]
    capacity = send_rec.shape[0] // part_count
    arrays = (elem_code, rec_elem, rec_dir, rec_sub, rec_peer, rec_index)
    vmem = pl.BlockSpec(memory_space=pltpu.VMEM)
    rows, col, send, flag, elem = set_up(slots, capacity, arrays, send_rec)

    weight = np.concatenate([face_weight, face_weight], axis=0)
    quarters = [interp[72 * s : 72 * s + 72] for s in range(4)]
    eye = np.eye(72)
    onto = three(wide_rows(quarters + [eye]))
    own = three(wide_rows([j.T @ (weight * j) for j in quarters] + [weight * eye]))
    back = [j.T * weight.T for j in quarters]
    near = three(wide_rows(back + [weight * j for j in quarters] + [weight * eye]))
    far = wide_rows(back + [weight * eye])
    far = three(wide_rows([far.T]).T)
    trace_high, trace_low = split_np(traces)
    stiff_high, stiff_low = split_np(stiffness)
    lift = np.zeros((216, 480))
    for d in range(6):
        lift[:, 80 * d : 80 * d + 36] = traces.T[:, 72 * d : 72 * d + 36]
        lift[:, 80 * d + 40 : 80 * d + 76] = traces.T[:, 72 * d + 36 : 72 * d + 72]
    lift_high, lift_low = split_np(lift)
    prec = (1.0 / stiff_diag).reshape(216, 1).astype(np.float32)
    constants = (
        prec, trace_high, trace_low, stiff_high, stiff_low, lift_high, lift_low, onto, own, near, far
    )
    copies, half = 5 * LD, capacity // 2
    hbm = pl.BlockSpec(memory_space=pltpu.HBM)
    x, shown = pl.pallas_call(
        functools.partial(main_kernel, "parts", ITERS, capacity),
        in_specs=[hbm] * 2 + [pl.BlockSpec(memory_space=pltpu.SMEM)] + [vmem] * 6 + [hbm] * 10,
        out_specs=[vmem] * 2,
        out_shape=[jax.ShapeDtypeStruct((216, slots), F32), jax.ShapeDtypeStruct((8, 128), F32)],
        scratch_shapes=[
            pltpu.VMEM((216, slots), F32),
            *[pltpu.VMEM(array.shape, BF16) for array in constants[1:]],
            pltpu.SemaphoreType.DMA((12,)),
            pltpu.VMEM((216, slots), F32),
            pltpu.VMEM((216, slots), F32),
            pltpu.VMEM((432, slots), F32),
            pltpu.VMEM((6, 144, slots), BF16),
            pltpu.VMEM((480, slots), F32),
            pltpu.VMEM((6, slots, slots), BF16),
            pltpu.VMEM((6, slots, slots), BF16),
            pltpu.VMEM((2, capacity, capacity), BF16),
            pltpu.VMEM((4, LD * LATERAL, LATERAL), BF16),
            pltpu.VMEM((2, slots, capacity), BF16),
            pltpu.VMEM((slots, LD * LATERAL), BF16),
            pltpu.VMEM((8, 2 * capacity + 4 * LATERAL), F32),
            pltpu.VMEM((16, 128), F32),
            pltpu.VMEM((2, LD, 40, half), F32),
            pltpu.VMEM((LD - 1, 80, LATERAL), F32),
            pltpu.VMEM((2, LD - 1, 40, half), F32),
            pltpu.VMEM((2, 40, half), F32),
            pltpu.VMEM((ITERS, 2, LD, 40, half), F32),
            pltpu.VMEM((ITERS, LD - 1, 80, LATERAL), F32),
            pltpu.VMEM((ITERS, 2, LD - 1, 40, half), F32),
            pltpu.VMEM((8, 128), F32),
            pltpu.VMEM((part_count, 8, 128), F32),
            pltpu.SemaphoreType.DMA((ITERS, copies)),
            pltpu.SemaphoreType.DMA((ITERS, copies)),
            pltpu.SemaphoreType.DMA((part_count,)),
            pltpu.SemaphoreType.DMA((part_count,)),
        ],
        compiler_params=pltpu.CompilerParams(
            collective_id=2, has_side_effects=True, vmem_limit_bytes=60 * 1024 * 1024
        ),
        name="smooth",
    )(
        start, rhs, spectrum_top, rows, col, send, flag, elem, *map(jnp.asarray, constants)
    )
    return x, shown


def on_device(*arguments):
    rhs, send_rec, rec_elem = arguments[0], arguments[9], arguments[4]
    part_count = lax.axis_size("parts")
    capacity, slots = send_rec.shape[0] // part_count, rhs.shape[1]
    suits = slots % 128 == 0 and rec_elem.shape[0] % 1024 == 0 and capacity % 256 == 0
    suits = suits and capacity <= slots <= 4096 and part_count % LD == 0 and part_count >= 3 * LD
    if not suits:
        return general_path(*arguments)
    x, shown = fast_path(*arguments)
    norms = shown[: 2 * ITERS, 0].reshape(ITERS, 2)
    return lax.cond(
        shown[2 * ITERS, 0] > 0.0, lambda: general_path(*arguments), lambda: (x, norms)
    )


def solution(mesh):
    placed = (
        P(None, "parts"),
        P(None, "parts"),
        P(),
        P("parts"),
        P("parts"),
        P("parts"),
        P("parts"),
        P("parts"),
        P("parts"),
        P("parts"),
    )
    return jax.shard_map(
        on_device, mesh=mesh, in_specs=placed, out_specs=(P(None, "parts"), P()), check_vma=False
    )
```

```python
import functools
import math

import jax
import jax.numpy as jnp
import numpy as np
from jax import lax
from jax.experimental import pallas as pl
from jax.experimental.pallas import tpu as pltpu
from jax.sharding import PartitionSpec as P

LD = 4
ITERS = 3


PENALTY = 36.0
BOTTOM_RATIO = 8.0


def lobatto_tables():
    root_seven = math.sqrt(7.0)
    inner_root = math.sqrt(1.0 / 3.0 - 2.0 * root_seven / 21.0)
    outer_root = math.sqrt(1.0 / 3.0 + 2.0 * root_seven / 21.0)
    points = (np.array([-1.0, -outer_root, -inner_root, inner_root, outer_root, 1.0]) + 1.0) / 2.0
    weights = (
        np.array(
            [
                1.0 / 15.0,
                (14.0 - root_seven) / 30.0,
                (14.0 + root_seven) / 30.0,
                (14.0 + root_seven) / 30.0,
                (14.0 - root_seven) / 30.0,
                1.0 / 15.0,
            ]
        )
        / 2.0
    )
    barycentric = np.array(
        [1.0 / np.prod([points[j] - points[k] for k in range(6) if k != j]) for j in range(6)]
    )
    derivative = np.zeros((6, 6))
    for i in range(6):
        for j in range(6):
            if i != j:
                derivative[i, j] = barycentric[j] / barycentric[i] / (points[i] - points[j])
        derivative[i, i] = -np.sum(derivative[i])
    halves = np.zeros((2, 6, 6))
    for which_half in range(2):
        targets = (points + which_half) / 2.0
        for i in range(6):
            for j in range(6):
                halves[which_half, i, j] = np.prod(
                    [(targets[i] - points[k]) / (points[j] - points[k]) for k in range(6) if k != j]
                )
    column_sums = np.sum(derivative * derivative * weights[:, None], axis=0)
    stiff_diag = (
        column_sums[:, None, None] * weights[None, :, None] * weights[None, None, :]
        + weights[:, None, None] * column_sums[None, :, None] * weights[None, None, :]
        + weights[:, None, None] * weights[None, :, None] * column_sums[None, None, :]
    )
    return (weights, derivative, halves, stiff_diag.reshape(216))


BF16 = jnp.bfloat16
F32 = jnp.float32


def split_np(matrix):
    high = np.asarray(matrix, np.float32).astype(BF16)
    low = (np.asarray(matrix, np.float64) - high.astype(np.float64)).astype(np.float32).astype(BF16)
    return high, low


def operators():
    weights, derivative, halves, stiff_diag = lobatto_tables()
    eye = np.eye(6)
    trace_rows = []
    for direction in range(6):
        axis_index = direction // 2
        layer_index = 5 * (direction % 2)
        orientation = 2.0 * (direction % 2) - 1.0
        for row in (eye[layer_index], orientation * derivative[layer_index]):
            factors = [eye, eye, eye]
            factors[axis_index] = row[None, :]
            trace_rows.append(np.kron(np.kron(factors[0], factors[1]), factors[2]))
    traces = np.concatenate(trace_rows, axis=0)
    stiff_1d = derivative.T @ (weights[:, None] * derivative)
    mass = np.diag(weights)
    stiffness = (
        np.kron(np.kron(stiff_1d, mass), mass)
        + np.kron(np.kron(mass, stiff_1d), mass)
        + np.kron(np.kron(mass, mass), stiff_1d)
    )
    blocks = []
    for sub in range(4):
        quarter = np.kron(halves[sub % 2], halves[sub // 2])
        blocks.append(np.kron(np.eye(2), quarter))
    return traces, stiffness, np.concatenate(blocks, axis=0), np.outer(weights, weights).reshape(36, 1), stiff_diag


def split(value):
    high = value.astype(BF16)
    return high, (value - high.astype(F32)).astype(BF16)


def dot(left, right):
    return jnp.dot(left, right, preferred_element_type=F32)


def dot3(left_high, left_low, right):
    high, low = split(right)
    return dot(left_high, high) + (dot(left_high, low) + dot(left_low, high))


def one_hot(index_row, rows, base=0):
    count = index_row.shape[1]
    position = lax.broadcasted_iota(jnp.int32, (rows, count), 0)
    return jnp.where(position == index_row - base, 1.0, 0.0).astype(BF16)


def pick(traces, elem, direction, sub, onto):
    wide = dot(traces, one_hot(elem, traces.shape[1]))
    face = jnp.zeros((72, elem.shape[1]), F32)
    for d in range(6):
        both = wide[72 * d : 72 * d + 72] + wide[432 + 72 * d : 432 + 72 * d + 72]
        face = jnp.where(direction == d, both, face)
    high, low = split(face)
    quarters = dot(onto, jnp.concatenate([high, low, high], axis=0))
    result = face
    for s in range(4):
        result = jnp.where(sub == s, quarters[72 * s : 72 * s + 72], result)
    return result


def send_kernel(x_ref, inv_ref, code_ref, mat_high, mat_low, onto_ref, out_ref, traces_ref):
    @pl.when(pl.program_id(0) == 0)
    def _():
        raw = dot3(mat_high[...], mat_low[...], x_ref[...])
        row = lax.broadcasted_iota(jnp.int32, raw.shape, 0)
        raw = jnp.where(lax.rem(row, 72) >= 36, raw * inv_ref[...], raw)
        high, low = split(raw)
        traces_ref[0:432] = high
        traces_ref[432:864] = low

    code = code_ref[...]
    picked = pick(traces_ref[...], code[0:1], code[1:2], code[2:3], onto_ref[...])
    capacity = out_ref.shape[2]
    for k in range(out_ref.shape[0]):
        out_ref[k] = picked[:, k * capacity : (k + 1) * capacity]


def exchange_kernel(
    steps, axis, width, src_ref, x_ref, traces_ref, code_ref, onto_ref, stiff_high, stiff_low,
    dst_ref, own_ref, near_ref, volume_ref, send_sem, recv_sem,
):
    count = lax.axis_size(axis)
    me = lax.axis_index(axis)
    barrier = pltpu.get_barrier_semaphore()
    peers = [lax.rem(me + step + count, count) for step in steps]
    for peer in peers:
        pl.semaphore_signal(barrier, inc=1, device_id=(peer,), device_id_type=pl.DeviceIdType.MESH)
    pl.semaphore_wait(barrier, len(steps))
    copies = []
    for k, peer in enumerate(peers):
        copy = pltpu.make_async_remote_copy(
            src_ref=src_ref.at[k],
            dst_ref=dst_ref.at[k],
            send_sem=send_sem.at[k],
            recv_sem=recv_sem.at[k],
            device_id=(peer,),
            device_id_type=pl.DeviceIdType.MESH,
        )
        copy.start()
        copies.append(copy)

    def step_tile(i, carry):
        part = pl.ds(pl.multiple_of(i * width, width), width)
        code = code_ref[:, part]
        own_ref[:, part] = pick(traces_ref[...], code[0:1], code[1:2], code[2:3], onto_ref[...])
        near_ref[:, part] = pick(traces_ref[...], code[3:4], code[4:5], code[5:6], onto_ref[...])
        return carry

    lax.fori_loop(0, code_ref.shape[1] // width, step_tile, 0)
    volume_ref[...] = dot3(stiff_high[...], stiff_low[...], x_ref[...])
    for copy in copies:
        copy.wait()


def norms_kernel(axis, sums_ref, out_ref, landing, send_sem, recv_sem):
    count = lax.axis_size(axis)
    me = lax.axis_index(axis)
    barrier = pltpu.get_barrier_semaphore()

    def greet(k, carry):
        peer = lax.rem(me + k, count)
        pl.semaphore_signal(barrier, inc=1, device_id=(peer,), device_id_type=pl.DeviceIdType.MESH)
        return carry

    def copy_to(k):
        return pltpu.make_async_remote_copy(
            src_ref=sums_ref,
            dst_ref=landing.at[k],
            send_sem=send_sem.at[k],
            recv_sem=recv_sem.at[k],
            device_id=(lax.rem(me + k, count),),
            device_id_type=pl.DeviceIdType.MESH,
        )

    def start(k, carry):
        copy_to(k).start()
        return carry

    def finish(k, carry):
        copy_to(k).wait()
        return carry

    lax.fori_loop(1, count, greet, 0)
    pl.semaphore_wait(barrier, count - 1)
    lax.fori_loop(1, count, start, 0)
    landing[0] = sums_ref[...]
    lax.fori_loop(1, count, finish, 0)

    def add(j, total):
        return total + landing[lax.rem(me + count - j, count)]

    total = lax.fori_loop(0, count, add, jnp.zeros(out_ref.shape, F32))
    out_ref[...] = jnp.broadcast_to(jnp.sum(total, axis=1, keepdims=True), out_ref.shape)


def apply_kernel(
    row_ref, coef_ref, x_ref, dirn_ref, rhs_ref, elem_ref, prec_ref, recv_ref, own_ref, near_ref,
    volume_ref, code_ref, rows_ref, size_ref, off_ref, weight_ref, lift_high, lift_low, prior_ref,
    x_out, dirn_out, sums_out, pool, total,
):
    peer_count = recv_ref.shape[0]

    @pl.when(pl.program_id(0) == 0)
    def _():
        for k in range(peer_count):
            high, low = split(recv_ref[k])
            pool[144 * k : 144 * k + 72] = high
            pool[144 * k + 72 : 144 * k + 144] = low
        total[...] = jnp.zeros_like(total)

    code = code_ref[...]
    direction, sub = code[1:2], code[2:3]
    bound = code[6:7] == -1
    width = sub.shape[1]
    own = own_ref[...]
    wide = dot(pool[...], one_hot(code[7:8], pool.shape[1]))
    partner = near_ref[...]
    for k in range(peer_count):
        both = wide[144 * k : 144 * k + 72] + wide[144 * k + 72 : 144 * k + 144]
        partner = jnp.where(code[6:7] == k, both, partner)
    own_value, own_slope = own[0:36], own[36:72]
    part_value = jnp.where(bound, 0.0, partner[0:36])
    part_slope = jnp.where(bound, -own_slope, partner[36:72])
    jump = own_value - part_value
    flux = 0.5 * (own_slope - part_slope)
    mortar = size_ref[0:1]
    area = mortar * mortar
    weight = weight_ref[...] * size_ref[1:2]
    term_value = weight * (PENALTY * mortar * jump - area * flux)
    term_slope = -weight * (jnp.where(bound, 1.0, 0.5) * area) * jump
    terms = jnp.concatenate([term_value, term_slope], axis=0)
    spread = jnp.concatenate([jnp.where(sub == s, terms, 0.0) for s in range(4)], axis=0)
    spread_high, spread_low = split(spread)
    back = dot(off_ref[...], jnp.concatenate([spread_high, spread_low, spread_high], axis=0))
    back = jnp.where(sub >= 4, terms, back)
    spread = jnp.concatenate([jnp.where(direction == d, back, 0.0) for d in range(6)], axis=0)
    wide_high, wide_low = split(spread)
    lanes = lax.broadcasted_iota(jnp.int32, (width, total.shape[1]), 1)
    hot = jnp.where(lanes == rows_ref[...], 1.0, 0.0).astype(BF16)
    total[...] += dot(wide_high, hot) + dot(wide_low, hot)

    @pl.when(pl.program_id(0) == pl.num_programs(0) - 1)
    def _():
        size, inv = elem_ref[0:1], elem_ref[1:2]
        field = x_ref[...]
        row = lax.broadcasted_iota(jnp.int32, total.shape, 0)
        faces = jnp.where(lax.rem(row, 72) >= 36, total[...] * inv, total[...])
        applied = size * volume_ref[...]
        applied = applied + dot3(lift_high[...], lift_low[...], faces)
        residual = jnp.where(size > 0.0, rhs_ref[...] - applied, 0.0)
        scaled = residual * (inv * prec_ref[...])
        step = coef_ref[0] * dirn_ref[...] + coef_ref[1] * scaled
        dirn_out[...] = step
        x_out[...] = field + step
        squares = jnp.sum(residual * residual, axis=0, keepdims=True)
        products = jnp.sum(residual * scaled, axis=0, keepdims=True)
        fold = lambda line: sum(line[:, k : k + 128] for k in range(0, line.shape[1], 128))
        row = lax.broadcasted_iota(jnp.int32, sums_out.shape, 0)
        row_index = row_ref[0]
        later = jnp.where(row == 2 * row_index + 1, fold(products), prior_ref[...])
        sums_out[...] = jnp.where(row == 2 * row_index, fold(squares), later)


def take_small(tables, index):
    rows = tables.shape[1] // 128
    fine = (jnp.arange(128, dtype=jnp.int32)[:, None] == (index % 128)[None, :]).astype(BF16)
    wide = jnp.dot(tables.reshape(-1, 128).astype(BF16), fine, preferred_element_type=F32)
    wide = wide.reshape(tables.shape[0], rows, -1)
    coarse = jnp.arange(rows, dtype=jnp.int32)[:, None] == (index // 128)[None, :]
    return jnp.sum(jnp.where(coarse[None], wide, 0.0), axis=1).astype(jnp.int32)


def tile(count):
    for width in (512, 256, 128):
        if count % width == 0:
            return width
    return count


def whole(shape):
    return pl.BlockSpec(shape, lambda i: (0,) * len(shape))


def general_path(
    rhs, start, spectrum_top, elem_code, rec_elem, rec_dir, rec_sub, rec_peer, rec_index, send_rec
):
    traces, stiffness, interp, face_weight, stiff_diag = operators()
    part_count = lax.axis_size("parts")
    own_index = lax.axis_index("parts")
    elem_count = rhs.shape[1]
    record_count = rec_elem.shape[0]
    capacity = send_rec.shape[0] // part_count
    far_reach = 2 * LD - 1
    code_float = elem_code.astype(F32)
    elem_size = 0.5 * code_float
    inv_size = jnp.where(elem_code > 0, 2.0 / jnp.maximum(code_float, 1.0), 0.0)
    elem_rows = jnp.stack([elem_size, inv_size])
    is_bound = rec_peer < 0
    is_local = rec_peer == own_index
    is_remote = jnp.logical_and(jnp.logical_not(is_bound), jnp.logical_not(is_local))
    offset = own_index - rec_peer
    position = jnp.where(offset < 0, offset + far_reach, offset + far_reach - 1)
    block = jnp.where(is_remote, position, jnp.where(is_bound, -1, -2))
    steps = list(range(-far_reach, 0)) + list(range(1, far_reach + 1))
    lists = send_rec.reshape(part_count, capacity)
    lists = jnp.concatenate([lists[part_count - far_reach :], lists, lists[:far_reach]], axis=0)
    lists = lax.dynamic_slice_in_dim(lists, own_index, 2 * far_reach + 1, 0)
    send_cols = jnp.concatenate([lists[:far_reach], lists[far_reach + 1 :]], axis=0).reshape(-1)
    send_count = send_cols.shape[0]

    own_size = 0.5 * take_small(elem_code[None], rec_elem)[0].astype(F32)
    mortar_size = jnp.where(rec_sub < 4, 0.5 * own_size, own_size)
    size_rows = jnp.stack([mortar_size, (rec_sub < 5).astype(F32)])
    tables = jnp.stack([rec_elem // 256, rec_elem % 256, rec_dir * 8 + rec_sub])
    found = take_small(tables, jnp.concatenate([send_cols, rec_index]))
    found = jnp.stack([found[0] * 256 + found[1], found[2] // 8, found[2] % 8])
    send_code = found[:, :send_count]
    near = jnp.where(is_local[None], found[:, send_count:], -1)
    rec_code = jnp.concatenate(
        [jnp.stack([rec_elem, rec_dir, rec_sub]), near, block[None], rec_index[None]],
        axis=0,
    )
    rec_rows = rec_elem[:, None]

    mat_high, mat_low = split_np(traces)
    lift_high, lift_low = split_np(traces.T)
    stiff_high, stiff_low = split_np(stiffness)
    onto_high, onto_low = split_np(interp)
    onto = np.concatenate([onto_high, onto_high, onto_low], axis=1)
    flat = np.concatenate([interp[72 * s : 72 * s + 72].T for s in range(4)], axis=1)
    off_high, off_low = split_np(flat)
    off = np.concatenate([off_high, off_high, off_low], axis=1)
    prec = jnp.asarray((1.0 / stiff_diag).reshape(216, 1), F32)
    weight = jnp.asarray(face_weight, F32)

    send_tile, rec_tile, peer_count = 2 * capacity, tile(record_count), len(steps)
    params = pltpu.CompilerParams(vmem_limit_bytes=60 * 1024 * 1024)
    field = (216, elem_count)

    def send_call(x):
        return pl.pallas_call(
            send_kernel,
            grid=(send_count // send_tile,),
            in_specs=[
                whole(field),
                whole((1, elem_count)),
                pl.BlockSpec((3, send_tile), lambda i: (0, i)),
                whole((432, 216)),
                whole((432, 216)),
                whole((288, 216)),
            ],
            out_specs=[pl.BlockSpec((2, 72, capacity), lambda i: (i, 0, 0)), whole((864, elem_count))],
            out_shape=[
                jax.ShapeDtypeStruct((peer_count, 72, capacity), F32),
                jax.ShapeDtypeStruct((864, elem_count), BF16),
            ],
            compiler_params=params,
            name="send_traces",
        )(x, inv_size[None], send_code, jnp.asarray(mat_high), jnp.asarray(mat_low), jnp.asarray(onto))

    vmem = pl.BlockSpec(memory_space=pltpu.VMEM)

    def exchange(outgoing, x, element_traces):
        return pl.pallas_call(
            functools.partial(exchange_kernel, steps, "parts", rec_tile),
            in_specs=[pl.BlockSpec(memory_space=pl.ANY)] + [vmem] * 6,
            out_specs=[pl.BlockSpec(memory_space=pl.ANY)] + [vmem] * 3,
            out_shape=[
                jax.ShapeDtypeStruct((peer_count, 72, capacity), F32),
                jax.ShapeDtypeStruct((72, record_count), F32),
                jax.ShapeDtypeStruct((72, record_count), F32),
                jax.ShapeDtypeStruct(field, F32),
            ],
            scratch_shapes=[
                pltpu.SemaphoreType.DMA((peer_count,)),
                pltpu.SemaphoreType.DMA((peer_count,)),
            ],
            compiler_params=pltpu.CompilerParams(
                collective_id=0, has_side_effects=True, vmem_limit_bytes=60 * 1024 * 1024
            ),
            name="exchange",
        )(
            outgoing, x, element_traces, rec_code, jnp.asarray(onto),
            jnp.asarray(stiff_high), jnp.asarray(stiff_low),
        )

    def all_sums(sums):
        return pl.pallas_call(
            functools.partial(norms_kernel, "parts"),
            in_specs=[vmem],
            out_specs=vmem,
            out_shape=jax.ShapeDtypeStruct((8, 128), F32),
            scratch_shapes=[
                pltpu.VMEM((part_count, 8, 128), F32),
                pltpu.SemaphoreType.DMA((part_count,)),
                pltpu.SemaphoreType.DMA((part_count,)),
            ],
            compiler_params=pltpu.CompilerParams(collective_id=1, has_side_effects=True),
            name="all_sums",
        )(sums)

    def apply_call(row_index, coef, x, dirn, received, own, near_traces, volume, sums):
        tiles = lambda rows: pl.BlockSpec((rows, rec_tile), lambda i: (0, i))
        return pl.pallas_call(
            apply_kernel,
            grid=(record_count // rec_tile,),
            in_specs=[
                pl.BlockSpec(memory_space=pltpu.SMEM),
                pl.BlockSpec(memory_space=pltpu.SMEM),
                whole(field),
                whole(field),
                whole(field),
                whole((2, elem_count)),
                whole((216, 1)),
                whole((peer_count, 72, capacity)),
                tiles(72),
                tiles(72),
                whole(field),
                tiles(8),
                pl.BlockSpec((rec_tile, 1), lambda i: (i, 0)),
                tiles(2),
                whole((72, 864)),
                whole((36, 1)),
                whole((216, 432)),
                whole((216, 432)),
                whole((8, 128)),
            ],
            out_specs=[whole(field), whole(field), whole((8, 128))],
            out_shape=[
                jax.ShapeDtypeStruct(field, F32),
                jax.ShapeDtypeStruct(field, F32),
                jax.ShapeDtypeStruct((8, 128), F32),
            ],
            scratch_shapes=[
                pltpu.VMEM((144 * peer_count, capacity), BF16),
                pltpu.VMEM((432, elem_count), F32),
            ],
            compiler_params=params,
            name="apply_operator",
        )(
            row_index[None], coef, x, dirn, rhs, elem_rows, prec, received, own, near_traces, volume, rec_code, rec_rows,
            size_rows, jnp.asarray(off), weight, jnp.asarray(lift_high), jnp.asarray(lift_low), sums,
        )

    scale_total = 216.0 * elem_count * part_count
    top_value = spectrum_top[0]
    bottom = top_value / BOTTOM_RATIO
    center = 0.5 * (top_value + bottom)
    radius = 0.5 * (top_value - bottom)
    sigma_ratio = center / radius
    rho_prev = 1.0 / sigma_ratio
    coefs = [jnp.stack([jnp.zeros_like(center), 1.0 / center])]
    for step_index in range(1, ITERS):
        rho_next = 1.0 / (2.0 * sigma_ratio - rho_prev)
        coefs.append(jnp.stack([rho_next * rho_prev, 2.0 * rho_next / radius]))
        rho_prev = rho_next
    coefs = jnp.stack(coefs)

    def one_step(step_index, state):
        x, dirn, sums = state
        outgoing, element_traces = send_call(x)
        moved = exchange(outgoing, x, element_traces)
        coef = lax.dynamic_index_in_dim(coefs, step_index, 0, False)
        return tuple(apply_call(step_index, coef, x, dirn, *moved, sums))

    x, dirn, sums = lax.fori_loop(0, ITERS, one_step, (start, start, jnp.zeros((8, 128), F32)))
    norms = 0.5 * jnp.log(all_sums(sums)[: 2 * ITERS, 0].reshape(ITERS, 2) / scale_total)
    return (x, norms)


LATERAL = 128
FIELDS = 9


def iota(shape, axis):
    return lax.broadcasted_iota(jnp.int32, shape, axis)


def sum_rows(value):
    return jnp.sum(value, axis=0, keepdims=True)


def total_of(value):
    return jnp.sum(value, axis=1, keepdims=True)


def look_up(tables, rows, index):
    hot = jnp.where(iota((128, index.shape[1]), 0) == (index & 127), 1.0, 0.0).astype(BF16)
    wide = dot(tables, hot)
    mask = iota((rows, index.shape[1]), 0) == (index >> 7)
    count = tables.shape[0] // rows
    return [sum_rows(jnp.where(mask, wide[k * rows : (k + 1) * rows], 0.0)) for k in range(count)]


def regroup(columns, position, rows):
    mask = iota((rows, position.shape[1]), 0) == (position >> 7)
    left = jnp.concatenate([jnp.where(mask, column, 0.0) for column in columns], axis=0).astype(BF16)
    hot = jnp.where(iota((128, position.shape[1]), 0) == (position & 127), 1.0, 0.0).astype(BF16)
    return lax.dot_general(left, hot, (((1,), (1,)), ((), ())), preferred_element_type=F32)


def setup_kernel(
    axis, capacity, code_ref, elem_ref, dir_ref, sub_ref, peer_ref, index_ref,
    code_line, elem_line, dir_line, sub_line, peer_line, index_line, lists_ref,
    rows_ref, col_ref, send_ref, flag_ref, elem_out,
):
    me = lax.axis_index(axis)
    count = lax.axis_size(axis)
    group, place = me // LD, lax.rem(me, LD)
    elem, direction, sub = elem_line[...], dir_line[...], sub_line[...]
    peer, index = peer_line[...], index_line[...]
    records, slots = elem.shape[1], code_line.shape[1]
    chunks, table_rows, slot_rows = records // 128, records // 128, 6 * slots // 128
    used = sub < 5
    local = used & (peer == me)
    bound = used & (peer < 0)
    remote = used & (peer >= 0) & (peer != me)

    kind = jnp.where(used, jnp.where(remote, direction, direction + 8), -1)
    member = jnp.where(iota((16, records), 0) == kind, 1.0, 0.0)
    stacked = jnp.concatenate([member[:, 128 * k : 128 * k + 128] for k in range(chunks)], axis=0)
    upper = jnp.where(iota((128, 128), 0) < iota((128, 128), 1), 1.0, 0.0)
    counted = dot(
        stacked.astype(BF16), jnp.concatenate([upper, jnp.ones((128, 128), F32)], axis=1).astype(BF16)
    )
    carry = jnp.zeros((16, 128), F32)
    before = []
    for k in range(chunks):
        before.append(counted[16 * k : 16 * k + 16, :128] + carry)
        carry = carry + counted[16 * k : 16 * k + 16, 128:]
    base = jnp.concatenate([jnp.zeros((8, 128), F32), carry[:8]], axis=0)
    before = jnp.concatenate([part + base for part in before], axis=1)
    rank = sum_rows(before * member).astype(jnp.int32)
    in_range = used & (rank < slots)
    slot = jnp.where(in_range, direction * slots + rank, -1)

    tables = jnp.concatenate(
        [
            (elem_ref[...] & 127).astype(F32),
            ((elem_ref[...] >> 7) * 8 + sub_ref[...]).astype(F32),
            dir_ref[...].astype(F32),
        ],
        axis=0,
    ).astype(BF16)
    rows_per = capacity // 128
    list_rows = iota(lists_ref.shape, 0)
    lists = lists_ref[...].astype(F32)
    channel = []
    for d, other in ((1, group + 1), (0, group - 1)):
        here = remote & (direction == d)
        most = jnp.max(jnp.where(here, peer, -1), axis=1, keepdims=True)
        least = jnp.min(jnp.where(here, peer, count), axis=1, keepdims=True)
        wrong = here & (peer // LD != other)
        channel.append((most, jnp.where((most >= 0) & (most != least), 1.0, 0.0), wrong))
    wanted = []
    for most, _, _ in channel:
        for part in range(rows_per):
            wanted.append(sum_rows(jnp.where(list_rows == most * rows_per + part, lists, 0.0)))
    for pos in range(LD - 1):
        dest = group * LD + lax.rem(place + pos + 1, LD)
        wanted.append(sum_rows(jnp.where(list_rows == dest * rows_per, lists, 0.0)))
    wanted.append(jnp.zeros((1, LATERAL), F32))
    wanted = jnp.concatenate(wanted, axis=1).astype(jnp.int32)
    wanted_count = wanted.shape[1]
    low, high, found_dir = look_up(tables, table_rows, jnp.concatenate([wanted, index], axis=1))
    high = high.astype(jnp.int32)
    found_elem = low.astype(jnp.int32) + 128 * (high >> 3)
    found_sub = high & 7
    send_ref[0:1] = found_elem[:, :wanted_count]
    send_ref[1:2] = found_dir[:, :wanted_count].astype(jnp.int32)
    send_ref[2:3] = found_sub[:, :wanted_count]
    send_ref[3:8] = jnp.zeros((5, wanted_count), jnp.int32)
    near_elem, near_sub = found_elem[:, wanted_count:], found_sub[:, wanted_count:]

    code_rows = -(-slots // 1024) * 8
    code_table = code_ref[...].astype(F32)
    if code_rows > code_table.shape[0]:
        pad = jnp.zeros((code_rows - code_table.shape[0], 128), F32)
        code_table = jnp.concatenate([code_table, pad], axis=0)
    code = look_up(code_table.astype(BF16), code_rows, elem)[0]
    size = 0.5 * code
    mortar = jnp.where(sub < 4, 0.5 * size, size)

    turn = lax.rem(place - lax.rem(peer, LD) + LD, LD) - 1
    landed = jnp.where(direction < 2, index, turn * LATERAL + index)
    split_near = jnp.where(sub < 4, sub, jnp.where(near_sub < 4, near_sub + 4, 8))
    split_far = jnp.minimum(sub, 4)
    real = lambda value: value.astype(F32)
    columns = [
        real(elem & 127),
        real((elem >> 7) + 1),
        real(near_elem & 127),
        jnp.where(local, real((near_elem >> 7) + 1), 0.0),
        jnp.where(remote, real(landed & 127), 0.0),
        jnp.where(remote, real((landed >> 7) + 1), 0.0),
        real(split_near),
        real(split_far),
        mortar,
    ]
    moved = regroup(columns, slot, slot_rows)
    part = lambda k: moved[k * slot_rows : (k + 1) * slot_rows]
    join = lambda k: jnp.where(part(k + 1) > 0.0, part(k) + 128.0 * (part(k + 1) - 1.0), -1.0)
    own = join(0)
    spare = col_ref.shape[1] - slot_rows
    own_all = jnp.concatenate([own, jnp.zeros((spare, 128), F32)], axis=0)
    col_ref[...] = jnp.transpose(own_all).astype(jnp.int32)
    mort = part(8)
    fields = [join(2), join(4), part(6), part(7), 36.0 * mort, 0.5 * mort * mort]

    face = jnp.where(used, direction * slots + elem, -1)
    marks = [jnp.where(used & (sub == s), 1.0, 0.0) for s in range(5)]
    marks.append(jnp.where(bound & (sub == 4), 1.0, 0.0))
    tally = regroup(marks, face, slot_rows)
    fields += [tally[k * slot_rows : (k + 1) * slot_rows] for k in range(6)]
    per = slots // 128
    lines = []
    for value in fields:
        pieces = []
        for d in range(6):
            pieces.append(
                jnp.concatenate([value[per * d + q : per * d + q + 1] for q in range(per)], axis=1)
            )
        pieces.append(jnp.zeros((2, slots), F32))
        lines.append(jnp.concatenate(pieces, axis=0))
    code_all = code_line[...].astype(F32)
    size_all = 0.5 * code_all
    inv_all = jnp.where(code_all > 0.0, 2.0 / jnp.maximum(code_all, 1.0), 0.0)
    elem_out[0:1] = size_all
    elem_out[1:2] = inv_all
    elem_out[2:8] = jnp.zeros((6, slots), F32)
    half = 0.5 * size_all
    counts, bounds = lines[6:11], lines[11]
    lines = lines[:6]
    for s in range(5):
        lines.append(36.0 * (half if s < 4 else size_all) * counts[s])
    for s in range(4):
        lines.append(half * half * (0.5 * counts[s]))
    lines.append(size_all * size_all * (0.5 * (counts[4] + bounds)))
    for k, line in enumerate(lines):
        rows_ref[8 * k : 8 * k + 8] = line
    rows_ref[8 * len(lines) :] = jnp.zeros((rows_ref.shape[0] - 8 * len(lines), slots), F32)

    wrong = jnp.where(remote & (direction >= 2) & ((peer // LD != group) | (index >= LATERAL)), 1.0, 0.0)
    wrong = wrong + jnp.where(bound & (sub < 4), 1.0, 0.0)
    wrong = wrong + jnp.where(local & (sub < 4) & (near_sub < 4), 1.0, 0.0)
    wrong = wrong + jnp.where(used & (rank >= slots), 1.0, 0.0)
    for _, _, off in channel:
        wrong = wrong + jnp.where(off, 1.0, 0.0)
    faults = total_of(wrong) + channel[0][1] + channel[1][1]
    row = iota((8, 128), 0)
    allowed = jnp.where(row < 2, float(capacity), float(LATERAL))
    over = jnp.where((row < 6) & (carry[:8] > allowed), 1.0, 0.0)
    faults = faults + total_of(sum_rows(over))
    turns = [
        lax.rem(place - lax.rem(jnp.maximum(most, 0), LD) + LD, LD).astype(F32) for most, _, _ in channel
    ]
    ahead = [
        jnp.where(most >= 0, lax.rem(jnp.maximum(most, 0) % LD - place + LD, LD), -1).astype(F32)
        for most, _, _ in channel
    ]
    flags = jnp.where(row == 0, faults, jnp.where(row == 1, turns[1], turns[0]))
    flag_ref[...] = jnp.where(row == 3, ahead[0], jnp.where(row == 4, ahead[1], flags))


def stack2(value):
    high = value.astype(BF16).astype(F32)
    return jnp.concatenate([high, value - high], axis=0).astype(BF16)


def stack3(value):
    high = value.astype(BF16).astype(F32)
    return jnp.concatenate([high, value - high, high], axis=0).astype(BF16)


def fold_pair(value):
    half = value.shape[0] // 2
    return value[:half] + value[half:]


def choose(blocks, rows, code):
    last = blocks.shape[0] // rows - 1
    result = blocks[last * rows :]
    for q in range(last):
        result = jnp.where(code == q, blocks[q * rows : q * rows + rows], result)
    return result


def main_kernel(
    axis, iters, capacity,
    x_ref, rhs_hbm, top_ref, rows_ref, col_ref, send_ref, flag_ref, elem_ref, prec_ref,
    trace_high_hbm, trace_low_hbm, stiff_high_hbm, stiff_low_hbm, lift_high_hbm, lift_low_hbm,
    onto_hbm, own_hbm, near_hbm, far_hbm,
    x_out, norm_out,
    rhs_ref, trace_high, trace_low, stiff_high, stiff_low, lift_high, lift_low,
    onto_ref, own_ref, near_ref, far_ref, load_sem,
    dirn, volume, traces, pairs, faces, scatter, gather, gather_chan, gather_lat, send_chan, send_lat,
    far_rows, coefs, snd_chan, snd_lat, snd_pass, kept_pass, rcv_chan, rcv_lat, rcv_pass, sums, landing,
    send_sem, recv_sem, sum_send, sum_recv,
):
    count = lax.axis_size(axis)
    me = lax.axis_index(axis)
    group, place = me // LD, lax.rem(me, LD)
    groups = count // LD
    slots, half = x_ref.shape[1], capacity // 2
    mesh_id = pl.DeviceIdType.MESH
    barrier = pltpu.get_barrier_semaphore()

    def greet(k, carry):
        peer = lax.rem(me + k, count)
        pl.semaphore_signal(barrier, inc=1, device_id=(peer,), device_id_type=mesh_id)
        return carry

    lax.fori_loop(1, count, greet, 0)
    held = [
        (x_ref, x_out),
        (trace_high_hbm, trace_high),
        (trace_low_hbm, trace_low),
        (onto_hbm, onto_ref),
        (stiff_high_hbm, stiff_high),
        (stiff_low_hbm, stiff_low),
        (own_hbm, own_ref),
        (near_hbm, near_ref),
        (far_hbm, far_ref),
        (lift_high_hbm, lift_high),
        (lift_low_hbm, lift_low),
        (rhs_hbm, rhs_ref),
    ]
    loads = [pltpu.make_async_copy(src, dst, load_sem.at[k]) for k, (src, dst) in enumerate(held)]
    for load in loads:
        load.start()

    def hot(mask):
        return jnp.where(mask, 1.0, 0.0).astype(BF16)

    per = slots // 128
    columns = col_ref[...]
    for d in range(6):
        line = rows_ref[d : d + 1].astype(jnp.int32)
        gather[d] = hot(iota((slots, slots), 0) == line)
        for q in range(per):
            column = columns[:, per * d + q : per * d + q + 1]
            scatter[d, 128 * q : 128 * q + 128] = hot(iota((128, slots), 1) == column)
        line = rows_ref[8 + d : 9 + d].astype(jnp.int32)
        if d < 2:
            gather_chan[d] = hot(iota((capacity, capacity), 0) == line[:, :capacity])
        else:
            gather_lat[d - 2] = hot(iota((LD * LATERAL, LATERAL), 0) == line[:, :LATERAL])
    size, inv = elem_ref[0:1], elem_ref[1:2]
    def across(side, turn):
        other = lax.rem(group + (1 if side == 0 else groups - 1), groups)
        return (other * LD + lax.rem(place + turn, LD),)

    send_elem = send_ref[0:1]
    send_chan[0] = hot(iota((slots, capacity), 0) == send_elem[:, :capacity])
    send_chan[1] = hot(iota((slots, capacity), 0) == send_elem[:, capacity : 2 * capacity])
    send_lat[...] = hot(iota((slots, LD * LATERAL), 0) == send_elem[:, 2 * capacity :])
    chosen = jnp.zeros(far_rows.shape, F32)
    for k, field in enumerate((3, 4, 5)):
        block = rows_ref[8 * field : 8 * field + 8]
        pieces = []
        for d in range(6):
            part = block[:, : capacity if d < 2 else LATERAL]
            pieces.append(sum_rows(jnp.where(iota(part.shape, 0) == d, part, 0.0)))
        chosen = jnp.where(iota(chosen.shape, 0) == k, jnp.concatenate(pieces, axis=1), chosen)
    far_rows[...] = chosen

    line = jnp.ones((1, 128), F32)
    top = top_ref[0] * line
    bottom = top / BOTTOM_RATIO
    center = 0.5 * (top + bottom)
    radius = 0.5 * (top - bottom)
    sigma = center / radius
    rho = 1.0 / sigma
    coefs[0:1] = 0.0 * line
    coefs[1:2] = 1.0 / center
    for k in range(1, iters):
        rho_next = 1.0 / (2.0 * sigma - rho)
        coefs[2 * k : 2 * k + 1] = rho_next * rho
        coefs[2 * k + 1 : 2 * k + 2] = 2.0 * rho_next / radius
        rho = rho_next
    dirn[...] = jnp.zeros_like(dirn)
    sums[...] = jnp.where(iota(sums.shape, 0) == 2 * iters, flag_ref[0:1], 0.0) * jnp.where(
        iota(sums.shape, 1) == 0, 1.0, 0.0
    )

    for load in loads:
        load.wait()
    pl.semaphore_wait(barrier, count - 1)

    def step(it, carry):
        field = x_out[...]
        field_high, field_low = split(field)

        def trace(first, last):
            high, low = trace_high[first:last], trace_low[first:last]
            raw = dot(high, field_high) + (dot(high, field_low) + dot(low, field_high))
            raw = jnp.where(lax.rem(iota(raw.shape, 0), 72) >= 36, raw * inv, raw)
            traces[first:last] = raw
            for d in range(first // 72, last // 72):
                pairs[d] = stack2(raw[72 * d - first : 72 * d + 72 - first])

        trace(0, 144)
        outgoing = jnp.concatenate(
            [fold_pair(dot(pairs[1], send_chan[0])), fold_pair(dot(pairs[0], send_chan[1]))], axis=1
        )
        outgoing = choose(dot(onto_ref[...], stack3(outgoing)), 80, send_ref[2:3, : 2 * capacity])
        spare = iota((40, half), 0) >= 36
        for side in range(2):
            ahead = flag_ref[3 + side : 4 + side, 0:1]
            for turn in range(LD):
                low, left = 40 * (turn // 2), side * capacity + half * (turn % 2)
                snd_chan[side, turn] = jnp.where(spare, ahead, outgoing[low : low + 40, left : left + half])

        def send(source, target, k, place_of):
            return pltpu.make_async_remote_copy(
                src_ref=source,
                dst_ref=target,
                send_sem=send_sem.at[it, k],
                recv_sem=recv_sem.at[it, k],
                device_id=place_of,
                device_id_type=mesh_id,
            )

        def beside(turn):
            return (group * LD + lax.rem(place + turn, LD),)

        pairs_of = [(side, turn) for side in range(2) for turn in range(LD)]
        channel = [
            send(snd_chan.at[side, turn], rcv_chan.at[it, side, turn], side * LD + turn, across(side, turn))
            for side, turn in pairs_of
        ]
        lateral = [
            send(snd_lat.at[pos], rcv_lat.at[it, pos], 2 * LD + pos, beside(pos + 1)) for pos in range(LD - 1)
        ]
        passed = [
            send(
                snd_pass.at[side, turn - 1],
                rcv_pass.at[it, side, turn - 1],
                (3 + side) * LD + turn - 1,
                beside(turn),
            )
            for side, turn in pairs_of
            if turn
        ]
        for copy in channel:
            copy.start()

        trace(144, 432)
        send_dir = send_ref[1:2, 2 * capacity :]
        outgoing = jnp.zeros((72, LD * LATERAL), F32)
        for d in range(2, 6):
            outgoing = jnp.where(send_dir == d, fold_pair(dot(pairs[d], send_lat[...])), outgoing)
        outgoing = choose(dot(onto_ref[...], stack3(outgoing)), 80, send_ref[2:3, 2 * capacity :])
        for pos in range(LD - 1):
            snd_lat[pos] = outgoing[:, pos * LATERAL : (pos + 1) * LATERAL]
        for copy in lateral:
            copy.start()

        volume[...] = dot3(stiff_high[...], stiff_low[...], field) * size

        def local_faces(d, inner):
            line = lambda k: rows_ref[pl.ds(8 * k + d, 1)]
            mass = dot(own_ref[...], stack3(traces[pl.ds(pl.multiple_of(72 * d, 8), 72)]))
            value = jnp.zeros((40, slots), F32)
            slope = jnp.zeros((40, slots), F32)
            for s in range(5):
                mass_value, mass_slope = mass[80 * s : 80 * s + 40], mass[80 * s + 40 : 80 * s + 80]
                flux = line(11 + s)
                value = value + (line(6 + s) * mass_value - flux * mass_slope)
                slope = slope - flux * mass_value
            facing = d + 1 - 2 * lax.rem(d, 2)
            found = fold_pair(dot(pairs[facing], gather[d]))
            found = choose(dot(near_ref[...], stack3(found)), 80, line(2).astype(jnp.int32))
            jump, flux = line(4), line(5)
            terms = jnp.concatenate([flux * found[40:] - jump * found[:40], flux * found[:40]], axis=0)
            back = fold_pair(dot(stack2(terms), scatter[d]))
            faces[pl.ds(pl.multiple_of(80 * d, 8), 80)] = back + jnp.concatenate([value, slope], axis=0)
            return inner

        def two_faces(k, inner):
            return local_faces(2 * k + 1, local_faces(2 * k, inner))

        lax.fori_loop(1, 3, two_faces, 0)
        for copy in channel:
            copy.wait()
        for side in range(2):
            for turn in range(LD):
                chunk = jnp.zeros((40, half), F32)
                for k in range(LD):
                    mine = rcv_chan[it, side, k][36:37, 0:1] == float((turn + k) % LD)
                    chunk = jnp.where(mine, rcv_chan[it, side, k], chunk)
                if turn:
                    snd_pass[side, turn - 1] = chunk
                else:
                    kept_pass[side] = chunk
        for copy in passed:
            copy.start()
        lax.fori_loop(0, 1, two_faces, 0)
        for copy in lateral:
            copy.wait()

        def add_far(pieces, first, last, width):
            found = jnp.concatenate(pieces, axis=1)
            left = first * capacity if first < 2 else 2 * capacity
            part = slice(left, left + width * (last - first))
            found = choose(dot(far_ref[...], stack3(found)), 80, far_rows[0:1, part].astype(jnp.int32))
            jump, flux = far_rows[1:2, part], far_rows[2:3, part]
            terms = stack2(
                jnp.concatenate([flux * found[40:] - jump * found[:40], flux * found[:40]], axis=0)
            )
            for d in range(first, last):
                start = (d - first) * width
                faces[80 * d : 80 * d + 80] += fold_pair(
                    dot(terms[:, start : start + width], scatter[d, :width])
                )

        def lifted(first, last):
            total = faces[80 * first : 80 * last]
            total = jnp.where(lax.rem(iota(total.shape, 0), 80) >= 40, total * inv, total)
            high, low = split(total)
            left, rest = lift_high[:, 80 * first : 80 * last], lift_low[:, 80 * first : 80 * last]
            return dot(left, high) + (dot(left, low) + dot(rest, high))

        sides = [rcv_lat[it, pos] for pos in range(LD - 1)] + [jnp.zeros((80, LATERAL), F32)]
        got = stack2(jnp.concatenate(sides, axis=1))
        add_far([fold_pair(dot(got, gather_lat[d])) for d in range(4)], 2, 6, LATERAL)
        volume[...] += lifted(2, 6)
        for copy in passed:
            copy.wait()

        pieces = []
        for side in range(2):
            turn = flag_ref[side + 1 : side + 2, 0:1]
            landed = [kept_pass[side]] + [rcv_pass[it, side, k] for k in range(LD - 1)]
            chunks = []
            for k in range(LD):
                chunk = landed[(-k) % LD]
                for t in range(1, LD):
                    chunk = jnp.where(turn == float(t), landed[(t - k) % LD], chunk)
                chunks.append(chunk)
            got = jnp.concatenate(
                [jnp.concatenate(chunks[:2], axis=1), jnp.concatenate(chunks[2:], axis=1)], axis=0
            )
            pieces.append(fold_pair(dot(stack2(got), gather_chan[side])))
        add_far(pieces, 0, 2, capacity)
        applied = volume[...] + lifted(0, 2)
        residual = jnp.where(size > 0.0, rhs_ref[...] - applied, 0.0)
        scaled = residual * (inv * prec_ref[...])
        first = coefs[pl.ds(2 * it, 1), 0:1]
        second = coefs[pl.ds(2 * it + 1, 1), 0:1]
        change = first * dirn[...] + second * scaled
        dirn[...] = change
        x_out[...] = field + change
        squares = sum_rows(residual * residual)
        products = sum_rows(residual * scaled)
        fold = lambda row: sum(row[:, k : k + 128] for k in range(0, row.shape[1], 128))
        row = iota(sums.shape, 0)
        kept = jnp.where(row == 2 * it + 1, fold(products), sums[...])
        sums[...] = jnp.where(row == 2 * it, fold(squares), kept)
        return carry

    lax.fori_loop(0, iters, step, 0)

    def copy_to(k):
        return pltpu.make_async_remote_copy(
            src_ref=sums,
            dst_ref=landing.at[k],
            send_sem=sum_send.at[k],
            recv_sem=sum_recv.at[k],
            device_id=(lax.rem(me + k, count),),
            device_id_type=mesh_id,
        )

    def begin(k, carry):
        copy_to(k).start()
        return carry

    def finish(k, carry):
        copy_to(k).wait()
        return carry

    def add(j, total):
        return total + landing[lax.rem(me + count - j, count)]

    lax.fori_loop(1, count, begin, 0)
    landing[0] = sums[...]
    lax.fori_loop(1, count, finish, 0)
    total = total_of(lax.fori_loop(0, count, add, jnp.zeros(sums.shape, F32)))
    mean = total / (216.0 * slots * count)
    logs = 0.5 * jnp.log(jnp.where(iota(total.shape, 0) < 2 * iters, mean, 1.0))
    shown = jnp.where(iota(total.shape, 0) < 2 * iters, logs, total)
    norm_out[...] = jnp.broadcast_to(shown, norm_out.shape)


def wide_rows(blocks):
    padded = []
    for block in blocks:
        rows = np.zeros((80, block.shape[1]))
        rows[0:36], rows[40:76] = block[0:36], block[36:72]
        padded.append(rows)
    return np.concatenate(padded, axis=0)


def three(matrix):
    high, low = split_np(matrix)
    return np.concatenate([high, high, low], axis=1)


def set_up(slots, capacity, arrays, send_rec):
    slot_rows = 6 * slots // 128
    to_lines = lambda array: array.reshape(-1, 128)
    to_line = lambda array: array.reshape(1, -1)
    vmem = pl.BlockSpec(memory_space=pltpu.VMEM)
    columns = 2 * capacity + LD * LATERAL
    return pl.pallas_call(
        functools.partial(setup_kernel, "parts", capacity),
        in_specs=[vmem] * 13,
        out_specs=[vmem] * 5,
        out_shape=[
            jax.ShapeDtypeStruct((136, slots), F32),
            jax.ShapeDtypeStruct((128, 128 * -(-slot_rows // 128)), jnp.int32),
            jax.ShapeDtypeStruct((8, columns), jnp.int32),
            jax.ShapeDtypeStruct((8, 128), F32),
            jax.ShapeDtypeStruct((8, slots), F32),
        ],
        compiler_params=pltpu.CompilerParams(vmem_limit_bytes=60 * 1024 * 1024),
        name="set_up",
    )(*map(to_lines, arrays), *map(to_line, arrays), to_lines(send_rec))


def fast_path(
    rhs, start, spectrum_top, elem_code, rec_elem, rec_dir, rec_sub, rec_peer, rec_index, send_rec
):
    traces, stiffness, interp, face_weight, stiff_diag = operators()
    part_count = lax.axis_size("parts")
    slots = rhs.shape[1]
    capacity = send_rec.shape[0] // part_count
    arrays = (elem_code, rec_elem, rec_dir, rec_sub, rec_peer, rec_index)
    vmem = pl.BlockSpec(memory_space=pltpu.VMEM)
    rows, col, send, flag, elem = set_up(slots, capacity, arrays, send_rec)

    weight = np.concatenate([face_weight, face_weight], axis=0)
    quarters = [interp[72 * s : 72 * s + 72] for s in range(4)]
    eye = np.eye(72)
    onto = three(wide_rows(quarters + [eye]))
    own = three(wide_rows([j.T @ (weight * j) for j in quarters] + [weight * eye]))
    back = [j.T * weight.T for j in quarters]
    near = three(wide_rows(back + [weight * j for j in quarters] + [weight * eye]))
    far = wide_rows(back + [weight * eye])
    far = three(wide_rows([far.T]).T)
    trace_high, trace_low = split_np(traces)
    stiff_high, stiff_low = split_np(stiffness)
    lift = np.zeros((216, 480))
    for d in range(6):
        lift[:, 80 * d : 80 * d + 36] = traces.T[:, 72 * d : 72 * d + 36]
        lift[:, 80 * d + 40 : 80 * d + 76] = traces.T[:, 72 * d + 36 : 72 * d + 72]
    lift_high, lift_low = split_np(lift)
    prec = (1.0 / stiff_diag).reshape(216, 1).astype(np.float32)
    constants = (
        prec, trace_high, trace_low, stiff_high, stiff_low, lift_high, lift_low, onto, own, near, far
    )
    copies, half = 5 * LD, capacity // 2
    hbm = pl.BlockSpec(memory_space=pltpu.HBM)
    x, shown = pl.pallas_call(
        functools.partial(main_kernel, "parts", ITERS, capacity),
        in_specs=[hbm] * 2 + [pl.BlockSpec(memory_space=pltpu.SMEM)] + [vmem] * 6 + [hbm] * 10,
        out_specs=[vmem] * 2,
        out_shape=[jax.ShapeDtypeStruct((216, slots), F32), jax.ShapeDtypeStruct((8, 128), F32)],
        scratch_shapes=[
            pltpu.VMEM((216, slots), F32),
            *[pltpu.VMEM(array.shape, BF16) for array in constants[1:]],
            pltpu.SemaphoreType.DMA((12,)),
            pltpu.VMEM((216, slots), F32),
            pltpu.VMEM((216, slots), F32),
            pltpu.VMEM((432, slots), F32),
            pltpu.VMEM((6, 144, slots), BF16),
            pltpu.VMEM((480, slots), F32),
            pltpu.VMEM((6, slots, slots), BF16),
            pltpu.VMEM((6, slots, slots), BF16),
            pltpu.VMEM((2, capacity, capacity), BF16),
            pltpu.VMEM((4, LD * LATERAL, LATERAL), BF16),
            pltpu.VMEM((2, slots, capacity), BF16),
            pltpu.VMEM((slots, LD * LATERAL), BF16),
            pltpu.VMEM((8, 2 * capacity + 4 * LATERAL), F32),
            pltpu.VMEM((16, 128), F32),
            pltpu.VMEM((2, LD, 40, half), F32),
            pltpu.VMEM((LD - 1, 80, LATERAL), F32),
            pltpu.VMEM((2, LD - 1, 40, half), F32),
            pltpu.VMEM((2, 40, half), F32),
            pltpu.VMEM((ITERS, 2, LD, 40, half), F32),
            pltpu.VMEM((ITERS, LD - 1, 80, LATERAL), F32),
            pltpu.VMEM((ITERS, 2, LD - 1, 40, half), F32),
            pltpu.VMEM((8, 128), F32),
            pltpu.VMEM((part_count, 8, 128), F32),
            pltpu.SemaphoreType.DMA((ITERS, copies)),
            pltpu.SemaphoreType.DMA((ITERS, copies)),
            pltpu.SemaphoreType.DMA((part_count,)),
            pltpu.SemaphoreType.DMA((part_count,)),
        ],
        compiler_params=pltpu.CompilerParams(
            collective_id=2, has_side_effects=True, vmem_limit_bytes=60 * 1024 * 1024
        ),
        name="smooth",
    )(
        start, rhs, spectrum_top, rows, col, send, flag, elem, *map(jnp.asarray, constants)
    )
    return x, shown


def on_device(*arguments):
    rhs, send_rec, rec_elem = arguments[0], arguments[9], arguments[4]
    part_count = lax.axis_size("parts")
    capacity, slots = send_rec.shape[0] // part_count, rhs.shape[1]
    suits = slots % 128 == 0 and rec_elem.shape[0] % 1024 == 0 and capacity % 256 == 0
    suits = suits and capacity <= slots <= 4096 and part_count % LD == 0 and part_count >= 3 * LD
    if not suits:
        return general_path(*arguments)
    x, shown = fast_path(*arguments)
    norms = shown[: 2 * ITERS, 0].reshape(ITERS, 2)
    return lax.cond(
        shown[2 * ITERS, 0] > 0.0, lambda: general_path(*arguments), lambda: (x, norms)
    )


def solution(mesh):
    placed = (
        P(None, "parts"),
        P(None, "parts"),
        P(),
        P("parts"),
        P("parts"),
        P("parts"),
        P("parts"),
        P("parts"),
        P("parts"),
        P("parts"),
    )
    return jax.shard_map(
        on_device, mesh=mesh, in_specs=placed, out_specs=(P(None, "parts"), P()), check_vma=False
    )
```
